32 devices in a mesh: model: 4 (over z), data: 8 (over y, x, core).
Axes of the slice: x: 2, y: 2, z: 4, core: 2. Of those that a mesh axis runs over, the one named last changes fastest.
Arguments:
- tokens: bfloat16 [65536, 768], P('data')
- w_up: bfloat16 [768, 3072], P(None, 'model')
- w_down: bfloat16 [3072, 768], P('model')
- task_heads: bfloat16 [2, 768, 19], replicated
- labels: int32 [2, 65536], P(None, 'data')
Outputs:
- output 1: float32 [2], replicated
- output 2: float32 [768, 3072], P('data', 'model')
- output 3: float32 [3072, 768], P(('model', 'data'))
All inputs are finite; a program needn't handle non-finite values.
Results may differ from the reference program's by a relative error of at most 0.001.
Values are sent between devices in bfloat16 or wider.
A program may use at most 1 GiB of HBM per device.

```python
import jax
import jax.numpy as jnp
from jax import lax

HIDDEN = 768
FFN = 3072
CLASSES = 19
TASKS = 2
TOKENS = 65536
SEGMENT = 8192
BLOCK = 256
STEPS = 20


def setup_inputs(seed: int = 0) -> dict:
    key_list = jax.random.split(jax.random.key(seed), 12)
    n_seg = TOKENS // SEGMENT
    seg_shift = jax.random.normal(key_list[0], (n_seg, 1, HIDDEN), jnp.float32)
    x_body = jax.random.normal(key_list[1], (n_seg, SEGMENT, HIDDEN), jnp.float32)
    tokens = (x_body + 0.5 * seg_shift).reshape(TOKENS, HIDDEN).astype(jnp.bfloat16)
    w_up = (jax.random.normal(key_list[2], (HIDDEN, FFN), jnp.float32) * HIDDEN ** -0.5).astype(jnp.bfloat16)
    w_down = (jax.random.normal(key_list[3], (FFN, HIDDEN), jnp.float32) * FFN ** -0.5).astype(jnp.bfloat16)
    task_sign = jnp.where(jnp.arange(TASKS) % 2 == 0, 1.0, -1.0).astype(jnp.float32)
    head_base = jax.random.normal(key_list[4], (HIDDEN, CLASSES), jnp.float32)
    head_own = jax.random.normal(key_list[5], (TASKS, HIDDEN, CLASSES), jnp.float32)
    task_heads = ((0.8 * task_sign[:, None, None] * head_base[None] + 0.6 * head_own) * (1.5 * HIDDEN ** -0.5)).astype(jnp.bfloat16)
    seg_pref = jax.random.randint(key_list[6], (n_seg, 1), 0, CLASSES)
    keep_pref = jax.random.randint(key_list[7], (n_seg, SEGMENT), 0, 4)
    any_label = jax.random.randint(key_list[8], (n_seg, SEGMENT), 0, CLASSES)
    shared = jnp.where(keep_pref < 3, seg_pref, any_label).reshape(TOKENS)
    own_label = jax.random.randint(key_list[9], (TASKS, TOKENS), 0, CLASSES)
    keep_shared = jax.random.randint(key_list[10], (TASKS, TOKENS), 0, 4)
    labels = jnp.where(keep_shared < 3, shared[None, :], own_label).astype(jnp.int32)
    return {'tokens': tokens, 'w_up': w_up, 'w_down': w_down, 'task_heads': task_heads, 'labels': labels}


def simplex_weights(gram_mat):
    trace_scale = jnp.trace(gram_mat) / TASKS

    def eg_step(weights, unused):
        updated = weights * jnp.exp(-jnp.sum(gram_mat * weights[None, :], axis=1) / trace_scale)
        return updated / jnp.sum(updated), None

    start_w = jnp.full((TASKS,), 1.0 / TASKS, jnp.float32)
    weights, unused = lax.scan(eg_step, start_w, None, length=STEPS)
    return weights


def reference(tokens, w_up, w_down, task_heads, labels):
    n_blocks = TOKENS // BLOCK
    tok_blocks = tokens.reshape(n_blocks, BLOCK, HIDDEN)
    lab_blocks = labels.reshape(TASKS, n_blocks, BLOCK).transpose(1, 0, 2)
    heads_f = task_heads.astype(jnp.float32)
    down_f = w_down.astype(jnp.float32)

    def block_grads(grad_acc, block_in):
        tok_blk, lab_blk = block_in
        pre_act = jnp.dot(tok_blk, w_up, preferred_element_type=jnp.float32)
        act_val, gelu_slope = jax.jvp(jax.nn.gelu, (pre_act,), (jnp.ones_like(pre_act),))
        act_bf = act_val.astype(jnp.bfloat16)
        mlp_out = jnp.dot(act_bf, w_down, preferred_element_type=jnp.float32)
        trunk_out = (tok_blk.astype(jnp.float32) + mlp_out).astype(jnp.bfloat16)
        logits = jnp.einsum('bd,tdc->tbc', trunk_out.astype(jnp.float32), heads_f)
        class_prob = jax.nn.softmax(logits, axis=-1)
        onehot = jax.nn.one_hot(lab_blk, CLASSES, dtype=jnp.float32)
        dlogit = (class_prob - onehot) / TOKENS
        d_trunk = jnp.einsum('tbc,tdc->tbd', dlogit, heads_f).astype(jnp.bfloat16).astype(jnp.float32)
        g_down = jnp.einsum('bf,tbd->tfd', act_bf.astype(jnp.float32), d_trunk)
        d_act = jnp.einsum('tbd,fd->tbf', d_trunk, down_f)
        d_pre = (d_act * gelu_slope[None]).astype(jnp.bfloat16).astype(jnp.float32)
        g_up = jnp.einsum('bd,tbf->tdf', tok_blk.astype(jnp.float32), d_pre)
        return (grad_acc[0] + g_up, grad_acc[1] + g_down), None

    zero_acc = (jnp.zeros((TASKS, HIDDEN, FFN), jnp.float32), jnp.zeros((TASKS, FFN, HIDDEN), jnp.float32))
    (g_up, g_down), unused = lax.scan(block_grads, zero_acc, (tok_blocks, lab_blocks))
    gram_mat = jnp.einsum('tij,sij->ts', g_up, g_up) + jnp.einsum('tij,sij->ts', g_down, g_down)
    task_weights = simplex_weights(gram_mat)
    grad_up = jnp.einsum('t,tij->ij', task_weights, g_up)
    grad_down = jnp.einsum('t,tij->ij', task_weights, g_down)
    return task_weights, grad_up, grad_down
```

```python
import jax
import jax.numpy as jnp
from jax import lax
from jax.experimental import pallas as pl
from jax.experimental.pallas import tpu as pltpu
from jax.sharding import PartitionSpec as P

STEPS = 20
BF = jnp.bfloat16
F32 = jnp.float32
MESH = pl.DeviceIdType.MESH
VMEM_BYTES = 63 * 1024 * 1024

D = 768
FL = 768
NTOK = 8192
NOWN = 2048
TB = 1024
NC = 19
ER = 40
CH = 256
NCH = 3

G0 = 0.7978845608028654
G1C = 0.044715 * G0


def dot_nn(a, b):
    return lax.dot_general(a, b, (((1,), (0,)), ((), ())), preferred_element_type=F32)


def dot_nt(a, b):
    return lax.dot_general(a, b, (((1,), (1,)), ((), ())), preferred_element_type=F32)


def dot_tn(a, b):
    return lax.dot_general(a, b, (((0,), (0,)), ((), ())), preferred_element_type=F32)


def gelu(x):
    t = jnp.tanh(x * (G0 + G1C * (x * x)))
    h = 0.5 * x
    return h + h * t


def gelu_and_slope(x):
    x2 = x * x
    t = jnp.tanh(x * (G0 + G1C * x2))
    h = 0.5 * x
    u = h + h * t
    s = 0.5 + 0.5 * t + h * (1.0 - t * t) * (G0 + (3.0 * G1C) * x2)
    return u, s


class Place:
    def __init__(self):
        self.z = lax.axis_index('model')
        self.j = lax.axis_index('data')
        self.core = self.j % 2
        self.x = (self.j // 2) % 2
        self.y = self.j // 4
        self.jc = self.j + 1 - 2 * self.core
        self.jx = self.j + 2 - 4 * self.x
        self.jy = self.j + 4 - 8 * self.y
        self.jd = self.jx + 4 - 8 * self.y

    def zmate(self, k):
        if isinstance(k, int):
            k0, k1 = k % 2, k // 2
        else:
            k0, k1 = k % 2, k // 2
        return (self.z % 2 + k0) % 2 + 2 * ((self.z // 2 + k1) % 2)


def remote(src, dst, ssem, rsem, z, j):
    return pltpu.make_async_remote_copy(
        src_ref=src, dst_ref=dst, send_sem=ssem, recv_sem=rsem, device_id=(z, j), device_id_type=MESH)


def forward_kernel(x_hbm, w1_ref, w2_hbm, hcat_ref, lab_hbm,
                   a_hbm, e_ref,
                   wg, w1t, xo, acc, xs, ast, lab_v, us,
                   zss, zrs, xss, xrs, yss, yrs, dss, drs, css, crs,
                   ld_sem, w2_sem, xs_sem, as_sem):
    pos = Place()
    z, j = pos.z, pos.j
    n_gran = 3 * NCH

    barrier = pltpu.get_barrier_semaphore()
    for k in (1, 2, 3):
        pl.semaphore_signal(barrier, 1, device_id=(pos.zmate(k), j), device_id_type=MESH)
    for jj in (pos.jc, pos.jx, pos.jy):
        pl.semaphore_signal(barrier, 1, device_id=(z, jj), device_id_type=MESH)

    own_rows = pl.multiple_of(z * NOWN, NOWN)
    ld_x = pltpu.make_async_copy(x_hbm.at[pl.ds(own_rows, NOWN)], xo, ld_sem.at[0])
    ld_l = pltpu.make_async_copy(lab_hbm.at[:, pl.ds(own_rows, NOWN)], lab_v, ld_sem.at[1])
    ld_w2 = [pltpu.make_async_copy(w2_hbm.at[:, c], wg.at[0, c, 1], w2_sem.at[c]) for c in range(NCH)]
    for cp in ld_w2:
        cp.start()

    def x_load(i):
        k = 1 + i // 2
        row = (pos.zmate(k) * 2 + i % 2) * TB
        return pltpu.make_async_copy(
            x_hbm.at[pl.ds(pl.multiple_of(row, TB), TB)], xs.at[i % 2], xs_sem.at[i % 2])

    x_load(0).start()
    ld_x.start()
    ld_l.start()

    w1t[...] = w1_ref[...].T
    for c in range(NCH):
        for g in range(8):
            wg[0, c, 0, g] = w1t[g * 96 + c * 32:g * 96 + c * 32 + 32, :]
    for cp in ld_w2:
        cp.wait()
    pl.semaphore_wait(barrier, 6)

    def piece(i, jj):
        return wg.at[1 + i // NCH, i % NCH, :, jj]

    def z_copy(i):
        k, c = 1 + i // NCH, i % NCH
        return remote(wg.at[0, c, :, j], wg.at[k, c, :, j], zss.at[i], zrs.at[i], pos.zmate(k), j)

    def x_copy(i):
        return remote(piece(i, j), piece(i, j), xss.at[i], xrs.at[i], z, pos.jx)

    def y_copy(i):
        return remote(piece(i, j), piece(i, j), yss.at[i], yrs.at[i], z, pos.jy)

    def diag_copy_y(i):
        return remote(piece(i, pos.jx), piece(i, pos.jx), dss.at[i], drs.at[i], z, pos.jy)

    def diag_copy_x(i):
        return remote(piece(i, pos.jy), piece(i, pos.jy), dss.at[i], drs.at[i], z, pos.jx)

    def core_copy(i, q):
        jj = (j, pos.jx, pos.jy, pos.jd)[q]
        return remote(piece(i, jj), piece(i, jj), css.at[i, q], crs.at[i, q], z, pos.jc)

    def send_own(i):
        z_copy(i).wait_recv()
        x_copy(i).start()
        y_copy(i).start()
        core_copy(i, 0).start()

    def send_side(i):
        x_copy(i).wait_recv()

        @pl.when(pos.core == 0)
        def _():
            diag_copy_y(i).start()

        core_copy(i, 1).start()
        y_copy(i).wait_recv()

        @pl.when(pos.core == 1)
        def _():
            diag_copy_x(i).start()

        core_copy(i, 2).start()

    def send_diag(i):
        diag_copy_y(i).wait_recv()
        core_copy(i, 3).start()

    def tick(i):
        if isinstance(i, int):
            if 0 <= i - 2 < n_gran:
                send_diag(i - 2)
            if 0 <= i - 1 < n_gran:
                send_side(i - 1)
            if i < n_gran:
                send_own(i)
        else:
            @pl.when(jnp.logical_and(i >= 2, i < n_gran + 2))
            def _():
                send_diag(i - 2)

            @pl.when(jnp.logical_and(i >= 1, i < n_gran + 1))
            def _():
                send_side(i - 1)

            @pl.when(i < n_gran)
            def _():
                send_own(i)

    def start_z(i, carry):
        z_copy(i).start()
        return carry

    lax.fori_loop(0, n_gran, start_z, 0)

    def a_store(c, row, slot):
        return pltpu.make_async_copy(
            ast.at[slot, c], a_hbm.at[c, pl.ds(pl.multiple_of(row, TB), TB)], as_sem.at[slot, c])

    def other_tokens(i, carry):
        slot = i % 2
        k = 1 + i // 2
        row = (pos.zmate(k) * 2 + i % 2) * TB
        x_load(i).wait()

        @pl.when(i < 5)
        def _():
            x_load(i + 1).start()

        @pl.when(i >= 2)
        def _():
            for c in range(NCH):
                a_store(c, row, slot).wait()

        for c in range(NCH):
            ast[slot, c] = dot_nt(xs[slot], wg[0, c, 0].reshape(CH, D))
            a_store(c, row, slot).start()

        @pl.when(i == 2)
        def _():
            tick(0)

        @pl.when(i == 4)
        def _():
            tick(1)

        return carry

    lax.fori_loop(0, 6, other_tokens, 0)
    ld_x.wait()

    def own_block(b, carry):
        rows = pl.ds(pl.multiple_of(b * TB, TB), TB)
        row = (z * 2 + b) * TB
        for c in range(NCH):
            a_store(c, row, b).wait()
        for c in range(NCH):
            a = dot_nt(xo[rows, :], wg[0, c, 0].reshape(CH, D))
            ast[b, c] = a
            us[:, c * CH:(c + 1) * CH] = gelu(a).astype(BF)
            a_store(c, row, b).start()
        total = dot_nn(us[:, 0:CH], wg[0, 0, 1].reshape(CH, D))
        total = total + dot_nn(us[:, CH:2 * CH], wg[0, 1, 1].reshape(CH, D))
        total = total + dot_nn(us[:, 2 * CH:3 * CH], wg[0, 2, 1].reshape(CH, D))
        acc[rows, :] = total

        @pl.when(b == 0)
        def _():
            tick(2)

        return carry

    lax.fori_loop(0, 2, own_block, 0)

    def granule(n, carry):
        tick(n + 3)
        for q in range(4):
            core_copy(n, q).wait_recv()
        k, c = 1 + n // NCH, n % NCH

        def block(b, inner):
            rows = pl.ds(pl.multiple_of(b * TB, TB), TB)
            u = gelu(dot_nt(xo[rows, :], wg[k, c, 0].reshape(CH, D))).astype(BF)
            us[:, 0:CH] = u
            acc[rows, :] += dot_nn(us[:, 0:CH], wg[k, c, 1].reshape(CH, D))
            return inner

        return lax.fori_loop(0, 2, block, carry)

    lax.fori_loop(0, n_gran, granule, 0)

    ld_l.wait()
    blk = 512
    for b in range(NOWN // blk):
        rows = slice(b * blk, (b + 1) * blk)
        zb = (xo[rows, :].astype(F32) + acc[rows, :]).astype(BF)
        logit = dot_nt(hcat_ref[...], zb)
        r = lax.broadcasted_iota(jnp.int32, (ER, blk), 0)
        first = r < NC
        second = jnp.logical_and(r >= NC, r < 2 * NC)
        neg = jnp.float32(-jnp.inf)
        m0 = jnp.max(jnp.where(first, logit, neg), axis=0, keepdims=True)
        m1 = jnp.max(jnp.where(second, logit, neg), axis=0, keepdims=True)
        ex = jnp.exp(logit - jnp.where(first, m0, m1))
        ex = jnp.where(r < 2 * NC, ex, 0.0)
        s0 = jnp.sum(jnp.where(first, ex, 0.0), axis=0, keepdims=True)
        s1 = jnp.sum(jnp.where(second, ex, 0.0), axis=0, keepdims=True)
        prob = ex / jnp.where(first, s0, s1)
        lab = jnp.where(first, lab_v[0:1, rows], lab_v[1:2, rows] + NC)
        hot = jnp.where(r == lab, 1.0, 0.0)
        e_ref[:, rows] = (prob - hot) / (NTOK * 8.0)

    for c in range(NCH):
        for b in range(2):
            a_store(c, (z * 2 + b) * TB, b).wait()

    def drain(i, carry):
        z_copy(i).wait_send()
        x_copy(i).wait_send()
        y_copy(i).wait_send()
        diag_copy_y(i).wait_send()
        for q in range(4):
            core_copy(i, q).wait_send()
        return carry

    lax.fori_loop(0, n_gran, drain, 0)


def forward(x, w1, w2r, hcat, labels):
    n_gran = 3 * NCH
    dma = pltpu.SemaphoreType.DMA
    anyspec = pl.BlockSpec(memory_space=pl.ANY)
    vspec = pl.BlockSpec(memory_space=pltpu.VMEM)
    return pl.pallas_call(
        forward_kernel,
        out_shape=(jax.ShapeDtypeStruct((NCH, NTOK, CH), F32), jax.ShapeDtypeStruct((ER, NOWN), F32)),
        in_specs=[anyspec, vspec, anyspec, vspec, anyspec],
        out_specs=(anyspec, vspec),
        scratch_shapes=[
            pltpu.VMEM((4, NCH, 2, 8, 32, D), BF),
            pltpu.VMEM((FL, D), BF),
            pltpu.VMEM((NOWN, D), BF),
            pltpu.VMEM((NOWN, D), F32),
            pltpu.VMEM((2, TB, D), BF),
            pltpu.VMEM((2, NCH, TB, CH), F32),
            pltpu.VMEM((2, NOWN), jnp.int32),
            pltpu.VMEM((TB, FL), BF),
            dma((n_gran,)), dma((n_gran,)), dma((n_gran,)), dma((n_gran,)), dma((n_gran,)), dma((n_gran,)),
            dma((n_gran,)), dma((n_gran,)), dma((n_gran, 4)), dma((n_gran, 4)),
            dma((2,)), dma((NCH,)), dma((2,)), dma((2, NCH)),
        ],
        compiler_params=pltpu.CompilerParams(
            collective_id=0, has_side_effects=True, vmem_limit_bytes=VMEM_BYTES),
        name='forward',
    )(x, w1, w2r, hcat, labels)


def backward_kernel(x_hbm, a_hbm, w2_hbm, hcat_ref, e_ref,
                    aw_ref, g1_ref, g2_ref,
                    dz, acc1, acc2, r1a, r1b, r2a, r2b, r3a, r3b,
                    abuf, xbuf, us, das, eall, w2v, hbd, mbuf, nbuf,
                    ess, ers, w2_sem, a_sem, x_sem,
                    s1s, s1r, s2s, s2r, s3s, s3r, mss, mrs, nss, nrs):
    pos = Place()
    z, j, core, px, py = pos.z, pos.j, pos.core, pos.x, pos.y

    barrier = pltpu.get_barrier_semaphore()
    for k in (1, 2, 3):
        pl.semaphore_signal(barrier, 1, device_id=(pos.zmate(k), j), device_id_type=MESH)
    for i in range(1, 8):
        pl.semaphore_signal(barrier, 1, device_id=(z, (j + i) % 8), device_id_type=MESH)

    ld_w2 = [pltpu.make_async_copy(w2_hbm.at[:, c], w2v.at[c], w2_sem.at[c]) for c in range(NCH)]
    for cp in ld_w2:
        cp.start()

    def step_of(s):
        early = s < 12
        s2 = s - 12
        c = jnp.where(early, (s % 6) // 2, s2 // 4)
        k = jnp.where(early, s // 6, 2 + (s2 % 4) // 2)
        return c, k, s % 2

    def a_load(s):
        c, k, b = step_of(s)
        row = pl.multiple_of((pos.zmate(k) * 2 + b) * TB, TB)
        return pltpu.make_async_copy(a_hbm.at[c, pl.ds(row, TB)], abuf.at[s % 2], a_sem.at[s % 2])

    def x_load(s):
        c, k, b = step_of(s)
        row = pl.multiple_of((pos.zmate(k) * 2 + b) * TB, TB)
        return pltpu.make_async_copy(x_hbm.at[pl.ds(row, TB)], xbuf.at[s % 2], x_sem.at[s % 2])

    a_load(0).start()
    x_load(0).start()

    acc1[...] = jnp.zeros_like(acc1)
    acc2[...] = jnp.zeros_like(acc2)
    hc = hcat_ref[...].astype(F32)
    r = lax.broadcasted_iota(jnp.int32, (ER, D), 0)
    h0 = jnp.where(r < NC, hc, 0.0)
    h1 = jnp.where(r >= NC, hc, 0.0)
    hb = jnp.concatenate([h0, h1], axis=1)
    hbd[...] = jnp.concatenate([hb, hb, hb], axis=0).astype(BF)
    eall[0] = e_ref[...]
    for cp in ld_w2:
        cp.wait()
    pl.semaphore_wait(barrier, 10)

    def e_copy(k):
        return remote(e_ref, eall.at[k], ess.at[k], ers.at[k], pos.zmate(k), j)

    for k in (1, 2, 3):
        e_copy(k).start()

    def core_copies(c):
        return (remote(acc1.at[c, :, :, 1 - core], r1a.at[c], s1s.at[c, 0], s1r.at[c, 0], z, pos.jc),
                remote(acc2.at[c, :, :, 1 - core], r1b.at[c], s1s.at[c, 1], s1r.at[c, 1], z, pos.jc))

    def side_copies(c):
        return (remote(acc1.at[c, :, 1 - px, core], r2a.at[c], s2s.at[c, 0], s2r.at[c, 0], z, pos.jx),
                remote(acc2.at[c, 1 - py, :, core], r2b.at[c], s2s.at[c, 1], s2r.at[c, 1], z, pos.jy))

    def last_copies(c):
        return (remote(acc1.at[c, 1 - py, px, core], r3a.at[c], s3s.at[c, 0], s3r.at[c, 0], z, pos.jy),
                remote(acc2.at[c, py, 1 - px, core], r3b.at[c], s3s.at[c, 1], s3r.at[c, 1], z, pos.jx))

    def rs_core(c):
        for cp in core_copies(c):
            cp.start()

    def rs_side(c):
        for cp in core_copies(c):
            cp.wait_recv()
        for yy in range(2):
            for xx in range(2):
                acc1[c, yy, xx, core] += r1a[c, yy, xx]
                acc2[c, yy, xx, core] += r1b[c, yy, xx]
        for cp in side_copies(c):
            cp.start()

    def rs_last(c):
        for cp in side_copies(c):
            cp.wait_recv()
        for i in range(2):
            acc1[c, i, px, core] += r2a[c, i]
            acc2[c, py, i, core] += r2b[c, i]
        for cp in last_copies(c):
            cp.start()

    def rs_done(c):
        for cp in last_copies(c):
            cp.wait_recv()
        acc1[c, py, px, core] += r3a[c]
        acc2[c, py, px, core] += r3b[c]

    sub = 256

    def step(s, carry):
        c, k, b = step_of(s)
        slot = s % 2
        t = k * 2 + b
        a_load(s).wait()
        x_load(s).wait()

        @pl.when(s < 23)
        def _():
            a_load(s + 1).start()
            x_load(s + 1).start()

        @pl.when(c == 0)
        def _():
            @pl.when(jnp.logical_and(b == 0, k > 0))
            def _():
                e_copy(k).wait_recv()

            e = eall[k, :, pl.ds(pl.multiple_of(b * TB, TB), TB)]
            e1 = e.astype(BF).astype(F32)
            rest = e - e1
            e2 = rest.astype(BF).astype(F32)
            e3 = rest - e2
            es = jnp.concatenate([e1, e2, e3], axis=0).astype(BF)
            dz[t] = dot_tn(es, hbd[...]).astype(BF)

        w2c = w2v[c].reshape(CH, D)
        for m in range(TB // sub):
            rows = slice(m * sub, (m + 1) * sub)
            u, slope = gelu_and_slope(abuf[slot, rows, :])
            us[rows, :] = u.astype(BF)
            for task in range(2):
                da = dot_nt(dz[t, rows, task * D:(task + 1) * D], w2c)
                das[rows, task * CH:(task + 1) * CH] = (da * slope).astype(BF)
        acc2[c] += dot_tn(us[...], dz[t]).reshape(2, 2, 2, 32, 2 * D)
        acc1[c] += dot_tn(xbuf[slot], das[...]).reshape(2, 2, 2, 96, 2 * CH)

        @pl.when(s == 15)
        def _():
            rs_core(0)

        @pl.when(s == 16)
        def _():
            rs_side(0)

        @pl.when(s == 19)
        def _():
            rs_core(1)

        @pl.when(s == 20)
        def _():
            rs_last(0)
            rs_side(1)

        @pl.when(s == 22)
        def _():
            rs_done(0)

        return carry

    lax.fori_loop(0, 24, step, 0)
    rs_core(2)
    rs_last(1)
    rs_side(2)
    rs_done(1)
    rs_last(2)
    rs_done(2)

    m00 = jnp.zeros((8, 128), F32)
    m01 = jnp.zeros((8, 128), F32)
    m11 = jnp.zeros((8, 128), F32)

    def fold(v):
        rows, cols = v.shape
        total = jnp.zeros((8, 128), F32)
        for q in range(cols // 128):
            total = total + jnp.sum(v[:, q * 128:(q + 1) * 128].reshape(rows // 8, 8, 128), axis=0)
        return total

    for c in range(NCH):
        for ref, width in ((acc1, CH), (acc2, D)):
            v0 = ref[c, py, px, core, :, 0:width]
            v1 = ref[c, py, px, core, :, width:2 * width]
            m00 = m00 + fold(v0 * v0)
            m01 = m01 + fold(v0 * v1)
            m11 = m11 + fold(v1 * v1)

    def full(v):
        return jnp.sum(jnp.sum(v, axis=0, keepdims=True), axis=1, keepdims=True)

    row = lax.broadcasted_iota(jnp.int32, (8, 128), 0)
    part = jnp.where(row == 0, full(m00), jnp.where(row == 1, full(m01), full(m11)))
    mbuf[j] = part

    def m_copy(i):
        return remote(mbuf.at[j], mbuf.at[j], mss.at[i], mrs.at[i], z, (j + i) % 8)

    for i in range(1, 8):
        m_copy(i).start()
    for i in range(1, 8):
        m_copy(i).wait_recv()
    total = mbuf[0]
    for i in range(1, 8):
        total = total + mbuf[i]
    nbuf[z] = total

    def n_copy(k):
        return remote(nbuf.at[z], nbuf.at[z], nss.at[k], nrs.at[k], pos.zmate(k), j)

    for k in (1, 2, 3):
        n_copy(k).start()
    for k in (1, 2, 3):
        n_copy(k).wait_recv()
    gram = nbuf[0]
    for k in (1, 2, 3):
        gram = gram + nbuf[k]

    g00, g01, g11 = gram[0:1, :], gram[1:2, :], gram[2:3, :]
    scale = (g00 + g11) / 2.0

    def eg_step(i, weights):
        a0, a1 = weights
        v0 = a0 * jnp.exp(-(g00 * a0 + g01 * a1) / scale)
        v1 = a1 * jnp.exp(-(g01 * a0 + g11 * a1) / scale)
        tot = v0 + v1
        return v0 / tot, v1 / tot

    half = jnp.full((1, 128), 0.5, F32)
    a0, a1 = lax.fori_loop(0, STEPS, eg_step, (half, half))
    lane = lax.broadcasted_iota(jnp.int32, (8, 128), 1)
    aw_ref[...] = jnp.where(lane == 0, a0, a1)

    b0 = jnp.concatenate([a0] * 6, axis=1)
    b1 = jnp.concatenate([a1] * 6, axis=1)
    for c in range(NCH):
        v = acc1[c, py, px, core]
        comb = b0[:, 0:CH] * v[:, 0:CH] + b1[:, 0:CH] * v[:, CH:2 * CH]
        for g in range(8):
            g1_ref[:, g * 96 + c * 32:g * 96 + c * 32 + 32] = comb[:, g * 32:g * 32 + 32]
        v = acc2[c, py, px, core]
        g2_ref[c * 32:(c + 1) * 32, :] = b0 * v[:, 0:D] + b1 * v[:, D:2 * D]

    for k in (1, 2, 3):
        e_copy(k).wait_send()
        n_copy(k).wait_send()
    for c in range(NCH):
        for cp in core_copies(c) + side_copies(c) + last_copies(c):
            cp.wait_send()
    for i in range(1, 8):
        m_copy(i).wait_send()


def backward(x, a, w2r, hcat, e):
    dma = pltpu.SemaphoreType.DMA
    anyspec = pl.BlockSpec(memory_space=pl.ANY)
    vspec = pl.BlockSpec(memory_space=pltpu.VMEM)
    return pl.pallas_call(
        backward_kernel,
        out_shape=(jax.ShapeDtypeStruct((8, 128), F32), jax.ShapeDtypeStruct((96, FL), F32),
                   jax.ShapeDtypeStruct((96, D), F32)),
        in_specs=[anyspec, anyspec, anyspec, vspec, vspec],
        out_specs=(vspec, vspec, vspec),
        scratch_shapes=[
            pltpu.VMEM((8, TB, 2 * D), BF),
            pltpu.VMEM((NCH, 2, 2, 2, 96, 2 * CH), F32),
            pltpu.VMEM((NCH, 2, 2, 2, 32, 2 * D), F32),
            pltpu.VMEM((NCH, 2, 2, 96, 2 * CH), F32),
            pltpu.VMEM((NCH, 2, 2, 32, 2 * D), F32),
            pltpu.VMEM((NCH, 2, 96, 2 * CH), F32),
            pltpu.VMEM((NCH, 2, 32, 2 * D), F32),
            pltpu.VMEM((NCH, 96, 2 * CH), F32),
            pltpu.VMEM((NCH, 32, 2 * D), F32),
            pltpu.VMEM((2, TB, CH), F32),
            pltpu.VMEM((2, TB, D), BF),
            pltpu.VMEM((TB, CH), BF),
            pltpu.VMEM((TB, 2 * CH), BF),
            pltpu.VMEM((4, ER, NOWN), F32),
            pltpu.VMEM((NCH, 8, 32, D), BF),
            pltpu.VMEM((3 * ER, 2 * D), BF),
            pltpu.VMEM((8, 8, 128), F32),
            pltpu.VMEM((4, 8, 128), F32),
            dma((4,)), dma((4,)), dma((NCH,)), dma((2,)), dma((2,)),
            dma((NCH, 2)), dma((NCH, 2)), dma((NCH, 2)), dma((NCH, 2)), dma((NCH, 2)), dma((NCH, 2)),
            dma((8,)), dma((8,)), dma((4,)), dma((4,)),
        ],
        compiler_params=pltpu.CompilerParams(
            collective_id=1, has_side_effects=True, vmem_limit_bytes=VMEM_BYTES),
        name='backward',
    )(x, a, w2r, hcat, e)


def solution(mesh):
    def local_step(tokens, w_up, w_down, task_heads, labels):
        heads = jnp.transpose(task_heads, (0, 2, 1)).reshape(2 * NC, D)
        hcat = jnp.pad(heads, ((0, ER - 2 * NC), (0, 0)))
        w2r = w_down.reshape(8, NCH, 32, D)
        a, e = forward(tokens, w_up, w2r, hcat, labels)
        weights, grad_up, grad_down = backward(tokens, a, w2r, hcat, e)
        return weights[0, 0:2], grad_up, grad_down

    return jax.shard_map(
        local_step, mesh=mesh,
        in_specs=(P('data', None), P(None, 'model'), P('model', None), P(None, None, None), P(None, 'data')),
        out_specs=(P(None), P('data', 'model'), P(('model', 'data'), None)),
        check_vma=False)
```

```python
import jax
import jax.numpy as jnp
from jax import lax
from jax.experimental import pallas as pl
from jax.experimental.pallas import tpu as pltpu
from jax.sharding import PartitionSpec as P

STEPS = 20
BF = jnp.bfloat16
F32 = jnp.float32
MESH = pl.DeviceIdType.MESH
VMEM_BYTES = 67043328

D = 768
FL = 768
NTOK = 8192
NOWN = 2048
TB = 1024
SUB = 256
NC = 19
ER = 40
CH = 256
NCH = 3
NG = 9
LAST = NCH - 1

G0 = 0.7978845608028654
G1C = 0.044715 * G0


def dot_nn(a, b):
    return lax.dot_general(a, b, (((1,), (0,)), ((), ())), preferred_element_type=F32)


def dot_nt(a, b):
    return lax.dot_general(a, b, (((1,), (1,)), ((), ())), preferred_element_type=F32)


def dot_tn(a, b):
    return lax.dot_general(a, b, (((0,), (0,)), ((), ())), preferred_element_type=F32)


def gelu(x):
    t = jnp.tanh(x * (G0 + G1C * (x * x)))
    h = 0.5 * x
    return h + h * t


def gelu_and_slope(x):
    x2 = x * x
    t = jnp.tanh(x * (G0 + G1C * x2))
    h = 0.5 * x
    u = h + h * t
    s = 0.5 + 0.5 * t + h * (1.0 - t * t) * (G0 + (3.0 * G1C) * x2)
    return u, s


class Place:
    def __init__(self):
        self.z = lax.axis_index('model')
        self.j = lax.axis_index('data')
        self.core = self.j % 2
        self.x = (self.j // 2) % 2
        self.y = self.j // 4
        self.jc = self.j + 1 - 2 * self.core
        self.jx = self.j + 2 - 4 * self.x
        self.jy = self.j + 4 - 8 * self.y
        self.jd = self.jx + 4 - 8 * self.y

    def zmate(self, k):
        return (self.z % 2 + k % 2) % 2 + 2 * ((self.z // 2 + k // 2) % 2)


def remote(src, dst, ssem, rsem, z, j):
    return pltpu.make_async_remote_copy(
        src_ref=src, dst_ref=dst, send_sem=ssem, recv_sem=rsem, device_id=(z, j), device_id_type=MESH)


class Scatter:
    def __init__(self, pos, acc, r1, r2, r3, lanes, sems, idx, x_first):
        self.pos, self.acc, self.r1, self.r2, self.r3 = pos, acc, r1, r2, r3
        self.lanes, self.sems, self.idx, self.x_first = lanes, sems, idx, x_first

    def copy(self, stage):
        p, ln = self.pos, self.lanes
        ssem, rsem = self.sems[0].at[self.idx, stage], self.sems[1].at[self.idx, stage]
        if stage == 0:
            return remote(self.acc.at[:, :, 1 - p.core, :, ln], self.r1.at[:, :, :, ln], ssem, rsem, p.z, p.jc)
        if stage == 1:
            if self.x_first:
                return remote(self.acc.at[:, 1 - p.x, p.core, :, ln], self.r2.at[:, :, ln], ssem, rsem, p.z, p.jx)
            return remote(self.acc.at[1 - p.y, :, p.core, :, ln], self.r2.at[:, :, ln], ssem, rsem, p.z, p.jy)
        if self.x_first:
            return remote(self.acc.at[1 - p.y, p.x, p.core, :, ln], self.r3.at[:, ln], ssem, rsem, p.z, p.jy)
        return remote(self.acc.at[p.y, 1 - p.x, p.core, :, ln], self.r3.at[:, ln], ssem, rsem, p.z, p.jx)

    def start(self):
        self.copy(0).start()

    def side(self):
        p, ln = self.pos, self.lanes
        self.copy(0).wait_recv()
        for yy in range(2):
            for xx in range(2):
                self.acc[yy, xx, p.core, :, ln] += self.r1[yy, xx, :, ln]
        self.copy(1).start()

    def last(self):
        p, ln = self.pos, self.lanes
        self.copy(1).wait_recv()
        for i in range(2):
            if self.x_first:
                self.acc[i, p.x, p.core, :, ln] += self.r2[i, :, ln]
            else:
                self.acc[p.y, i, p.core, :, ln] += self.r2[i, :, ln]
        self.copy(2).start()

    def done(self):
        p, ln = self.pos, self.lanes
        self.copy(2).wait_recv()
        self.acc[p.y, p.x, p.core, :, ln] += self.r3[:, ln]

    def drain(self):
        for stage in range(3):
            self.copy(stage).wait_send()


def main_kernel(x_hbm, w1_hbm, w2_hbm, heads_hbm, lab_hbm,
                a_hbm, sh1_hbm, sh2_hbm, aw_ref,
                dz, wown, acc1, acc2, r1a, r1b, r2a, r2b, r3a, r3b, eall, ast, hbd, hcat, heads, lab_v,
                gm, mbuf, nbuf,
                zss, zrs, xss, xrs, yss, yrs, dss, drs, css, crs,
                ld_sem, w2_sem, xs_sem, as_sem, ess, ers,
                rss, rsr, mss, mrs, nss, nrs, sh_sem):
    pos = Place()
    z, j = pos.z, pos.j

    barrier = pltpu.get_barrier_semaphore()
    for k in (1, 2, 3):
        pl.semaphore_signal(barrier, 1, device_id=(pos.zmate(k), j), device_id_type=MESH)
    for i in range(1, 8):
        pl.semaphore_signal(barrier, 1, device_id=(z, (j + i) % 8), device_id_type=MESH)

    w1_raw = dz.at[3, 0:D, 0:FL]
    w1_nat = dz.at[3, 0:D, FL:FL + CH]

    def xo_at(m):
        return dz.at[0, (m % 4) * SUB:(m % 4 + 1) * SUB, (m // 4) * D:(m // 4 + 1) * D]

    def us_at(m):
        return dz.at[2, (m % 4) * SUB:(m % 4 + 1) * SUB, D + (m // 4) * CH:D + (m // 4 + 1) * CH]

    own_row = pl.multiple_of(z * NOWN, NOWN)
    ld_w1 = pltpu.make_async_copy(w1_hbm, w1_raw, ld_sem.at[0])
    ld_x = [pltpu.make_async_copy(x_hbm.at[pl.ds(own_row + b * TB, TB)], dz.at[0, :, b * D:(b + 1) * D],
                                  ld_sem.at[1 + b]) for b in range(2)]
    ld_l = pltpu.make_async_copy(lab_hbm.at[:, pl.ds(own_row, NOWN)], lab_v, ld_sem.at[3])
    ld_h = pltpu.make_async_copy(heads_hbm, heads, ld_sem.at[4])
    ld_w2 = [pltpu.make_async_copy(w2_hbm.at[:, c], wown.at[c, :, :, D:2 * D], w2_sem.at[c]) for c in range(NCH)]

    def share_row(k, b):
        return pl.multiple_of((pos.zmate(k) * 2 + b) * TB, TB)

    def xs_load(i):
        half = dz.at[1, :, pl.ds(pl.multiple_of((i % 2) * D, D), D)]
        return pltpu.make_async_copy(x_hbm.at[pl.ds(share_row(1 + i // 2, i % 2), TB)], half, xs_sem.at[i % 2])

    ld_w1.start()
    for cp in ld_w2:
        cp.start()
    xs_load(0).start()
    for cp in ld_x:
        cp.start()
    ld_h.start()
    ld_l.start()

    ld_w1.wait()
    w1t = w1_raw[...].T
    for c in range(NCH):
        for g in range(8):
            wown[c, g, :, 0:D] = w1t[g * 96 + c * 32:g * 96 + c * 32 + 32, :]
    acc1[...] = jnp.zeros_like(acc1)
    acc2[...] = jnp.zeros_like(acc2)
    gm[...] = jnp.zeros_like(gm)
    for cp in ld_w2:
        cp.wait()
    pl.semaphore_wait(barrier, 10)

    def piece(i, jj):
        row = pl.multiple_of((i % NCH) * CH + jj * 32, 32)
        return dz.at[5 + i // NCH, pl.ds(row, 32), :]

    def z_copy(i):
        return remote(wown.at[i % NCH, j], piece(i, j), zss.at[i], zrs.at[i], pos.zmate(1 + i // NCH), j)

    def x_copy(i):
        return remote(piece(i, j), piece(i, j), xss.at[i], xrs.at[i], z, pos.jx)

    def y_copy(i):
        return remote(piece(i, j), piece(i, j), yss.at[i], yrs.at[i], z, pos.jy)

    def diag_copy_y(i):
        return remote(piece(i, pos.jx), piece(i, pos.jx), dss.at[i], drs.at[i], z, pos.jy)

    def diag_copy_x(i):
        return remote(piece(i, pos.jy), piece(i, pos.jy), dss.at[i], drs.at[i], z, pos.jx)

    def core_copy(i, q):
        jj = (j, pos.jx, pos.jy, pos.jd)[q]
        return remote(piece(i, jj), piece(i, jj), css.at[i, q], crs.at[i, q], z, pos.jc)

    def send_own(i):
        z_copy(i).wait_recv()
        x_copy(i).start()
        y_copy(i).start()
        core_copy(i, 0).start()

    def send_side(i):
        x_copy(i).wait_recv()

        @pl.when(pos.core == 0)
        def _():
            diag_copy_y(i).start()

        core_copy(i, 1).start()
        y_copy(i).wait_recv()

        @pl.when(pos.core == 1)
        def _():
            diag_copy_x(i).start()

        core_copy(i, 2).start()

    def send_diag(i):
        diag_copy_y(i).wait_recv()
        core_copy(i, 3).start()

    def start_z(i, carry):
        z_copy(i).start()
        return carry

    lax.fori_loop(0, NG, start_z, 0)

    def a_store(c, row):
        return pltpu.make_async_copy(
            ast.at[c], a_hbm.at[c, pl.ds(pl.multiple_of(row, TB), TB)], as_sem.at[c])

    def other_tokens(i, carry):
        xs_load(i).wait()

        @pl.when(i < 5)
        def _():
            xs_load(i + 1).start()

        xs = dz.at[1, :, pl.ds(pl.multiple_of((i % 2) * D, D), D)]
        for c in range(NCH):
            @pl.when(i >= 1)
            def _():
                a_store(c, 0).wait()

            ast[c] = dot_nt(xs[...], wown[c, :, :, 0:D].reshape(CH, D))
            a_store(c, share_row(1 + i // 2, i % 2)).start()

        @pl.when(i == 2)
        def _():
            send_own(0)

        @pl.when(i == 3)
        def _():
            send_own(1)

        @pl.when(i == 5)
        def _():
            send_side(0)
            send_own(2)

        return carry

    lax.fori_loop(0, 6, other_tokens, 0)
    for cp in ld_x:
        cp.wait()

    def forward(facc):
        for b in range(2):
            for c in range(NCH):
                a_store(c, 0).wait()
            for m in range(4):
                rows = slice(m * SUB, (m + 1) * SUB)
                for c in range(NCH):
                    a = dot_nt(xo_at(b * 4 + m)[...], wown[c, :, :, 0:D].reshape(CH, D))
                    ast[c, rows, :] = a
                    dz[2, rows, c * CH:(c + 1) * CH] = gelu(a).astype(BF)
            for m in range(4):
                rows = slice(m * SUB, (m + 1) * SUB)
                facc[b * TB + m * SUB:b * TB + (m + 1) * SUB, :] = dot_nn(
                    dz[2, rows, 0:FL], wown[:, :, :, D:2 * D].reshape(FL, D))
            for c in range(NCH):
                a_store(c, (z * 2 + b) * TB).start()
            if b == 0:
                send_diag(0)
                send_side(1)
                send_own(3)

        def granule(n, carry):
            for q in range(4):
                core_copy(n, q).wait_recv()
            gran = dz.at[5 + n // NCH, pl.ds(pl.multiple_of((n % NCH) * CH, CH), CH), :]
            w1_nat[...] = gran[:, 0:D].T
            for m in range(8):
                us_at(m)[...] = gelu(dot_nn(xo_at(m)[...], w1_nat[...])).astype(BF)
            for m in range(8):
                facc[m * SUB:(m + 1) * SUB, :] += dot_nn(us_at(m)[...], gran[:, D:2 * D])

            @pl.when(n + 1 < NG)
            def _():
                send_diag(n + 1)

            @pl.when(n + 2 < NG)
            def _():
                send_side(n + 2)

            @pl.when(n + 4 < NG)
            def _():
                send_own(n + 4)

            return carry

        lax.fori_loop(0, NG, granule, 0)

        for m in range(8):
            us = (xo_at(m)[...].astype(F32) + facc[m * SUB:(m + 1) * SUB, :]).astype(BF)
            xo_at(m)[...] = us

    ld_h.wait()
    r40 = lax.broadcasted_iota(jnp.int32, (ER, NC), 0)
    c19 = lax.broadcasted_iota(jnp.int32, (ER, NC), 1)
    hc = (dot_nt(jnp.where(r40 == c19, 1.0, 0.0).astype(BF), heads[0])
          + dot_nt(jnp.where(r40 == c19 + NC, 1.0, 0.0).astype(BF), heads[1]))
    hcat[...] = hc.astype(BF)
    r = lax.broadcasted_iota(jnp.int32, (ER, D), 0)
    hb = jnp.concatenate([jnp.where(r < NC, hc, 0.0), jnp.where(r >= NC, hc, 0.0)], axis=1)
    hbd[...] = jnp.concatenate([hb, hb, hb], axis=0).astype(BF)

    pl.run_scoped(forward, pltpu.VMEM((NOWN, D), F32))

    ld_l.wait()
    r = lax.broadcasted_iota(jnp.int32, (ER, TB), 0)
    first = r < NC
    real = r < 2 * NC
    second = jnp.logical_and(r >= NC, real)
    neg = jnp.float32(-jnp.inf)
    for b in range(2):
        cols = slice(b * TB, (b + 1) * TB)
        logit = dot_nt(hcat[...], dz[0, :, b * D:(b + 1) * D])
        m0 = jnp.max(jnp.where(first, logit, neg), axis=0, keepdims=True)
        m1 = jnp.max(jnp.where(second, logit, neg), axis=0, keepdims=True)
        ex = jnp.where(real, jnp.exp(logit - jnp.where(first, m0, m1)), 0.0)
        s0 = jnp.sum(jnp.where(first, ex, 0.0), axis=0, keepdims=True)
        s1 = jnp.sum(jnp.where(second, ex, 0.0), axis=0, keepdims=True)
        prob = ex / jnp.where(first, s0, s1)
        lab = jnp.where(first, lab_v[0:1, cols], lab_v[1:2, cols] + NC)
        eall[0, :, cols] = (prob - jnp.where(r == lab, 1.0, 0.0)) / (NTOK * 8.0)

    def e_copy(k):
        return remote(eall.at[0], eall.at[k], ess.at[k], ers.at[k], pos.zmate(k), j)

    for k in (1, 2, 3):
        e_copy(k).start()
    for c in range(NCH):
        a_store(c, 0).wait()

    def drain(i, carry):
        z_copy(i).wait_send()
        x_copy(i).wait_send()
        y_copy(i).wait_send()
        diag_copy_y(i).wait_send()
        for q in range(4):
            core_copy(i, q).wait_send()
        return carry

    lax.fori_loop(0, NG, drain, 0)

    everything = slice(None)
    sems = (rss, rsr)

    def up(c, t):
        return Scatter(pos, acc1.at[c, t], r1a.at[c, t], r2a.at[c, t], r3a.at[c, t], everything, sems,
                       c * 6 + t, t == 0)

    def down(c, t, part=None):
        if part is None:
            lanes, idx, x_first = everything, c * 6 + 2 + t, t == 0
        else:
            lanes, idx, x_first = slice(part * (D // 2), (part + 1) * (D // 2)), c * 6 + 2 + t * 2 + part, part == 0
        return Scatter(pos, acc2.at[c, t], r1b.at[c, t], r2b.at[c, t], r3b.at[c, t], lanes, sems, idx, x_first)

    def whole(c):
        return [up(c, 0), down(c, 1), up(c, 1), down(c, 0)]

    up_last = [up(LAST, 0), up(LAST, 1)]
    down_last = [[down(LAST, t, part) for part in range(2)] for t in range(2)]

    def fold(v):
        rows, cols = v.shape
        total = jnp.zeros((8, 128), F32)
        for q in range(cols // 128):
            total = total + jnp.sum(v[:, q * 128:(q + 1) * 128].reshape(rows // 8, 8, 128), axis=0)
        return total

    def shard(acc, c, t):
        return acc.at[c, t, pos.y, pos.x, pos.core]

    def finish(acc, out, c, sem):
        v0, v1 = shard(acc, c, 0)[...], shard(acc, c, 1)[...]
        gm[0] += fold(v0 * v0)
        gm[1] += fold(v0 * v1)
        gm[2] += fold(v1 * v1)
        for t in range(2):
            pltpu.make_async_copy(shard(acc, c, t), out.at[c, t], sh_sem.at[c, sem, t]).start()

    def backward(xbuf, us_all, das):
        def step_of(s):
            c = jnp.where(s < 8, (s // 2) % 2, jnp.where(s < 16, (s - 8) // 4, 2))
            k = jnp.where(s < 8, s // 4, jnp.where(s < 16, 2 + (s % 4) // 2, (s - 16) // 2))
            return c, k, s % 2

        def a_load(s):
            c, k, b = step_of(s)
            return pltpu.make_async_copy(a_hbm.at[c, pl.ds(share_row(k, b), TB)], ast.at[s % 2], as_sem.at[s % 2])

        def x_load(s):
            c, k, b = step_of(s)
            return pltpu.make_async_copy(x_hbm.at[pl.ds(share_row(k, b), TB)], xbuf.at[s % 2], xs_sem.at[s % 2])

        a_load(0).start()
        x_load(0).start()

        def prepare(s):
            c, k, b = step_of(s)
            a_load(s).wait()
            x_load(s).wait()

            @pl.when(s < 23)
            def _():
                a_load(s + 1).start()
                x_load(s + 1).start()

        def d_act(s, t, us):
            c, _, _ = step_of(s)
            w2c = wown[c, :, :, D:2 * D].reshape(CH, D)
            for m in range(TB // SUB):
                rows = slice(m * SUB, (m + 1) * SUB)
                u, slope = gelu_and_slope(ast[s % 2, rows, :])
                us[rows, :] = u.astype(BF)
                for task in range(2):
                    da = dot_nt(dz[t, rows, task * D:(task + 1) * D], w2c)
                    das[rows, task * CH:(task + 1) * CH] = (da * slope).astype(BF)

        def add_up(s, c):
            g = dot_tn(xbuf[s % 2], das[...])
            for task in range(2):
                acc1[c, task] += g[:, task * CH:(task + 1) * CH].reshape(2, 2, 2, 96, CH)

        def add_down(t, c, us):
            g = dot_tn(us[...], dz[t])
            for task in range(2):
                acc2[c, task] += g[:, task * D:(task + 1) * D].reshape(2, 2, 2, 32, D)

        def step(s, carry):
            c, k, b = step_of(s)
            t = k * 2 + b
            prepare(s)

            @pl.when(c == 0)
            def _():
                @pl.when(jnp.logical_and(b == 0, k > 0))
                def _():
                    e_copy(k).wait_recv()

                e = eall[k, :, pl.ds(pl.multiple_of(b * TB, TB), TB)]
                e1 = e.astype(BF).astype(F32)
                rest = e - e1
                e2 = rest.astype(BF).astype(F32)
                e3 = rest - e2
                es = jnp.concatenate([e1, e2, e3], axis=0).astype(BF)
                dz[t] = dot_tn(es, hbd[...]).astype(BF)

            us = us_all.at[0]
            d_act(s, t, us)
            add_down(t, c, us)
            add_up(s, c)

            @pl.when(s == 11)
            def _():
                for sc in whole(0):
                    sc.start()

            @pl.when(s == 12)
            def _():
                for sc in whole(0):
                    sc.side()

            @pl.when(s == 15)
            def _():
                for sc in whole(1):
                    sc.start()

            return carry

        lax.fori_loop(0, 16, step, 0)

        def last_step(s, carry):
            c, k, b = step_of(s)
            t = k * 2 + b
            prepare(s)
            d_act(s, t, us_all.at[t])
            add_up(s, c)

            @pl.when(s == 16)
            def _():
                for sc in whole(0):
                    sc.last()
                for sc in whole(1):
                    sc.side()

            @pl.when(s == 19)
            def _():
                for sc in whole(0):
                    sc.done()
                finish(acc1, sh1_hbm, 0, 0)
                finish(acc2, sh2_hbm, 0, 1)

            @pl.when(s == 21)
            def _():
                for sc in whole(1):
                    sc.last()

            return carry

        lax.fori_loop(16, 24, last_step, 0)
        for sc in up_last:
            sc.start()

        def down_pass(task):
            def two_blocks(i, carry):
                g = dot_tn(us_all[i * 2], dz[i * 2, :, task * D:(task + 1) * D])
                g = g + dot_tn(us_all[i * 2 + 1], dz[i * 2 + 1, :, task * D:(task + 1) * D])
                acc2[LAST, task] += g.reshape(2, 2, 2, 32, D)

                @pl.when(i == 1)
                def _():
                    if task == 0:
                        for sc in up_last:
                            sc.side()
                    else:
                        for sc in down_last[0]:
                            sc.side()

                return carry

            lax.fori_loop(0, 4, two_blocks, 0)
            for sc in down_last[task]:
                sc.start()

        down_pass(0)
        for sc in whole(1):
            sc.done()
        finish(acc1, sh1_hbm, 1, 0)
        finish(acc2, sh2_hbm, 1, 1)
        down_pass(1)

    pl.run_scoped(backward, pltpu.VMEM((2, TB, D), BF), pltpu.VMEM((8, TB, CH), BF), pltpu.VMEM((TB, 2 * CH), BF))

    for sc in up_last:
        sc.last()
    for sc in down_last[1]:
        sc.side()
    for sc in down_last[0]:
        sc.last()
    for sc in up_last:
        sc.done()
    finish(acc1, sh1_hbm, LAST, 0)
    for sc in down_last[1]:
        sc.last()
    for sc in down_last[0]:
        sc.done()
    for sc in down_last[1]:
        sc.done()
    finish(acc2, sh2_hbm, LAST, 1)

    def full(v):
        return jnp.sum(jnp.sum(v, axis=0, keepdims=True), axis=1, keepdims=True)

    row = lax.broadcasted_iota(jnp.int32, (8, 128), 0)
    mbuf[j] = jnp.where(row == 0, full(gm[0]), jnp.where(row == 1, full(gm[1]), full(gm[2])))

    def m_copy(i):
        return remote(mbuf.at[j], mbuf.at[j], mss.at[i], mrs.at[i], z, (j + i) % 8)

    for i in range(1, 8):
        m_copy(i).start()
    for i in range(1, 8):
        m_copy(i).wait_recv()
    total = mbuf[0]
    for i in range(1, 8):
        total = total + mbuf[i]
    nbuf[z] = total

    def n_copy(k):
        return remote(nbuf.at[z], nbuf.at[z], nss.at[k], nrs.at[k], pos.zmate(k), j)

    for k in (1, 2, 3):
        n_copy(k).start()

    for k in (1, 2, 3):
        e_copy(k).wait_send()
    for sc in whole(0) + whole(1) + up_last + down_last[0] + down_last[1]:
        sc.drain()
    for i in range(1, 8):
        m_copy(i).wait_send()
    for c in range(NCH):
        for t in range(2):
            pltpu.make_async_copy(shard(acc1, c, t), sh1_hbm.at[c, t], sh_sem.at[c, 0, t]).wait()
            pltpu.make_async_copy(shard(acc2, c, t), sh2_hbm.at[c, t], sh_sem.at[c, 1, t]).wait()

    for k in (1, 2, 3):
        n_copy(k).wait_recv()
    gram = nbuf[0]
    for k in (1, 2, 3):
        gram = gram + nbuf[k]
    g00, g01, g11 = gram[0:1, :], gram[1:2, :], gram[2:3, :]
    scale = (g00 + g11) / 2.0

    def eg_step(i, weights):
        a0, a1 = weights
        v0 = a0 * jnp.exp(-(g00 * a0 + g01 * a1) / scale)
        v1 = a1 * jnp.exp(-(g01 * a0 + g11 * a1) / scale)
        tot = v0 + v1
        return v0 / tot, v1 / tot

    half = jnp.full((1, 128), 0.5, F32)
    a0, a1 = lax.fori_loop(0, STEPS, eg_step, (half, half))
    aw_ref[...] = jnp.where(row == 0, a0, a1)
    for k in (1, 2, 3):
        n_copy(k).wait_send()


def main_call(x, w1, w2r, heads, labels):
    dma = pltpu.SemaphoreType.DMA
    anyspec = pl.BlockSpec(memory_space=pl.ANY)
    vspec = pl.BlockSpec(memory_space=pltpu.VMEM)
    return pl.pallas_call(
        main_kernel,
        out_shape=(jax.ShapeDtypeStruct((NCH, NTOK, CH), F32),
                   jax.ShapeDtypeStruct((NCH, 2, 96, CH), F32),
                   jax.ShapeDtypeStruct((NCH, 2, 32, D), F32),
                   jax.ShapeDtypeStruct((8, 128), F32)),
        in_specs=[anyspec] * 5,
        out_specs=(anyspec, anyspec, anyspec, vspec),
        scratch_shapes=[
            pltpu.VMEM((8, TB, 2 * D), BF),
            pltpu.VMEM((NCH, 8, 32, 2 * D), BF),
            pltpu.VMEM((NCH, 2, 2, 2, 2, 96, CH), F32),
            pltpu.VMEM((NCH, 2, 2, 2, 2, 32, D), F32),
            pltpu.VMEM((NCH, 2, 2, 2, 96, CH), F32),
            pltpu.VMEM((NCH, 2, 2, 2, 32, D), F32),
            pltpu.VMEM((NCH, 2, 2, 96, CH), F32),
            pltpu.VMEM((NCH, 2, 2, 32, D), F32),
            pltpu.VMEM((NCH, 2, 96, CH), F32),
            pltpu.VMEM((NCH, 2, 32, D), F32),
            pltpu.VMEM((4, ER, NOWN), F32),
            pltpu.VMEM((NCH, TB, CH), F32),
            pltpu.VMEM((3 * ER, 2 * D), BF),
            pltpu.VMEM((ER, D), BF),
            pltpu.VMEM((2, D, NC), BF),
            pltpu.VMEM((2, NOWN), jnp.int32),
            pltpu.VMEM((3, 8, 128), F32),
            pltpu.VMEM((8, 8, 128), F32),
            pltpu.VMEM((4, 8, 128), F32),
            dma((NG,)), dma((NG,)), dma((NG,)), dma((NG,)), dma((NG,)), dma((NG,)),
            dma((NG,)), dma((NG,)), dma((NG, 4)), dma((NG, 4)),
            dma((5,)), dma((NCH,)), dma((2,)), dma((NCH,)), dma((4,)), dma((4,)),
            dma((6 * NCH, 3)), dma((6 * NCH, 3)), dma((8,)), dma((8,)), dma((4,)), dma((4,)), dma((NCH, 2, 2)),
        ],
        compiler_params=pltpu.CompilerParams(
            collective_id=0, has_side_effects=True, vmem_limit_bytes=VMEM_BYTES),
        name='main',
    )(x, w1, w2r, heads, labels)


def result_kernel(aw_ref, sh1, sh2, a_ref, g1_ref, g2_ref):
    a0, a1 = aw_ref[0:1, :], aw_ref[1:2, :]
    a_ref[0] = aw_ref[0, 0]
    a_ref[1] = aw_ref[1, 0]
    b0 = jnp.concatenate([a0] * 6, axis=1)
    b1 = jnp.concatenate([a1] * 6, axis=1)
    for c in range(NCH):
        comb = b0[:, 0:CH] * sh1[c, 0] + b1[:, 0:CH] * sh1[c, 1]
        for g in range(8):
            g1_ref[:, g * 96 + c * 32:g * 96 + c * 32 + 32] = comb[:, g * 32:g * 32 + 32]
        g2_ref[c * 32:(c + 1) * 32, :] = b0 * sh2[c, 0] + b1 * sh2[c, 1]


def result_call(aw, sh1, sh2):
    vspec = pl.BlockSpec(memory_space=pltpu.VMEM)
    return pl.pallas_call(
        result_kernel,
        out_shape=(jax.ShapeDtypeStruct((2,), F32), jax.ShapeDtypeStruct((96, FL), F32),
                   jax.ShapeDtypeStruct((96, D), F32)),
        in_specs=[vspec] * 3,
        out_specs=(pl.BlockSpec(memory_space=pltpu.SMEM), vspec, vspec),
        name='result',
    )(aw, sh1, sh2)


def solution(mesh):
    def local_step(tokens, w_up, w_down, task_heads, labels):
        w2r = w_down.reshape(8, NCH, 32, D)
        _, sh1, sh2, aw = main_call(tokens, w_up, w2r, task_heads, labels)
        return result_call(aw, sh1, sh2)

    return jax.shard_map(
        local_step, mesh=mesh,
        in_specs=(P('data', None), P(None, 'model'), P('model', None), P(None, None, None), P(None, 'data')),
        out_specs=(P(None), P('data', 'model'), P(('model', 'data'), None)),
        check_vma=False)
```

```python
import jax
import jax.numpy as jnp
from jax import lax
from jax.experimental import pallas as pl
from jax.experimental.pallas import tpu as pltpu
from jax.sharding import PartitionSpec as P

STEPS = 20
BF = jnp.bfloat16
F32 = jnp.float32
MESH = pl.DeviceIdType.MESH
VMEM_BYTES = 67043328

D = 768
DD = D + D
NTOK = 8192
NOWN = 2048
TB = 1024
SUB = 256
NC = 19
ER = 40
CH = 256
NCH = 3
LAST = NCH - 1
NG = NCH * NCH
FAR = NG - NCH
GR = 32
OWN = CH // GR * 12
LO = slice(D)
HI = slice(D, DD)
SIDES = (LO, HI)
TWO = range(2)
MATES = range(1, 8)
LINE = range(1, 4)
BLOCKS = range(TB // SUB)
NDEV = 32

G0 = 0.7978845608028654
G1C = 0.044715 * G0


def dot_nn(a, b):
    return lax.dot_general(a, b, (((1,), (0,)), ((), ())), preferred_element_type=F32)


def dot_nt(a, b):
    return lax.dot_general(a, b, (((1,), (1,)), ((), ())), preferred_element_type=F32)


def dot_tn(a, b):
    return lax.dot_general(a, b, (((0,), (0,)), ((), ())), preferred_element_type=F32)


def gelu(x):
    t = jnp.tanh(x * (G0 + G1C * (x * x)))
    h = 0.5 * x
    return h + h * t


def gelu_and_slope(x):
    x2 = x * x
    t = jnp.tanh(x * (G0 + G1C * x2))
    h = 0.5 * x
    u = h + h * t
    s = 0.5 + 0.5 * t + h * (1.0 - t * t) * (G0 + (3.0 * G1C) * x2)
    return u, s


class Place:
    def __init__(self):
        self.z = lax.axis_index('model')
        self.j = lax.axis_index('data')
        self.core = self.j % 2
        self.x = (self.j // 2) % 2
        self.y = self.j // 4
        self.jc = self.j + 1 - 2 * self.core
        self.jx = self.j + 2 - 4 * self.x
        self.jy = self.j + 4 - 8 * self.y
        self.jd = self.jx + 4 - 8 * self.y
        self.js = self.jx + self.core * (self.jy - self.jx)
        self.j2 = self.jx + self.jy - self.js

        self.inner = self.z % 3 > 0
        self.pair = self.z + 1 - 2 * (self.z % 2)
        self.mirror = 3 - self.z
        half = self.z // 2
        self.shares = (self.z, self.pair, 2 - half, 3 - 3 * half)

    def share(self, k):
        own, near, far, end = self.shares
        return jnp.where(k == 0, own, jnp.where(k == 1, near, jnp.where(k == 2, far, end)))


def remote(src, dst, ssem, rsem, z, j):
    return pltpu.make_async_remote_copy(
        src_ref=src, dst_ref=dst, send_sem=ssem, recv_sem=rsem, device_id=(z, j), device_id_type=MESH)


class Scatter:
    def __init__(self, pos, acc, r1, r2, r3, lanes, sems, idx, x_first):
        self.pos, self.acc, self.r1, self.r2, self.r3 = pos, acc, r1, r2, r3
        self.lanes, self.sems, self.idx, self.x_first = lanes, sems, idx, x_first

    def copy(self, stage):
        p, ln = self.pos, self.lanes
        ssem, rsem = self.sems[0].at[self.idx, stage], self.sems[1].at[self.idx, stage]
        if stage == 0:
            return remote(self.acc.at[:, :, 1 - p.core, :, ln], self.r1.at[:, :, :, ln], ssem, rsem, p.z, p.jc)
        if stage == 1:
            if self.x_first:
                return remote(self.acc.at[:, 1 - p.x, p.core, :, ln], self.r2.at[:, :, ln], ssem, rsem, p.z, p.jx)
            return remote(self.acc.at[1 - p.y, :, p.core, :, ln], self.r2.at[:, :, ln], ssem, rsem, p.z, p.jy)
        if self.x_first:
            return remote(self.acc.at[1 - p.y, p.x, p.core, :, ln], self.r3.at[:, ln], ssem, rsem, p.z, p.jy)
        return remote(self.acc.at[p.y, 1 - p.x, p.core, :, ln], self.r3.at[:, ln], ssem, rsem, p.z, p.jx)

    def start(self):
        self.copy(0).start()

    def side(self):
        p, ln = self.pos, self.lanes
        self.copy(0).wait_recv()
        for yy in TWO:
            for xx in TWO:
                self.acc[yy, xx, p.core, :, ln] += self.r1[yy, xx, :, ln]
        self.copy(1).start()

    def last(self):
        p, ln = self.pos, self.lanes
        self.copy(1).wait_recv()
        for i in TWO:
            if self.x_first:
                self.acc[i, p.x, p.core, :, ln] += self.r2[i, :, ln]
            else:
                self.acc[p.y, i, p.core, :, ln] += self.r2[i, :, ln]
        self.copy(2).start()

    def done(self):
        p, ln = self.pos, self.lanes
        self.copy(2).wait_recv()
        self.acc[p.y, p.x, p.core, :, ln] += self.r3[:, ln]

    def drain(self):
        for stage in range(3):
            self.copy(stage).wait_send()


def main_kernel(x_hbm, w1_hbm, w2_hbm, heads_hbm, lab_hbm,
                a_hbm, sh1_hbm, sh2_hbm, aw_ref,
                dz, wown, acc1, acc2, r1a, r1b, r2a, r2b, r3a, r3b, eall, ast, xbuf, hbd, hcat, heads, lab_v,
                gm, mbuf,
                zss, zfs, zrs, zgs, zqs, xss, xrs, yss, yrs, dss, drs, css, crs,
                ld_sem, w2_sem, xs_sem, as_sem, ess, efs, ers,
                rss, rsr, mss, mrs, sh_sem):
    pos = Place()
    z, j, inner = pos.z, pos.j, pos.inner
    outer = jnp.logical_not(inner)

    barrier = pltpu.get_barrier_semaphore()
    me = z * 8 + j

    def greet(i, carry):
        to = (me + i) % NDEV
        pl.semaphore_signal(barrier, device_id=(to // 8, to % 8), device_id_type=MESH)
        return carry

    lax.fori_loop(1, NDEV, greet, 0)

    own_x, act, room = dz.at[0], dz.at[2], dz.at[3]
    w1_raw = room.at[LO, LO]
    w1_nat = room.at[LO, D:D + CH]
    w1_own = dz.at[4, LO, HI]

    def sub(m):
        return slice((m % 4) * SUB, (m % 4 + 1) * SUB)

    def xo_at(m):
        return own_x.at[sub(m), HI if m >= 4 else LO]

    def us_at(m):
        lane = D + (m // 4) * CH
        return act.at[sub(m), lane:lane + CH]

    def share_row(k, b):
        return pl.multiple_of((pos.share(k) * 2 + b) * TB, TB)

    own_row = pl.multiple_of(z * NOWN, NOWN)
    ld_w1 = pltpu.make_async_copy(w1_hbm, w1_raw, ld_sem.at[0])
    ld_x = [pltpu.make_async_copy(x_hbm.at[pl.ds(own_row + b * TB, TB)], own_x.at[:, SIDES[b]], ld_sem.at[1 + b])
            for b in TWO]
    ld_l = pltpu.make_async_copy(lab_hbm.at[:, pl.ds(own_row, NOWN)], lab_v, ld_sem.at[3])
    ld_h = pltpu.make_async_copy(heads_hbm, heads, ld_sem.at[4])
    ld_w2 = [pltpu.make_async_copy(w2_hbm.at[:, c], wown.at[c, :, :, HI], w2_sem.at[c]) for c in range(NCH)]

    def stream_half(i):
        return dz.at[1 + 3 * (i % 2), :, LO]

    def xs_load(i):
        return pltpu.make_async_copy(
            x_hbm.at[pl.ds(share_row(1 + i // 2, i % 2), TB)], stream_half(i), xs_sem.at[i % 2])

    ld_w1.start()
    for cp in ld_w2:
        cp.start()
    xs_load(0).start()
    for cp in ld_x:
        cp.start()
    ld_h.start()
    ld_l.start()

    ld_w1.wait()
    w1t = w1_raw[...].T
    for c in range(NCH):
        for g in range(8):
            row = g * NCH * GR + c * GR
            wown[c, g, :, LO] = w1t[row:row + GR, :]
    for cp in ld_w2:
        cp.wait()
    pl.semaphore_wait(barrier, NDEV - 1)

    def piece(i, jj):
        row = pl.multiple_of((i % NCH) * CH + jj * GR, GR)
        return dz.at[5 + i // NCH, pl.ds(row, GR), :]

    def z_pair(c):
        return remote(wown.at[c, j], piece(c, j), zss.at[c], zrs.at[c], pos.pair, j)

    def z_mirror(c):
        return remote(wown.at[c, j], piece(NCH + c, j), zss.at[NCH + c], zrs.at[NCH + c], pos.mirror, j)

    def z_forward(i):
        first = i < NCH
        to = jnp.where(first, i + 2 * NCH, i)
        return remote(piece(i, j), piece(to, j), zfs.at[i], zrs.at[to], jnp.where(first, pos.mirror, pos.pair), j)

    def more_forward(i):
        first = i < NCH
        to = jnp.where(first, i + 2 * NCH, i)
        return remote(piece(i, pos.j2), piece(to, pos.j2), zgs.at[i], zqs.at[to], jnp.where(first, pos.mirror, pos.pair), j)

    def side_copy(i):
        return remote(piece(i, j), piece(i, j), xss.at[i], xrs.at[i], z, pos.js)

    def more_copy(i):
        return remote(piece(i, pos.j2), piece(i, pos.j2), dss.at[i], drs.at[i], z, pos.js)

    def x_copy(i):
        return remote(piece(i, j), piece(i, j), xss.at[i], xrs.at[i], z, pos.jx)

    def y_copy(i):
        return remote(piece(i, j), piece(i, j), yss.at[i], yrs.at[i], z, pos.jy)

    def diag_copy_y(i):
        return remote(piece(i, pos.jx), piece(i, pos.jx), dss.at[i], drs.at[i], z, pos.jy)

    def diag_copy_x(i):
        return remote(piece(i, pos.jy), piece(i, pos.jy), dss.at[i], drs.at[i], z, pos.jx)

    def core_copy(i, q):
        jj = (j, pos.jx, pos.jy, pos.jd)[q]
        return remote(piece(i, jj), piece(i, jj), css.at[i, q], crs.at[i, q], z, pos.jc)

    def core_side(i, q):
        jj = (j, pos.js, pos.j2, pos.jd)[q]
        return remote(piece(i, jj), piece(i, jj), css.at[i, q], crs.at[i, q], z, pos.jc)

    def take(i):
        remote(piece(i, j), piece(i, j), zfs.at[i], zrs.at[i], pos.pair, j).wait_recv()

        @pl.when(inner)
        def _():
            z_forward(i).start()

    def take_both(i):
        remote(piece(i, j), piece(i, j), zfs.at[i], zrs.at[i], pos.pair, j).wait_recv()
        remote(piece(i, j), piece(i, j), zgs.at[i], zqs.at[i], pos.pair, j).wait_recv()

        @pl.when(inner)
        def _():
            z_forward(i).start()
            more_forward(i).start()

    def send_both(i):
        side_copy(i).start()
        more_copy(i).start()
        core_side(i, 0).start()
        core_side(i, 2).start()

    def pass_both(i):
        side_copy(i).wait_recv()
        core_side(i, 1).start()
        more_copy(i).wait_recv()
        core_side(i, 3).start()

    def take_if(cond, i):
        @pl.when(cond)
        def _():
            take(i)

    def send_own(i):
        x_copy(i).start()
        y_copy(i).start()
        core_copy(i, 0).start()

    def send_side(i):
        x_copy(i).wait_recv()

        @pl.when(pos.core == 0)
        def _():
            diag_copy_y(i).start()

        core_copy(i, 1).start()
        y_copy(i).wait_recv()

        @pl.when(pos.core == 1)
        def _():
            diag_copy_x(i).start()

        core_copy(i, 2).start()

    def more_on(i):
        @pl.when(inner)
        def _():
            more_forward(i).start()

    def send_diag(i):
        diag_copy_y(i).wait_recv()
        core_copy(i, 3).start()

    for c in range(NCH):
        z_pair(c).start()

    @pl.when(inner)
    def _():
        for c in range(NCH):
            z_mirror(c).start()

    def a_store(src, c, row, sem):
        return pltpu.make_async_copy(src, a_hbm.at[c, pl.ds(pl.multiple_of(row, TB), TB)], as_sem.at[sem])

    def forward(facc):
        for c in range(NCH):
            w1_own[:, c * CH:(c + 1) * CH] = wown[c, :, :, LO].reshape(CH, D).T

        def staged(i, c):
            rows = pl.ds(pl.multiple_of((i % 2) * TB, TB), TB)
            return a_store(facc.at[rows, c * CH:(c + 1) * CH], c, share_row(1 + i // 2, i % 2), (i % 2) * NCH + c)

        def other_tokens(i, carry):
            xs_load(i).wait()

            @pl.when(i < 5)
            def _():
                xs_load(i + 1).start()

            @pl.when(i >= 2)
            def _():
                for c in range(NCH):
                    staged(i, c).wait()

            base = (i % 2) * TB
            for m in BLOCKS:
                rows = pl.ds(pl.multiple_of(base + m * SUB, SUB), SUB)
                facc[rows, :] = dot_nn(stream_half(i)[sub(m), :], w1_own[...])
            for c in range(NCH):
                staged(i, c).start()

            @pl.when(i == 2)
            def _():
                take(0)
                send_own(0)
                take_if(inner, 3)

            @pl.when(i == 3)
            def _():
                take(1)
                send_own(1)
                take_if(inner, 4)

            @pl.when(i == 4)
            def _():
                take_if(inner, 5)

            @pl.when(i == 5)
            def _():
                take(2)
                send_own(2)
                send_side(0)
                more_on(0)

            return carry

        lax.fori_loop(0, 6, other_tokens, 0)
        for cp in ld_x:
            cp.wait()

        for b in TWO:
            for c in range(NCH):
                staged(b, c).wait()
            for m in BLOCKS:
                a = dot_nn(xo_at(b * 4 + m)[...], w1_own[...])
                for c in range(NCH):
                    ast[c, sub(m), :] = a[:, c * CH:(c + 1) * CH]
                act[sub(m), LO] = gelu(a).astype(BF)
            for m in BLOCKS:
                facc[b * TB + m * SUB:b * TB + (m + 1) * SUB, :] = dot_nn(
                    act[sub(m), LO], wown[:, :, :, HI].reshape(D, D))
            for c in range(NCH):
                a_store(ast.at[c], c, (z * 2 + b) * TB, c).start()
            if b == 0:
                send_side(1)
                more_on(1)
                send_diag(0)
                take_if(outer, 3)
                send_own(3)
                for c in range(NCH):
                    a_store(ast.at[c], c, z * NOWN, c).wait()
            else:
                send_side(2)
                more_on(2)

                @pl.when(inner)
                def _():
                    take_both(FAR)

        def granule(n, carry):
            for q in range(4):
                core_copy(n, q).wait_recv()
            gran = dz.at[5 + n // NCH, pl.ds(pl.multiple_of((n % NCH) * CH, CH), CH), :]
            w1_nat[...] = gran[:, LO].T
            for m in range(8):
                us_at(m)[...] = gelu(dot_nn(xo_at(m)[...], w1_nat[...])).astype(BF)
            for m in range(8):
                facc[m * SUB:(m + 1) * SUB, :] += dot_nn(us_at(m)[...], gran[:, HI])

            @pl.when(jnp.logical_and(n > 0, n + 2 < FAR))
            def _():
                send_side(n + 2)

            @pl.when(n + 1 < FAR)
            def _():
                send_diag(n + 1)

            @pl.when(jnp.logical_and(n + 1 >= FAR, n + 1 < NG))
            def _():
                pass_both(n + 1)

            @pl.when(n + 4 < FAR)
            def _():
                take_if(outer, n + 4)
                send_own(n + 4)

            @pl.when(jnp.logical_and(n + 4 >= FAR, n + 4 < NG))
            def _():
                @pl.when(outer)
                def _():
                    take_both(n + 4)

                send_both(n + 4)

            @pl.when(jnp.logical_and(inner, n < LAST))
            def _():
                take_both(n + FAR + 1)

            @pl.when(n < NCH)
            def _():
                acc1[n] = jnp.zeros(acc1.shape[1:], F32)
                acc2[n] = jnp.zeros(acc2.shape[1:], F32)

            return carry

        lax.fori_loop(0, NG, granule, 0)
        for m in range(8):
            xo_at(m)[...] = (xo_at(m)[...].astype(F32) + facc[m * SUB:(m + 1) * SUB, :]).astype(BF)

    ld_h.wait()
    hf = jnp.concatenate([heads[i].astype(F32) for i in range(NC)] + [jnp.zeros((2, D), F32)], axis=0)
    hcat[...] = hf.astype(BF)
    r = lax.broadcasted_iota(jnp.int32, (ER, D), 0)
    hb = jnp.concatenate([jnp.where(r % 2 == 0, hf, 0.0), jnp.where(r % 2 == 1, hf, 0.0)], axis=1)
    hbd[...] = jnp.concatenate([hb, hb, hb], axis=0).astype(BF)
    gm[...] = jnp.zeros_like(gm)

    pl.run_scoped(forward, pltpu.VMEM((NOWN, D), F32))

    for c in range(NCH):
        a_store(ast.at[c], c, z * NOWN, c).wait()

    def e_half(k, b):
        return eall.at[k, :, pl.ds(pl.multiple_of(b * TB, TB), TB)]

    def e_pair(b):
        return remote(e_half(0, b), e_half(1, b), ess.at[0, b], ers.at[1, b], pos.pair, j)

    def e_mirror(b):
        return remote(e_half(0, b), e_half(2, b), ess.at[1, b], ers.at[2, b], pos.mirror, j)

    def e_forward(k, b):
        to = 3 if k == 1 else k
        return remote(e_half(k, b), e_half(to, b), efs.at[k, b], ers.at[to, b], pos.mirror if k == 1 else pos.pair, j)

    def e_wait(k, b):
        remote(e_half(k, b), e_half(k, b), efs.at[k, b], ers.at[k, b], pos.pair, j).wait_recv()

    def step_of(s):
        return s // 8, (s % 8) // 2, s % 2

    def a_load(s):
        c, k, b = step_of(s)
        return pltpu.make_async_copy(a_hbm.at[c, pl.ds(share_row(k, b), TB)], ast.at[s % 2], as_sem.at[s % 2])

    def x_load(s):
        c, k, b = step_of(s)
        return pltpu.make_async_copy(x_hbm.at[pl.ds(share_row(k, b), TB)], xbuf.at[s % 2], xs_sem.at[s % 2])

    a_load(0).start()
    x_load(0).start()

    ld_l.wait()
    r = lax.broadcasted_iota(jnp.int32, (ER, TB), 0)
    first = r % 2 == 0
    real = r < 2 * NC
    neg = jnp.float32(-jnp.inf)
    for b in TWO:
        cols = slice(b * TB, (b + 1) * TB)
        logit = jnp.where(real, dot_nt(hcat[...], own_x[:, SIDES[b]]), neg)
        m0 = jnp.max(jnp.where(first, logit, neg), axis=0, keepdims=True)
        m1 = jnp.max(jnp.where(first, neg, logit), axis=0, keepdims=True)
        ex = jnp.exp(logit - jnp.where(first, m0, m1))
        s0 = jnp.sum(jnp.where(first, ex, 0.0), axis=0, keepdims=True)
        s1 = jnp.sum(jnp.where(first, 0.0, ex), axis=0, keepdims=True)
        prob = ex / jnp.where(first, s0, s1)
        lab = jnp.where(first, lab_v[0:1, cols], lab_v[1:2, cols])
        hot = jnp.where(jnp.logical_and(r // 2 == lab, real), 1.0, 0.0)
        eall[0, :, cols] = (prob - hot) / (NTOK * 8.0)
        e_pair(b).start()

        @pl.when(inner)
        def _():
            e_mirror(b).start()

    def drain(i, carry):
        x_copy(i).wait_send()
        diag_copy_y(i).wait_send()
        for q in range(4):
            core_copy(i, q).wait_send()

        @pl.when(i < FAR)
        def _():
            y_copy(i).wait_send()

        @pl.when(inner)
        def _():
            z_forward(i).wait_send()

            @pl.when(jnp.logical_or(i < NCH, i >= FAR))
            def _():
                more_forward(i).wait_send()

        return carry

    lax.fori_loop(0, NG, drain, 0)
    for c in range(NCH):
        z_pair(c).wait_send()

    @pl.when(inner)
    def _():
        for c in range(NCH):
            z_mirror(c).wait_send()

    everything = slice(None)
    sems = (rss, rsr)

    def up(c, t):
        return Scatter(pos, acc1.at[c, t], r1a.at[c, t], r2a.at[c, t], r3a.at[c, t], everything, sems,
                       c * 6 + t, t == 0)

    def down(c, t, part=None):
        if part is None:
            lanes, idx, x_first = everything, c * 6 + 2 + t, t == 0
        else:
            lanes, idx, x_first = slice(part * (D // 2), (part + 1) * (D // 2)), c * 6 + 2 + t * 2 + part, part == 0
        return Scatter(pos, acc2.at[c, t], r1b.at[c, t], r2b.at[c, t], r3b.at[c, t], lanes, sems, idx, x_first)

    ups = [[up(c, t) for t in TWO] for c in range(NCH)]
    downs = [[down(c, t) for t in TWO] for c in range(LAST)]
    tails = [[down(LAST, t, part) for part in TWO] for t in TWO]

    def each(group, stage):
        for sc in group:
            getattr(sc, stage)()

    def fold(v):
        rows, cols = v.shape
        total = jnp.zeros((8, 128), F32)
        for q in range(cols // 128):
            total = total + jnp.sum(v[:, q * 128:(q + 1) * 128].reshape(rows // 8, 8, 128), axis=0)
        return total

    def shard(acc, c, t):
        return acc.at[c, t, pos.y, pos.x, pos.core]

    def out_copy(acc, out, c, sem, t):
        return pltpu.make_async_copy(shard(acc, c, t), out.at[c, t], sh_sem.at[c, sem, t])

    def finish(acc, out, c, sem):
        v0, v1 = shard(acc, c, 0)[...], shard(acc, c, 1)[...]
        gm[0] += fold(v0 * v0)
        gm[1] += fold(v0 * v1)
        gm[2] += fold(v1 * v1)
        for t in TWO:
            out_copy(acc, out, c, sem, t).start()

    def finish_chunk(c):
        each(ups[c] + downs[c], 'done')
        finish(acc1, sh1_hbm, c, 0)
        finish(acc2, sh2_hbm, c, 1)

    def backward(us_all, das):
        def prepare(s):
            a_load(s).wait()
            x_load(s).wait()

            @pl.when(s < 23)
            def _():
                a_load(s + 1).start()
                x_load(s + 1).start()

        def d_act(s, us):
            c, k, b = step_of(s)
            w2c = wown[c, :, :, HI].reshape(CH, D)
            for m in BLOCKS:
                u, slope = gelu_and_slope(ast[s % 2, sub(m), :])
                us[sub(m), :] = u.astype(BF)
                for task in TWO:
                    da = dot_nt(dz[k * 2 + b, sub(m), SIDES[task]], w2c)
                    das[sub(m), task * CH:(task + 1) * CH] = (da * slope).astype(BF)

        def add_up(s):
            c, _, _ = step_of(s)
            g = dot_tn(xbuf[s % 2], das[...])
            for task in TWO:
                acc1[c, task] += g[:, task * CH:(task + 1) * CH].reshape(acc1.shape[2:])

        def step(s, carry):
            c, k, b = step_of(s)
            t = k * 2 + b
            prepare(s)

            @pl.when(c == 0)
            def _():
                @pl.when(jnp.logical_and(outer, k > 0))
                def _():
                    e_wait(k, b)

                e = e_half(k, b)[...]
                e1 = e.astype(BF).astype(F32)
                rest = e - e1
                e2 = rest.astype(BF).astype(F32)
                e3 = rest - e2
                es = jnp.concatenate([e1, e2, e3], axis=0).astype(BF)
                dz[t] = dot_tn(es, hbd[...]).astype(BF)

            us = us_all.at[0]
            d_act(s, us)
            add_up(s)
            g = dot_tn(us[...], dz[t])
            for task in TWO:
                acc2[c, task] += g[:, SIDES[task]].reshape(acc2.shape[2:])

            for when, k_f, b_f in ((1, 1, 0), (1, 2, 0), (2, 1, 1), (2, 2, 1), (3, 3, 0), (4, 3, 1)):
                @pl.when(jnp.logical_and(s == when, inner))
                def _():
                    e_forward_after_wait(k_f, b_f)

            @pl.when(s == 7)
            def _():
                each(ups[0] + downs[0], 'start')

            @pl.when(s == 9)
            def _():
                each(ups[0] + downs[0], 'side')

            @pl.when(s == 12)
            def _():
                each(ups[0], 'last')

            @pl.when(s == 13)
            def _():
                each(downs[0], 'last')

            @pl.when(s == 15)
            def _():
                each(ups[1] + downs[1], 'start')

            return carry

        def e_forward_after_wait(k, b):
            e_wait(k, b)
            e_forward(k, b).start()

        lax.fori_loop(0, 16, step, 0)

        def last_step(s, carry):
            c, k, b = step_of(s)
            prepare(s)
            d_act(s, us_all.at[k * 2 + b])
            add_up(s)

            @pl.when(s == 16)
            def _():
                finish_chunk(0)

            @pl.when(s == 17)
            def _():
                each(ups[1] + downs[1], 'side')

            @pl.when(s == 20)
            def _():
                each(ups[1], 'last')

            @pl.when(s == 22)
            def _():
                each(downs[1], 'last')

            return carry

        lax.fori_loop(16, 24, last_step, 0)
        each(ups[LAST], 'start')

        def down_pass(task):
            def two_blocks(i, carry):
                lanes = SIDES[task]
                g = dot_tn(us_all[i * 2], dz[i * 2, :, lanes])
                g = g + dot_tn(us_all[i * 2 + 1], dz[i * 2 + 1, :, lanes])
                acc2[LAST, task] += g.reshape(acc2.shape[2:])

                @pl.when(i == 1)
                def _():
                    each(ups[LAST] if task == 0 else tails[0], 'side')

                return carry

            lax.fori_loop(0, 4, two_blocks, 0)
            each(tails[task], 'start')

        down_pass(0)
        finish_chunk(1)
        down_pass(1)

    pl.run_scoped(backward, pltpu.VMEM((8, TB, CH), BF), pltpu.VMEM((TB, 2 * CH), BF))

    each(ups[LAST], 'last')
    each(tails[1], 'side')
    each(tails[0], 'last')
    each(ups[LAST], 'done')
    finish(acc1, sh1_hbm, LAST, 0)
    each(tails[1], 'last')
    each(tails[0], 'done')
    each(tails[1], 'done')
    finish(acc2, sh2_hbm, LAST, 1)

    def full(v):
        return jnp.sum(jnp.sum(v, axis=0, keepdims=True), axis=1, keepdims=True)

    lane = lax.broadcasted_iota(jnp.int32, (1, 128), 1)
    mbuf[pl.ds(me, 1), :] = jnp.where(lane == 0, full(gm[0]), jnp.where(lane == 1, full(gm[1]), full(gm[2])))

    def m_copy(i):
        to = (me + i) % NDEV
        line = mbuf.at[pl.ds(me, 1), :]
        return remote(line, line, mss.at[i], mrs.at[i], to // 8, to % 8)

    def m_start(i, carry):
        m_copy(i).start()
        return carry

    lax.fori_loop(1, NDEV, m_start, 0)

    for b in TWO:
        e_pair(b).wait_send()

        @pl.when(inner)
        def _():
            e_mirror(b).wait_send()
            for k in LINE:
                e_forward(k, b).wait_send()

    for group in ups + downs + tails:
        each(group, 'drain')
    for c in range(NCH):
        for t in TWO:
            out_copy(acc1, sh1_hbm, c, 0, t).wait()
            out_copy(acc2, sh2_hbm, c, 1, t).wait()

    def m_wait(i, carry):
        m_copy(i).wait()
        return carry

    lax.fori_loop(1, NDEV, m_wait, 0)
    gram = jnp.sum(mbuf[...], axis=0, keepdims=True)

    def entry(i):
        return jnp.sum(jnp.where(lane == i, gram, 0.0), axis=1, keepdims=True)

    g00, g01, g11 = entry(0), entry(1), entry(2)
    scale = (g00 + g11) / 2.0

    def eg_step(i, weights):
        a0, a1 = weights
        v0 = a0 * jnp.exp(-(g00 * a0 + g01 * a1) / scale)
        v1 = a1 * jnp.exp(-(g01 * a0 + g11 * a1) / scale)
        tot = v0 + v1
        return v0 / tot, v1 / tot

    half = jnp.full((1, 1), 0.5, F32)
    a0, a1 = lax.fori_loop(0, STEPS, eg_step, (half, half))
    row = lax.broadcasted_iota(jnp.int32, aw_ref.shape, 0)
    aw_ref[...] = jnp.where(row == 0, a0, a1)


def main_call(x, w1, w2r, heads, labels):
    dma = pltpu.SemaphoreType.DMA
    anyspec = pl.BlockSpec(memory_space=pl.ANY)
    vspec = pl.BlockSpec(memory_space=pltpu.VMEM)
    up, down = (OWN, CH), (GR, D)
    pair, quad, octet = (2,), (2, 2), (2, 2, 2)
    per_chunk = (NCH, 2)
    vmem = pltpu.VMEM
    return pl.pallas_call(
        main_kernel,
        out_shape=(jax.ShapeDtypeStruct((NCH, NTOK, CH), F32),
                   jax.ShapeDtypeStruct(per_chunk + up, F32),
                   jax.ShapeDtypeStruct(per_chunk + down, F32),
                   jax.ShapeDtypeStruct((8, 128), F32)),
        in_specs=[anyspec] * 5,
        out_specs=(anyspec, anyspec, anyspec, vspec),
        scratch_shapes=[
            vmem((8, TB, DD), BF),
            vmem((NCH, 8, GR, DD), BF),
            vmem(per_chunk + octet + up, F32), vmem(per_chunk + octet + down, F32),
            vmem(per_chunk + quad + up, F32), vmem(per_chunk + quad + down, F32),
            vmem(per_chunk + pair + up, F32), vmem(per_chunk + pair + down, F32),
            vmem(per_chunk + up, F32), vmem(per_chunk + down, F32),
            vmem((4, ER, NOWN), F32),
            vmem((NCH, TB, CH), F32),
            vmem((2, TB, D), BF),
            vmem((3 * ER, DD), BF),
            vmem((ER, D), BF),
            vmem((NC, 2, D), BF),
            vmem((2, NOWN), jnp.int32),
            vmem((3, 8, 128), F32), vmem((NDEV, 128), F32),
            dma((6,)), *[dma((NG,)) for _ in range(10)], dma((NG, 4)), dma((NG, 4)),
            dma((5,)), dma((NCH,)), dma(pair), dma((6,)), dma(quad), dma((4, 2)), dma((4, 2)),
            dma((6 * NCH, 3)), dma((6 * NCH, 3)), dma((NDEV,)), dma((NDEV,)), dma((NCH, 2, 2)),
        ],
        compiler_params=pltpu.CompilerParams(
            collective_id=0, has_side_effects=True, vmem_limit_bytes=VMEM_BYTES),
        name='main',
    )(x, w1, w2r, heads, labels)


def result_kernel(aw_ref, sh1, sh2, a_ref, g1_ref, g2_ref):
    a0, a1 = aw_ref[0:1, :], aw_ref[1:2, :]
    a_ref[0] = aw_ref[0, 0]
    a_ref[1] = aw_ref[1, 0]
    b0 = jnp.concatenate([a0] * 6, axis=1)
    b1 = jnp.concatenate([a1] * 6, axis=1)
    for c in range(NCH):
        comb = b0[:, 0:CH] * sh1[c, 0] + b1[:, 0:CH] * sh1[c, 1]
        for g in range(8):
            col = g * NCH * GR + c * GR
            g1_ref[:, col:col + GR] = comb[:, g * GR:(g + 1) * GR]
        g2_ref[c * GR:(c + 1) * GR, :] = b0 * sh2[c, 0] + b1 * sh2[c, 1]


def result_call(aw, sh1, sh2):
    vspec = pl.BlockSpec(memory_space=pltpu.VMEM)
    return pl.pallas_call(
        result_kernel,
        out_shape=(jax.ShapeDtypeStruct((2,), F32), jax.ShapeDtypeStruct((OWN, D), F32),
                   jax.ShapeDtypeStruct((OWN, D), F32)),
        in_specs=[vspec] * 3,
        out_specs=(pl.BlockSpec(memory_space=pltpu.SMEM), vspec, vspec),
        name='result',
    )(aw, sh1, sh2)


def solution(mesh):
    def local_step(tokens, w_up, w_down, task_heads, labels):
        w2r = w_down.reshape(8, NCH, GR, D)
        heads = jnp.transpose(task_heads, (2, 0, 1))
        _, sh1, sh2, aw = main_call(tokens, w_up, w2r, heads, labels)
        return result_call(aw, sh1, sh2)

    return jax.shard_map(
        local_step, mesh=mesh,
        in_specs=(P('data', None), P(None, 'model'), P('model', None), P(None, None, None), P(None, 'data')),
        out_specs=(P(None), P('data', 'model'), P(('model', 'data'), None)),
        check_vma=False)
```

```python
import jax
import jax.numpy as jnp
from jax import lax
from jax.experimental import pallas as pl
from jax.experimental.pallas import tpu as pltpu
from jax.sharding import PartitionSpec as P

STEPS = 20
BF = jnp.bfloat16
F32 = jnp.float32
MESH = pl.DeviceIdType.MESH
VMEM_BYTES = 67043328

D = 768
DD = D + D
NTOK = 8192
NOWN = 2048
TB = 1024
SUB = 256
NC = 19
ER = 40
CH = 256
NCH = 3
LAST = NCH - 1
NG = NCH * NCH
FAR = NG - NCH
GR = 32
OWN = CH // GR * 12
LO = slice(D)
HI = slice(D, DD)
SIDES = (LO, HI)
TWO = range(2)
MATES = range(1, 8)
LINE = range(1, 4)
BLOCKS = range(TB // SUB)
NDEV = 32

G0 = 0.7978845608028654
G1C = 0.044715 * G0


def dot_nn(a, b):
    return lax.dot_general(a, b, (((1,), (0,)), ((), ())), preferred_element_type=F32)


def dot_nt(a, b):
    return lax.dot_general(a, b, (((1,), (1,)), ((), ())), preferred_element_type=F32)


def dot_tn(a, b):
    return lax.dot_general(a, b, (((0,), (0,)), ((), ())), preferred_element_type=F32)


def gelu(x):
    t = jnp.tanh(x * (G0 + G1C * (x * x)))
    h = 0.5 * x
    return h + h * t


def gelu_and_slope(x):
    x2 = x * x
    t = jnp.tanh(x * (G0 + G1C * x2))
    h = 0.5 * x
    u = h + h * t
    s = 0.5 + 0.5 * t + h * (1.0 - t * t) * (G0 + (3.0 * G1C) * x2)
    return u, s


class Place:
    def __init__(self):
        self.z = lax.axis_index('model')
        self.j = lax.axis_index('data')
        self.core = self.j % 2
        self.x = (self.j // 2) % 2
        self.y = self.j // 4
        self.jc = self.j + 1 - 2 * self.core
        self.jx = self.j + 2 - 4 * self.x
        self.jy = self.j + 4 - 8 * self.y
        self.jd = self.jx + 4 - 8 * self.y
        self.js = self.jx + self.core * (self.jy - self.jx)
        self.j2 = self.jx + self.jy - self.js

        self.inner = self.z % 3 > 0
        self.pair = self.z + 1 - 2 * (self.z % 2)
        self.mirror = 3 - self.z
        half = self.z // 2
        self.shares = (self.z, self.pair, 2 - half, 3 - 3 * half)

    def share(self, k):
        own, near, far, end = self.shares
        return jnp.where(k == 0, own, jnp.where(k == 1, near, jnp.where(k == 2, far, end)))


def remote(src, dst, ssem, rsem, z, j):
    return pltpu.make_async_remote_copy(
        src_ref=src, dst_ref=dst, send_sem=ssem, recv_sem=rsem, device_id=(z, j), device_id_type=MESH)


class Scatter:
    def __init__(self, pos, acc, r1, r2, r3, lanes, sems, idx, x_first):
        self.pos, self.acc, self.r1, self.r2, self.r3 = pos, acc, r1, r2, r3
        self.lanes, self.sems, self.idx, self.x_first = lanes, sems, idx, x_first

    def copy(self, stage):
        p, ln = self.pos, self.lanes
        ssem, rsem = self.sems[0].at[stage], self.sems[1].at[self.idx, stage]
        if stage == 0:
            return remote(self.acc.at[:, :, 1 - p.core, :, ln], self.r1.at[:, :, :, ln], ssem, rsem, p.z, p.jc)
        if stage == 1:
            if self.x_first:
                return remote(self.acc.at[:, 1 - p.x, p.core, :, ln], self.r2.at[:, :, ln], ssem, rsem, p.z, p.jx)
            return remote(self.acc.at[1 - p.y, :, p.core, :, ln], self.r2.at[:, :, ln], ssem, rsem, p.z, p.jy)
        if self.x_first:
            return remote(self.acc.at[1 - p.y, p.x, p.core, :, ln], self.r3.at[:, ln], ssem, rsem, p.z, p.jy)
        return remote(self.acc.at[p.y, 1 - p.x, p.core, :, ln], self.r3.at[:, ln], ssem, rsem, p.z, p.jx)

    def start(self):
        self.copy(0).start()

    def side(self):
        p, ln = self.pos, self.lanes
        self.copy(0).wait_recv()
        for yy in TWO:
            for xx in TWO:
                self.acc[yy, xx, p.core, :, ln] += self.r1[yy, xx, :, ln]
        self.copy(1).start()

    def last(self):
        p, ln = self.pos, self.lanes
        self.copy(1).wait_recv()
        for i in TWO:
            if self.x_first:
                self.acc[i, p.x, p.core, :, ln] += self.r2[i, :, ln]
            else:
                self.acc[p.y, i, p.core, :, ln] += self.r2[i, :, ln]
        self.copy(2).start()

    def done(self):
        p, ln = self.pos, self.lanes
        self.copy(2).wait_recv()
        self.acc[p.y, p.x, p.core, :, ln] += self.r3[:, ln]


def main_kernel(x_hbm, w1_hbm, w2_hbm, heads_hbm, lab_hbm,
                a_hbm, sh1_hbm, sh2_hbm, rows_ref,
                dz, wown, acc1, acc2, r1a, r1b, r2a, r2b, r3a, r3b, eall, ast, xbuf, hbd, hcat, heads, lab_v,
                gm, mbuf,
                zss, zrs, zqs, xss, xrs, yss, yrs, dss, drs, css, crs,
                ld_sem, w2_sem, xs_sem, as_sem, ess, efs, ers,
                rss, rsr, mss, mrs, sh_sem):
    pos = Place()
    z, j, inner = pos.z, pos.j, pos.inner
    outer = jnp.logical_not(inner)

    barrier = pltpu.get_barrier_semaphore()
    me = z * 8 + j
    pl.semaphore_signal(barrier, device_id=(pos.pair, j), device_id_type=MESH)

    @pl.when(inner)
    def _():
        pl.semaphore_signal(barrier, device_id=(pos.mirror, j), device_id_type=MESH)

    for jj in (pos.jx, pos.jy, pos.jc):
        pl.semaphore_signal(barrier, device_id=(z, jj), device_id_type=MESH)

    own_x, act, room = dz.at[0], dz.at[2], dz.at[3]
    w1_raw = room.at[LO, LO]
    w1_nat = room.at[LO, D:D + CH]
    w1_own = dz.at[4, LO, HI]

    def sub(m):
        return slice((m % 4) * SUB, (m % 4 + 1) * SUB)

    def xo_at(m):
        return own_x.at[sub(m), HI if m >= 4 else LO]

    def us_at(m):
        lane = D + (m // 4) * CH
        return act.at[sub(m), lane:lane + CH]

    def share_row(k, b):
        return pl.multiple_of((pos.share(k) * 2 + b) * TB, TB)

    own_row = pl.multiple_of(z * NOWN, NOWN)
    ld_w1 = pltpu.make_async_copy(w1_hbm, w1_raw, ld_sem.at[0])
    ld_x = [pltpu.make_async_copy(x_hbm.at[pl.ds(own_row + b * TB, TB)], own_x.at[:, SIDES[b]], ld_sem.at[1 + b])
            for b in TWO]
    ld_l = pltpu.make_async_copy(lab_hbm.at[:, pl.ds(own_row, NOWN)], lab_v, ld_sem.at[3])
    ld_h = pltpu.make_async_copy(heads_hbm, heads, ld_sem.at[4])
    ld_w2 = [pltpu.make_async_copy(w2_hbm.at[:, c], wown.at[c, :, :, HI], w2_sem.at[c]) for c in range(NCH)]

    def stream_half(i):
        return dz.at[1 + 3 * (i % 2), :, LO]

    def xs_load(i):
        return pltpu.make_async_copy(
            x_hbm.at[pl.ds(share_row(1 + i // 2, i % 2), TB)], stream_half(i), xs_sem.at[i % 2])

    ld_w1.start()
    for cp in ld_w2:
        cp.start()
    xs_load(0).start()
    for cp in ld_x:
        cp.start()
    ld_h.start()
    ld_l.start()

    ld_w1.wait()
    w1t = w1_raw[...].T
    for c in range(NCH):
        for g in range(8):
            row = g * NCH * GR + c * GR
            wown[c, g, :, LO] = w1t[row:row + GR, :]
    for cp in ld_w2:
        cp.wait()
    pl.semaphore_wait(barrier, 4 + z * pos.mirror // 2)

    def piece(i, jj):
        row = pl.multiple_of((i % NCH) * CH + jj * GR, GR)
        return dz.at[5 + i // NCH, pl.ds(row, GR), :]

    def rows_of(n, ssem, rsem):
        part = dz.at[5, pl.ds(0, n * GR), :]
        return remote(part, part, ssem, rsem, z, pos.jc)

    def z_pair(c):
        return remote(wown.at[c, j], piece(c, j), zss.at[0], zrs.at[c], pos.pair, j)

    def z_mirror(c):
        return remote(wown.at[c, j], piece(NCH + c, j), zss.at[1], zrs.at[NCH + c], pos.mirror, j)

    def z_forward(i):
        first = i < NCH
        to = jnp.where(first, i + 2 * NCH, i)
        return remote(piece(i, j), piece(to, j), zss.at[2], zrs.at[to], jnp.where(first, pos.mirror, pos.pair), j)

    def more_forward(i):
        first = i < NCH
        to = jnp.where(first, i + 2 * NCH, i)
        return remote(piece(i, pos.j2), piece(to, pos.j2), zss.at[3], zqs.at[to - FAR], jnp.where(first, pos.mirror, pos.pair), j)

    def side_copy(i):
        return remote(piece(i, j), piece(i, j), xss, xrs.at[i], z, pos.js)

    def more_copy(i):
        return remote(piece(i, pos.j2), piece(i, pos.j2), dss, drs.at[i], z, pos.js)

    def x_copy(i):
        return remote(piece(i, j), piece(i, j), xss, xrs.at[i], z, pos.jx)

    def y_copy(i):
        return remote(piece(i, j), piece(i, j), yss, yrs.at[i], z, pos.jy)

    def diag_copy_y(i):
        return remote(piece(i, pos.jx), piece(i, pos.jx), dss, drs.at[i], z, pos.jy)

    def diag_copy_x(i):
        return remote(piece(i, pos.jy), piece(i, pos.jy), dss, drs.at[i], z, pos.jx)

    def core_copy(i, q):
        jj = (j, pos.jx, pos.jy, pos.jd)[q]
        return remote(piece(i, jj), piece(i, jj), css.at[i], crs.at[i], z, pos.jc)

    def core_side(i, q):
        jj = (j, pos.js, pos.j2, pos.jd)[q]
        return remote(piece(i, jj), piece(i, jj), css.at[i], crs.at[i], z, pos.jc)

    def take(i):
        remote(piece(i, j), piece(i, j), zss.at[2], zrs.at[i], pos.pair, j).wait_recv()

        @pl.when(inner)
        def _():
            z_forward(i).start()

    def take_both(i):
        remote(piece(i, j), piece(i, j), zss.at[2], zrs.at[i], pos.pair, j).wait_recv()
        remote(piece(i, j), piece(i, j), zss.at[3], zqs.at[i - FAR], pos.pair, j).wait_recv()

        @pl.when(inner)
        def _():
            z_forward(i).start()
            more_forward(i).start()

    def send_both(i):
        side_copy(i).start()
        more_copy(i).start()
        core_side(i, 0).start()
        core_side(i, 2).start()

    def pass_both(i):
        side_copy(i).wait_recv()
        core_side(i, 1).start()
        more_copy(i).wait_recv()
        core_side(i, 3).start()

    def take_if(cond, i):
        @pl.when(cond)
        def _():
            take(i)

    def send_own(i):
        x_copy(i).start()
        y_copy(i).start()
        core_copy(i, 0).start()

    def send_side(i):
        x_copy(i).wait_recv()

        @pl.when(pos.core == 0)
        def _():
            diag_copy_y(i).start()

        core_copy(i, 1).start()
        y_copy(i).wait_recv()

        @pl.when(pos.core == 1)
        def _():
            diag_copy_x(i).start()

        core_copy(i, 2).start()

    def more_on(i):
        @pl.when(inner)
        def _():
            more_forward(i).start()

    def send_diag(i):
        diag_copy_y(i).wait_recv()
        core_copy(i, 3).start()

    for c in range(NCH):
        z_pair(c).start()

    @pl.when(inner)
    def _():
        for c in range(NCH):
            z_mirror(c).start()

    def a_store(src, c, row, sem):
        return pltpu.make_async_copy(src, a_hbm.at[c, pl.ds(pl.multiple_of(row, TB), TB)], as_sem.at[sem])

    def forward(facc):
        for c in range(NCH):
            w1_own[:, c * CH:(c + 1) * CH] = wown[c, :, :, LO].reshape(CH, D).T

        def staged(i, c):
            rows = pl.ds(pl.multiple_of((i % 2) * TB, TB), TB)
            return a_store(facc.at[rows, c * CH:(c + 1) * CH], c, share_row(1 + i // 2, i % 2), (i % 2) * NCH + c)

        def other_tokens(i, carry):
            xs_load(i).wait()

            @pl.when(i < 5)
            def _():
                xs_load(i + 1).start()

            @pl.when(i >= 2)
            def _():
                for c in range(NCH):
                    staged(i, c).wait()

            base = (i % 2) * TB
            for m in BLOCKS:
                rows = pl.ds(pl.multiple_of(base + m * SUB, SUB), SUB)
                facc[rows, :] = dot_nn(stream_half(i)[sub(m), :], w1_own[...])
            for c in range(NCH):
                staged(i, c).start()

            @pl.when(i == 2)
            def _():
                take(0)
                send_own(0)
                take_if(inner, 3)

            @pl.when(i == 3)
            def _():
                take(1)
                send_own(1)
                take_if(inner, 4)

            @pl.when(i == 4)
            def _():
                take_if(inner, 5)

            @pl.when(i == 5)
            def _():
                send_side(0)
                more_on(0)
                take(2)
                send_own(2)

            return carry

        lax.fori_loop(0, 6, other_tokens, 0)
        for cp in ld_x:
            cp.wait()

        for b in TWO:
            for c in range(NCH):
                staged(b, c).wait()
            for m in BLOCKS:
                a = dot_nn(xo_at(b * 4 + m)[...], w1_own[...])
                for c in range(NCH):
                    ast[c, sub(m), :] = a[:, c * CH:(c + 1) * CH]
                act[sub(m), LO] = gelu(a).astype(BF)
            for m in BLOCKS:
                facc[b * TB + m * SUB:b * TB + (m + 1) * SUB, :] = dot_nn(
                    act[sub(m), LO], wown[:, :, :, HI].reshape(D, D))
            for c in range(NCH):
                a_store(ast.at[c], c, (z * 2 + b) * TB, c).start()
            if b == 0:
                send_side(1)
                more_on(1)
                send_diag(0)
                take_if(outer, 3)
                send_own(3)
                for c in range(NCH):
                    a_store(ast.at[c], c, z * NOWN, c).wait()
            else:
                send_side(2)
                more_on(2)
                send_diag(1)
                take_if(outer, 4)
                send_own(4)

                @pl.when(inner)
                def _():
                    take_both(FAR)

        def granule(n, carry):
            rows_of(4, css.at[n], crs.at[n]).wait_recv()
            gran = dz.at[5 + n // NCH, pl.ds(pl.multiple_of((n % NCH) * CH, CH), CH), :]
            w1_nat[...] = gran[:, LO].T
            for m in range(8):
                us_at(m)[...] = gelu(dot_nn(xo_at(m)[...], w1_nat[...])).astype(BF)
            for m in range(8):
                facc[m * SUB:(m + 1) * SUB, :] += dot_nn(us_at(m)[...], gran[:, HI])

            @pl.when(n + 3 < FAR)
            def _():
                send_side(n + 3)

            @pl.when(n + 2 < FAR)
            def _():
                send_diag(n + 2)

            @pl.when(jnp.logical_and(n + 2 >= FAR, n + 2 < NG))
            def _():
                pass_both(n + 2)

            @pl.when(n == 0)
            def _():
                take_if(outer, 5)
                send_own(5)

            @pl.when(jnp.logical_and(inner, n < LAST))
            def _():
                take_both(FAR + 1 + n)

            @pl.when(jnp.logical_and(n + 4 >= FAR, n + 4 < NG))
            def _():
                @pl.when(outer)
                def _():
                    take_both(n + 4)

                send_both(n + 4)

            @pl.when(n < NCH)
            def _():
                acc1[n] = jnp.zeros(acc1.shape[1:], F32)
                acc2[n] = jnp.zeros(acc2.shape[1:], F32)

            return carry

        lax.fori_loop(0, NG, granule, 0)
        for m in range(8):
            xo_at(m)[...] = (xo_at(m)[...].astype(F32) + facc[m * SUB:(m + 1) * SUB, :]).astype(BF)

    ld_h.wait()
    hf = jnp.concatenate([heads[i].astype(F32) for i in range(NC)] + [jnp.zeros((2, D), F32)], axis=0)
    hcat[...] = hf.astype(BF)
    r = lax.broadcasted_iota(jnp.int32, (ER, D), 0)
    hb = jnp.concatenate([jnp.where(r % 2 == 0, hf, 0.0), jnp.where(r % 2 == 1, hf, 0.0)], axis=1)
    hbd[...] = jnp.concatenate([hb, hb, hb], axis=0).astype(BF)
    gm[...] = jnp.zeros_like(gm)

    pl.run_scoped(forward, pltpu.VMEM((NOWN, D), F32))

    for c in range(NCH):
        a_store(ast.at[c], c, z * NOWN, c).wait()

    def e_half(k, b):
        return eall.at[k, :, pl.ds(pl.multiple_of(b * TB, TB), TB)]

    def e_pair(b):
        return remote(e_half(0, b), e_half(1, b), ess.at[0, b], ers.at[1, b], pos.pair, j)

    def e_mirror(b):
        return remote(e_half(0, b), e_half(2, b), ess.at[1, b], ers.at[2, b], pos.mirror, j)

    def e_forward(k, b):
        to = 3 if k == 1 else k
        return remote(e_half(k, b), e_half(to, b), efs.at[k, b], ers.at[to, b], pos.mirror if k == 1 else pos.pair, j)

    def e_wait(k, b):
        remote(e_half(k, b), e_half(k, b), efs.at[k, b], ers.at[k, b], pos.pair, j).wait_recv()

    def step_of(s):
        return s // 8, (s % 8) // 2, s % 2

    def a_load(s):
        c, k, b = step_of(s)
        return pltpu.make_async_copy(a_hbm.at[c, pl.ds(share_row(k, b), TB)], ast.at[s % 2], as_sem.at[s % 2])

    def x_load(s):
        c, k, b = step_of(s)
        return pltpu.make_async_copy(x_hbm.at[pl.ds(share_row(k, b), TB)], xbuf.at[s % 2], xs_sem.at[s % 2])

    a_load(0).start()
    x_load(0).start()

    ld_l.wait()
    r = lax.broadcasted_iota(jnp.int32, (ER, TB), 0)
    first = r % 2 == 0
    real = r < 2 * NC
    neg = jnp.float32(-jnp.inf)
    for b in TWO:
        cols = slice(b * TB, (b + 1) * TB)
        logit = jnp.where(real, dot_nt(hcat[...], own_x[:, SIDES[b]]), neg)
        m0 = jnp.max(jnp.where(first, logit, neg), axis=0, keepdims=True)
        m1 = jnp.max(jnp.where(first, neg, logit), axis=0, keepdims=True)
        ex = jnp.exp(logit - jnp.where(first, m0, m1))
        s0 = jnp.sum(jnp.where(first, ex, 0.0), axis=0, keepdims=True)
        s1 = jnp.sum(jnp.where(first, 0.0, ex), axis=0, keepdims=True)
        prob = ex / jnp.where(first, s0, s1)
        lab = jnp.where(first, lab_v[0:1, cols], lab_v[1:2, cols])
        hot = jnp.where(jnp.logical_and(r // 2 == lab, real), 1.0, 0.0)
        eall[0, :, cols] = (prob - hot) / (NTOK * 8.0)
        e_pair(b).start()

        @pl.when(inner)
        def _():
            e_mirror(b).start()

    rows_of(NG, xss, xrs.at[0]).wait_send()
    rows_of(FAR, yss, yrs.at[0]).wait_send()
    rows_of(NG, dss, drs.at[0]).wait_send()
    for i in range(NG):
        rows_of(4, css.at[i], crs.at[i]).wait_send()
    rows_of(NCH, zss.at[0], zrs.at[0]).wait_send()

    @pl.when(inner)
    def _():
        for n, i in ((NCH, 1), (NG, 2), (FAR, 3)):
            rows_of(n, zss.at[i], zrs.at[0]).wait_send()

    everything = slice(None)
    up_sems, down_sems = (rss.at[0], rsr), (rss.at[1], rsr)

    def up(c, t):
        return Scatter(pos, acc1.at[c, t], r1a.at[c, t], r2a.at[c, t], r3a.at[c, t], everything, up_sems,
                       c * 6 + t, t == 0)

    def down(c, t, part=None):
        if part is None:
            lanes, idx, x_first = everything, c * 6 + 2 + t, t == 0
        else:
            lanes, idx, x_first = slice(part * (D // 2), (part + 1) * (D // 2)), c * 6 + 2 + t * 2 + part, part == 0
        return Scatter(pos, acc2.at[c, t], r1b.at[c, t], r2b.at[c, t], r3b.at[c, t], lanes, down_sems, idx, x_first)

    ups = [[up(c, t) for t in TWO] for c in range(NCH)]
    downs = [[down(c, t) for t in TWO] for c in range(LAST)]
    tails = [[down(LAST, t, part) for part in TWO] for t in TWO]

    def each(group, stage):
        for sc in group:
            getattr(sc, stage)()

    def fold(v):
        rows, cols = v.shape
        total = jnp.zeros((8, 128), F32)
        for q in range(cols // 128):
            total = total + jnp.sum(v[:, q * 128:(q + 1) * 128].reshape(rows // 8, 8, 128), axis=0)
        return total

    def shard(acc, c, t):
        return acc.at[c, t, pos.y, pos.x, pos.core]

    def out_copy(acc, out, c, sem, t):
        return pltpu.make_async_copy(shard(acc, c, t), out.at[c, t], sh_sem.at[sem])

    def finish(acc, out, c, sem):
        v0, v1 = shard(acc, c, 0)[...], shard(acc, c, 1)[...]
        gm[0] += fold(v0 * v0)
        gm[1] += fold(v0 * v1)
        gm[2] += fold(v1 * v1)
        for t in TWO:
            out_copy(acc, out, c, sem, t).start()

    def finish_chunk(c):
        each(ups[c] + downs[c], 'done')
        finish(acc1, sh1_hbm, c, 0)
        finish(acc2, sh2_hbm, c, 1)

    def backward(us_all, das):
        def prepare(s):
            a_load(s).wait()
            x_load(s).wait()

            @pl.when(s < 23)
            def _():
                a_load(s + 1).start()
                x_load(s + 1).start()

        def d_act(s, us):
            c, k, b = step_of(s)
            w2c = wown[c, :, :, HI].reshape(CH, D)
            for m in BLOCKS:
                u, slope = gelu_and_slope(ast[s % 2, sub(m), :])
                us[sub(m), :] = u.astype(BF)
                for task in TWO:
                    da = dot_nt(dz[k * 2 + b, sub(m), SIDES[task]], w2c)
                    das[sub(m), task * CH:(task + 1) * CH] = (da * slope).astype(BF)

        def add_up(s):
            c, _, _ = step_of(s)
            g = dot_tn(xbuf[s % 2], das[...])
            for task in TWO:
                acc1[c, task] += g[:, task * CH:(task + 1) * CH].reshape(acc1.shape[2:])

        def fill_dz(s):
            _, k, b = step_of(s)
            e = e_half(k, b)[...]
            e1 = e.astype(BF).astype(F32)
            rest = e - e1
            e2 = rest.astype(BF).astype(F32)
            e3 = rest - e2
            es = jnp.concatenate([e1, e2, e3], axis=0).astype(BF)
            for m in BLOCKS:
                dz[k * 2 + b, sub(m), :] = dot_tn(es[:, sub(m)], hbd[...]).astype(BF)

        def both(s):
            c, k, b = step_of(s)
            us = us_all.at[0]
            d_act(s, us)
            add_up(s)
            g = dot_tn(us[...], dz[k * 2 + b])
            for task in TWO:
                acc2[c, task] += g[:, SIDES[task]].reshape(acc2.shape[2:])

        def first_step(s, carry):
            _, k, b = step_of(s)
            prepare(s)

            @pl.when(jnp.logical_and(outer, k > 0))
            def _():
                e_wait(k, b)

            fill_dz(s)
            both(s)

            for when, k_f, b_f in ((1, 1, 0), (1, 2, 0), (2, 1, 1), (2, 2, 1), (3, 3, 0), (4, 3, 1)):
                @pl.when(jnp.logical_and(s == when, inner))
                def _():
                    e_forward_after_wait(k_f, b_f)

            return carry

        def step(s, carry):
            prepare(s)
            both(s)

            @pl.when(s == 9)
            def _():
                each(ups[0] + downs[0], 'side')

            @pl.when(s == 12)
            def _():
                each(ups[0], 'last')

            @pl.when(s == 13)
            def _():
                each(downs[0], 'last')

            return carry

        def e_forward_after_wait(k, b):
            e_wait(k, b)
            e_forward(k, b).start()

        lax.fori_loop(0, 8, first_step, 0)
        each(ups[0] + downs[0], 'start')
        lax.fori_loop(8, 16, step, 0)
        each(ups[1] + downs[1], 'start')

        def last_step(s, carry):
            c, k, b = step_of(s)
            prepare(s)
            d_act(s, us_all.at[k * 2 + b])
            add_up(s)

            @pl.when(s == 16)
            def _():
                finish_chunk(0)

            @pl.when(s == 17)
            def _():
                each(ups[1], 'side')

            @pl.when(s == 19)
            def _():
                each(downs[1], 'side')

            @pl.when(s == 20)
            def _():
                each(ups[1], 'last')

            return carry

        lax.fori_loop(16, 24, last_step, 0)
        each(ups[LAST], 'start')
        each(downs[1], 'last')

        def down_pass(task):
            def two_blocks(i, carry):
                lanes = SIDES[task]
                g = dot_tn(us_all[i * 2], dz[i * 2, :, lanes])
                g = g + dot_tn(us_all[i * 2 + 1], dz[i * 2 + 1, :, lanes])
                acc2[LAST, task] += g.reshape(acc2.shape[2:])

                @pl.when(i == 1)
                def _():
                    each(ups[LAST] if task == 0 else tails[0], 'side')

                return carry

            lax.fori_loop(0, 4, two_blocks, 0)
            each(tails[task], 'start')

        down_pass(0)
        finish_chunk(1)
        down_pass(1)

    pl.run_scoped(backward, pltpu.VMEM((8, TB, CH), BF), pltpu.VMEM((TB, 2 * CH), BF))

    each(ups[LAST], 'last')
    each(tails[1], 'side')
    each(tails[0], 'last')
    each(ups[LAST], 'done')
    finish(acc1, sh1_hbm, LAST, 0)
    each(tails[1], 'last')
    each(tails[0], 'done')
    each(tails[1], 'done')
    finish(acc2, sh2_hbm, LAST, 1)

    def full(v):
        return jnp.sum(jnp.sum(v, axis=0, keepdims=True), axis=1, keepdims=True)

    lane = lax.broadcasted_iota(jnp.int32, (1, 128), 1)
    mbuf[pl.ds(me, 1), :] = jnp.where(lane == 0, full(gm[0]), jnp.where(lane == 1, full(gm[1]), full(gm[2])))

    def m_copy(i):
        to = (me + i) % NDEV
        line = mbuf.at[pl.ds(me, 1), :]
        return remote(line, line, mss, mrs, to // 8, to % 8)

    def m_start(i, carry):
        m_copy(i).start()
        return carry

    lax.fori_loop(1, NDEV, m_start, 0)

    for b in TWO:
        e_pair(b).wait_send()

        @pl.when(inner)
        def _():
            e_mirror(b).wait_send()
            for k in LINE:
                e_forward(k, b).wait_send()

    for kind, all_stages in enumerate(((r1a, r2a, r3a), (r1b, r2b, r3b))):
        for stage, buf in enumerate(all_stages):
            remote(buf, buf, rss.at[kind, stage], rsr.at[0, stage], z, pos.jc).wait_send()
    pltpu.make_async_copy(r3a, sh1_hbm, sh_sem.at[0]).wait()
    pltpu.make_async_copy(r3b, sh2_hbm, sh_sem.at[1]).wait()

    lines = mbuf.at[pl.ds(0, NDEV - 1), :]
    remote(lines, lines, mss, mrs, z, pos.jc).wait()
    rows_ref[...] = mbuf[...]


def main_call(x, w1, w2r, heads, labels):
    dma = pltpu.SemaphoreType.DMA
    anyspec = pl.BlockSpec(memory_space=pl.ANY)
    vspec = pl.BlockSpec(memory_space=pltpu.VMEM)
    up, down = (OWN, CH), (GR, D)
    pair, quad, octet = (2,), (2, 2), (2, 2, 2)
    per_chunk = (NCH, 2)
    vmem = pltpu.VMEM
    return pl.pallas_call(
        main_kernel,
        out_shape=(jax.ShapeDtypeStruct((NCH, NTOK, CH), F32),
                   jax.ShapeDtypeStruct(per_chunk + up, F32),
                   jax.ShapeDtypeStruct(per_chunk + down, F32),
                   jax.ShapeDtypeStruct((NDEV, 128), F32)),
        in_specs=[anyspec] * 5,
        out_specs=(anyspec, anyspec, anyspec, vspec),
        scratch_shapes=[
            vmem((8, TB, DD), BF),
            vmem((NCH, 8, GR, DD), BF),
            vmem(per_chunk + octet + up, F32), vmem(per_chunk + octet + down, F32),
            vmem(per_chunk + quad + up, F32), vmem(per_chunk + quad + down, F32),
            vmem(per_chunk + pair + up, F32), vmem(per_chunk + pair + down, F32),
            vmem(per_chunk + up, F32), vmem(per_chunk + down, F32),
            vmem((4, ER, NOWN), F32),
            vmem((NCH, TB, CH), F32),
            vmem((2, TB, D), BF),
            vmem((3 * ER, DD), BF),
            vmem((ER, D), BF),
            vmem((NC, 2, D), BF),
            vmem((2, NOWN), jnp.int32),
            vmem((3, 8, 128), F32), vmem((NDEV, 128), F32),
            dma((4,)), dma((NG,)), dma((NCH,)), dma(()), dma((NG,)), dma(()), dma((FAR,)), dma(()), dma((NG,)), dma((NG,)), dma((NG,)),
            dma((5,)), dma((NCH,)), dma(pair), dma((6,)), dma(quad), dma((4, 2)), dma((4, 2)),
            dma((2, NCH)), dma((6 * NCH, NCH)), dma(()), dma(()), dma(pair),
        ],
        compiler_params=pltpu.CompilerParams(
            collective_id=0, has_side_effects=True, vmem_limit_bytes=VMEM_BYTES),
        name='main',
    )(x, w1, w2r, heads, labels)


def result_kernel(rows_hbm, sh1_hbm, sh2_hbm, a_ref, g1_ref, g2_ref, rows, sh1, sh2, sem):
    ld_rows = pltpu.make_async_copy(rows_hbm, rows, sem.at[0])
    loads = [pltpu.make_async_copy(sh1_hbm, sh1, sem.at[1]), pltpu.make_async_copy(sh2_hbm, sh2, sem.at[2])]
    ld_rows.start()
    for cp in loads:
        cp.start()
    ld_rows.wait()

    gram = jnp.sum(rows[...], axis=0, keepdims=True)
    lane = lax.broadcasted_iota(jnp.int32, gram.shape, 1)

    def entry(i):
        return jnp.sum(jnp.where(lane == i, gram, 0.0), axis=1, keepdims=True)

    g00, g01, g11 = entry(0), entry(1), entry(2)
    scale = (g00 + g11) / 2.0

    def eg_step(i, weights):
        a0, a1 = weights
        v0 = a0 * jnp.exp(-(g00 * a0 + g01 * a1) / scale)
        v1 = a1 * jnp.exp(-(g01 * a0 + g11 * a1) / scale)
        tot = v0 + v1
        return v0 / tot, v1 / tot

    half = jnp.full((1, 1), 0.5, F32)
    a0, a1 = lax.fori_loop(0, STEPS, eg_step, (half, half))
    a_ref[0] = a0[0, 0]
    a_ref[1] = a1[0, 0]
    for cp in loads:
        cp.wait()
    for c in range(NCH):
        comb = a0 * sh1[c, 0] + a1 * sh1[c, 1]
        for g in range(8):
            col = g * NCH * GR + c * GR
            g1_ref[:, col:col + GR] = comb[:, g * GR:(g + 1) * GR]
        g2_ref[c * GR:(c + 1) * GR, :] = a0 * sh2[c, 0] + a1 * sh2[c, 1]


def result_call(rows, sh1, sh2):
    vspec = pl.BlockSpec(memory_space=pltpu.VMEM)
    anyspec = pl.BlockSpec(memory_space=pl.ANY)
    return pl.pallas_call(
        result_kernel,
        out_shape=(jax.ShapeDtypeStruct((2,), F32), jax.ShapeDtypeStruct((OWN, D), F32),
                   jax.ShapeDtypeStruct((OWN, D), F32)),
        in_specs=[anyspec] * NCH,
        out_specs=(pl.BlockSpec(memory_space=pltpu.SMEM), vspec, vspec),
        scratch_shapes=[pltpu.VMEM(v.shape, F32) for v in (rows, sh1, sh2)] + [pltpu.SemaphoreType.DMA((NCH,))],
        name='result',
    )(rows, sh1, sh2)


def solution(mesh):
    def local_step(tokens, w_up, w_down, task_heads, labels):
        w2r = w_down.reshape(8, NCH, GR, D)
        heads = jnp.transpose(task_heads, (2, 0, 1))
        _, sh1, sh2, rows = main_call(tokens, w_up, w2r, heads, labels)
        return result_call(rows, sh1, sh2)

    return jax.shard_map(
        local_step, mesh=mesh,
        in_specs=(P('data', None), P(None, 'model'), P('model', None), P(None, None, None), P(None, 'data')),
        out_specs=(P(None), P('data', 'model'), P(('model', 'data'), None)),
        check_vma=False)
```

```python
import jax
import jax.numpy as jnp
from jax import lax
from jax.experimental import pallas as pl
from jax.experimental.pallas import tpu as pltpu
from jax.sharding import PartitionSpec as P

STEPS = 20
BF = jnp.bfloat16
F32 = jnp.float32
MESH = pl.DeviceIdType.MESH
VMEM_BYTES = 67043328

D = 768
DD = D + D
NTOK = 8192
NOWN = 2048
TB = 1024
SUB = 256
NC = 19
ER = 40
CH = 256
NCH = 3
LAST = NCH - 1
NG = NCH * NCH
FAR = NG - NCH
GR = 32
OWN = CH // GR * 12
LO = slice(D)
HI = slice(D, DD)
SIDES = (LO, HI)
TWO = range(2)
MATES = range(1, 8)
LINE = range(1, 4)
BLOCKS = range(TB // SUB)
NDEV = 32

IN_OTHER = ('', 't0o0', 't1o1i3', 't2o2i4', 's0i5', 's1T3o3')
IN_OWN = ('i6', 's2d0T4o4i7', 'd1i8', 's3T5o5g6')
IN_LOOP = ('s4d2g7', 's5d3g8', 'B6x6d4', 'B7x7d5', 'p6B8x8', 'p7', 'p8', '', '')

G0 = 0.7978845608028654
G1C = 0.044715 * G0


def dot_nn(a, b):
    return lax.dot_general(a, b, (((1,), (0,)), ((), ())), preferred_element_type=F32)


def dot_nt(a, b):
    return lax.dot_general(a, b, (((1,), (1,)), ((), ())), preferred_element_type=F32)


def dot_tn(a, b):
    return lax.dot_general(a, b, (((0,), (0,)), ((), ())), preferred_element_type=F32)


def gelu(x):
    t = jnp.tanh(x * (G0 + G1C * (x * x)))
    h = 0.5 * x
    return h + h * t


def gelu_and_slope(x):
    x2 = x * x
    t = jnp.tanh(x * (G0 + G1C * x2))
    h = 0.5 * x
    u = h + h * t
    s = 0.5 + 0.5 * t + h * (1.0 - t * t) * (G0 + (3.0 * G1C) * x2)
    return u, s


class Place:
    def __init__(self):
        self.z = lax.axis_index('model')
        self.j = lax.axis_index('data')
        self.core = self.j % 2
        self.x = (self.j // 2) % 2
        self.y = self.j // 4
        self.jc = self.j + 1 - 2 * self.core
        self.jx = self.j + 2 - 4 * self.x
        self.jy = self.j + 4 - 8 * self.y
        self.jd = self.jx + 4 - 8 * self.y
        self.js = self.jx + self.core * (self.jy - self.jx)
        self.j2 = self.jx + self.jy - self.js

        self.inner = self.z % 3 > 0
        self.pair = self.z + 1 - 2 * (self.z % 2)
        self.mirror = 3 - self.z
        half = self.z // 2
        self.shares = (self.z, self.pair, 2 - half, 3 - 3 * half)

    def share(self, k):
        own, near, far, end = self.shares
        return jnp.where(k == 0, own, jnp.where(k == 1, near, jnp.where(k == 2, far, end)))


def remote(src, dst, ssem, rsem, z, j):
    return pltpu.make_async_remote_copy(
        src_ref=src, dst_ref=dst, send_sem=ssem, recv_sem=rsem, device_id=(z, j), device_id_type=MESH)


class Scatter:
    def __init__(self, pos, acc, r1, r2, r3, lanes, sems, idx, x_first):
        self.pos, self.acc, self.r1, self.r2, self.r3 = pos, acc, r1, r2, r3
        self.lanes, self.sems, self.idx, self.x_first = lanes, sems, idx, x_first

    def copy(self, stage):
        p, ln = self.pos, self.lanes
        ssem, rsem = self.sems[0].at[stage], self.sems[1].at[self.idx, stage]
        if stage == 0:
            return remote(self.acc.at[:, :, 1 - p.core, :, ln], self.r1.at[:, :, :, ln], ssem, rsem, p.z, p.jc)
        if stage == 1:
            if self.x_first:
                return remote(self.acc.at[:, 1 - p.x, p.core, :, ln], self.r2.at[:, :, ln], ssem, rsem, p.z, p.jx)
            return remote(self.acc.at[1 - p.y, :, p.core, :, ln], self.r2.at[:, :, ln], ssem, rsem, p.z, p.jy)
        if self.x_first:
            return remote(self.acc.at[1 - p.y, p.x, p.core, :, ln], self.r3.at[:, ln], ssem, rsem, p.z, p.jy)
        return remote(self.acc.at[p.y, 1 - p.x, p.core, :, ln], self.r3.at[:, ln], ssem, rsem, p.z, p.jx)

    def start(self):
        self.copy(0).start()

    def side(self):
        p, ln = self.pos, self.lanes
        self.copy(0).wait_recv()
        for yy in TWO:
            for xx in TWO:
                self.acc[yy, xx, p.core, :, ln] += self.r1[yy, xx, :, ln]
        self.copy(1).start()

    def last(self):
        p, ln = self.pos, self.lanes
        self.copy(1).wait_recv()
        for i in TWO:
            if self.x_first:
                self.acc[i, p.x, p.core, :, ln] += self.r2[i, :, ln]
            else:
                self.acc[p.y, i, p.core, :, ln] += self.r2[i, :, ln]
        self.copy(2).start()

    def done(self):
        p, ln = self.pos, self.lanes
        self.copy(2).wait_recv()
        self.acc[p.y, p.x, p.core, :, ln] += self.r3[:, ln]


def main_kernel(x_hbm, w1_hbm, w2_hbm, heads_hbm, lab_hbm,
                a_hbm, sh1_hbm, sh2_hbm, rows_ref,
                dz, wown, acc1, acc2, r1a, r1b, r2a, r2b, r3a, r3b, eall, ast, xbuf, hbd, hcat, heads, lab_v,
                gm, mbuf,
                zss, zrs, zqs, xss, xrs, yss, yrs, dss, drs, css, crs,
                ld_sem, w2_sem, xs_sem, as_sem, ess, efs, ers,
                rss, rsr, mss, mrs, sh_sem):
    pos = Place()
    z, j, inner = pos.z, pos.j, pos.inner
    outer = jnp.logical_not(inner)

    barrier = pltpu.get_barrier_semaphore()
    me = z * 8 + j
    pl.semaphore_signal(barrier, device_id=(pos.pair, j), device_id_type=MESH)

    @pl.when(inner)
    def _():
        pl.semaphore_signal(barrier, device_id=(pos.mirror, j), device_id_type=MESH)

    for jj in (pos.jx, pos.jy, pos.jc):
        pl.semaphore_signal(barrier, device_id=(z, jj), device_id_type=MESH)

    own_x, act, room = dz.at[0], dz.at[2], dz.at[3]
    w1_raw = room.at[LO, LO]
    w1_own = dz.at[4, LO, HI]

    def sub(m):
        return slice((m % 4) * SUB, (m % 4 + 1) * SUB)

    def xo_at(m):
        return own_x.at[sub(m), HI if m >= 4 else LO]

    def share_row(k, b):
        return pl.multiple_of((pos.share(k) * 2 + b) * TB, TB)

    own_row = pl.multiple_of(z * NOWN, NOWN)
    ld_w1 = pltpu.make_async_copy(w1_hbm, w1_raw, ld_sem.at[0])
    ld_x = [pltpu.make_async_copy(x_hbm.at[pl.ds(own_row + b * TB, TB)], own_x.at[:, SIDES[b]], ld_sem.at[1 + b])
            for b in TWO]
    ld_l = pltpu.make_async_copy(lab_hbm.at[:, pl.ds(own_row, NOWN)], lab_v, ld_sem.at[3])
    ld_h = pltpu.make_async_copy(heads_hbm, heads, ld_sem.at[4])
    ld_w2 = [pltpu.make_async_copy(w2_hbm.at[:, c], wown.at[c, :, :, HI], w2_sem.at[c]) for c in range(NCH)]

    def stream_half(i):
        return dz.at[1 + 3 * (i % 2), :, LO]

    def xs_load(i):
        return pltpu.make_async_copy(
            x_hbm.at[pl.ds(share_row(1 + i // 2, i % 2), TB)], stream_half(i), xs_sem.at[i % 2])

    ld_h.start()
    ld_w1.start()
    for cp in ld_w2:
        cp.start()
    xs_load(0).start()
    for cp in ld_x:
        cp.start()
    ld_l.start()

    ld_h.wait()
    hf = jnp.concatenate([heads[i].astype(F32) for i in range(NC)] + [jnp.zeros((2, D), F32)], axis=0)
    hcat[...] = hf.astype(BF)
    r = lax.broadcasted_iota(jnp.int32, (ER, D), 0)
    hb = jnp.concatenate([jnp.where(r % 2 == 0, hf, 0.0), jnp.where(r % 2 == 1, hf, 0.0)], axis=1)
    hbd[...] = jnp.concatenate([hb, hb, hb], axis=0).astype(BF)
    gm[...] = jnp.zeros_like(gm)
    acc1[...] = jnp.zeros_like(acc1)

    ld_w1.wait()
    w1t = w1_raw[...].T
    for c in range(NCH):
        for g in range(8):
            row = g * NCH * GR + c * GR
            wown[c, g, :, LO] = w1t[row:row + GR, :]
    for cp in ld_w2:
        cp.wait()
    pl.semaphore_wait(barrier, 4 + z * pos.mirror // 2)

    def piece(i, jj):
        row = pl.multiple_of((i % NCH) * CH + jj * GR, GR)
        return dz.at[5 + i // NCH, pl.ds(row, GR), :]

    def rows_of(n, ssem, rsem):
        part = dz.at[5, pl.ds(0, n * GR), :]
        return remote(part, part, ssem, rsem, z, pos.jc)

    def z_pair(c):
        return remote(wown.at[c, j], piece(c, j), zss.at[0], zrs.at[c], pos.pair, j)

    def z_mirror(c):
        return remote(wown.at[c, j], piece(NCH + c, j), zss.at[1], zrs.at[NCH + c], pos.mirror, j)

    def z_forward(i):
        first = i < NCH
        to = jnp.where(first, i + 2 * NCH, i)
        return remote(piece(i, j), piece(to, j), zss.at[2], zrs.at[to], jnp.where(first, pos.mirror, pos.pair), j)

    def more_forward(i):
        first = i < NCH
        to = jnp.where(first, i + 2 * NCH, i)
        return remote(piece(i, pos.j2), piece(to, pos.j2), zss.at[3], zqs.at[to - FAR], jnp.where(first, pos.mirror, pos.pair), j)

    def side_copy(i):
        return remote(piece(i, j), piece(i, j), xss, xrs.at[i], z, pos.js)

    def more_copy(i):
        return remote(piece(i, pos.j2), piece(i, pos.j2), dss, drs.at[i], z, pos.js)

    def x_copy(i):
        return remote(piece(i, j), piece(i, j), xss, xrs.at[i], z, pos.jx)

    def y_copy(i):
        return remote(piece(i, j), piece(i, j), yss, yrs.at[i], z, pos.jy)

    def diag_copy_y(i):
        return remote(piece(i, pos.jx), piece(i, pos.jx), dss, drs.at[i], z, pos.jy)

    def diag_copy_x(i):
        return remote(piece(i, pos.jy), piece(i, pos.jy), dss, drs.at[i], z, pos.jx)

    def core_copy(i, q):
        jj = (j, pos.jx, pos.jy, pos.jd)[q]
        return remote(piece(i, jj), piece(i, jj), css.at[i], crs.at[i], z, pos.jc)

    def core_side(i, q):
        jj = (j, pos.js, pos.j2, pos.jd)[q]
        return remote(piece(i, jj), piece(i, jj), css.at[i], crs.at[i], z, pos.jc)

    def take(i):
        remote(piece(i, j), piece(i, j), zss.at[2], zrs.at[i], pos.pair, j).wait_recv()

        @pl.when(inner)
        def _():
            z_forward(i).start()

    def take_more(i):
        remote(piece(i, j), piece(i, j), zss.at[3], zqs.at[i - FAR], pos.pair, j).wait_recv()

        @pl.when(inner)
        def _():
            more_forward(i).start()

    def take_both(i):
        take(i)
        take_more(i)

    def send_both(i):
        side_copy(i).start()
        more_copy(i).start()
        core_side(i, 0).start()
        core_side(i, 2).start()

    def pass_both(i):
        side_copy(i).wait_recv()
        core_side(i, 1).start()
        more_copy(i).wait_recv()
        core_side(i, 3).start()

    def send_own(i):
        x_copy(i).start()
        y_copy(i).start()
        core_copy(i, 0).start()

    def send_side(i):
        x_copy(i).wait_recv()

        @pl.when(pos.core == 0)
        def _():
            diag_copy_y(i).start()

        core_copy(i, 1).start()
        y_copy(i).wait_recv()

        @pl.when(pos.core == 1)
        def _():
            diag_copy_x(i).start()

        core_copy(i, 2).start()

    def send_diag(i):
        diag_copy_y(i).wait_recv()
        core_copy(i, 3).start()

    def side_and_on(i):
        send_side(i)
        if i < NCH:
            @pl.when(inner)
            def _():
                more_forward(i).start()

    def when_inner(f):
        return lambda i: pl.when(inner)(lambda: f(i))

    def when_outer(f):
        return lambda i: pl.when(outer)(lambda: f(i))

    kinds = {'t': take, 'T': when_outer(take), 'i': when_inner(take), 'o': send_own, 's': side_and_on, 'd': send_diag,
             'g': when_inner(take_more), 'B': when_outer(take_both), 'x': send_both, 'p': pass_both}

    def events(codes):
        for kind, i in zip(codes[::2], codes[1::2]):
            kinds[kind](int(i))

    def events_at(i, table):
        for n, codes in enumerate(table):
            if codes:
                pl.when(i == n)(lambda codes=codes: events(codes))

    for c in range(NCH):
        z_pair(c).start()

    @pl.when(inner)
    def _():
        for c in range(NCH):
            z_mirror(c).start()

    acc2[...] = jnp.zeros_like(acc2)

    def a_store(src, c, row, sem):
        return pltpu.make_async_copy(src, a_hbm.at[c, pl.ds(pl.multiple_of(row, TB), TB)], as_sem.at[sem])

    def forward(facc, u_own, w1_nat, w2_nat):
        for c in range(NCH):
            w1_own[:, c * CH:(c + 1) * CH] = wown[c, :, :, LO].reshape(CH, D).T

        def staged(i, c):
            rows = pl.ds(pl.multiple_of((i % 2) * TB, TB), TB)
            return a_store(facc.at[rows, c * CH:(c + 1) * CH], c, share_row(1 + i // 2, i % 2), (i % 2) * NCH + c)

        def other_tokens(i, carry):
            xs_load(i).wait()

            @pl.when(i < 5)
            def _():
                xs_load(i + 1).start()

            @pl.when(i >= 2)
            def _():
                for c in range(NCH):
                    staged(i, c).wait()

            base = (i % 2) * TB
            for m in BLOCKS:
                rows = pl.ds(pl.multiple_of(base + m * SUB, SUB), SUB)
                facc[rows, :] = dot_nn(stream_half(i)[sub(m), :], w1_own[...])
            for c in range(NCH):
                staged(i, c).start()

            events_at(i, IN_OTHER)
            return carry

        lax.fori_loop(0, 6, other_tokens, 0)
        for cp in ld_x:
            cp.wait()

        for b in TWO:
            for c in range(NCH):
                staged(b, c).wait()
            for m in BLOCKS:
                a = dot_nn(xo_at(b * 4 + m)[...], w1_own[...])
                for c in range(NCH):
                    ast[c, sub(m), :] = a[:, c * CH:(c + 1) * CH]
                act[sub(m), LO] = gelu(a).astype(BF)
            events(IN_OWN[2 * b])
            for m in BLOCKS:
                facc[b * TB + m * SUB:b * TB + (m + 1) * SUB, :] = dot_nn(
                    act[sub(m), LO], wown[:, :, :, HI].reshape(D, D))
            for c in range(NCH):
                a_store(ast.at[c], c, (z * 2 + b) * TB, c).start()
            events(IN_OWN[2 * b + 1])
            if b == 0:
                for c in range(NCH):
                    a_store(ast.at[c], c, z * NOWN, c).wait()

        def granule(n, carry):
            rows_of(4, css.at[n], crs.at[n]).wait_recv()
            gran = dz.at[5 + n // NCH, pl.ds(pl.multiple_of((n % NCH) * CH, CH), CH), :]
            w1_nat[...] = gran[:, LO].T
            w2_nat[...] = gran[:, HI]
            for m in range(8):
                u_own[m * SUB:(m + 1) * SUB, :] = gelu(dot_nn(xo_at(m)[...], w1_nat[...])).astype(BF)
            for m in range(8):
                rows = slice(m * SUB, (m + 1) * SUB)
                facc[rows, :] += dot_nn(u_own[rows, :], w2_nat[...])

            events_at(n, IN_LOOP)

            return carry

        lax.fori_loop(0, NG, granule, 0)
        for m in range(8):
            xo_at(m)[...] = (xo_at(m)[...].astype(F32) + facc[m * SUB:(m + 1) * SUB, :]).astype(BF)

    pl.run_scoped(forward, pltpu.VMEM((NOWN, D), F32), pltpu.VMEM((NOWN, CH), BF), pltpu.VMEM((D, CH), BF),
                  pltpu.VMEM((CH, D), BF))

    for c in range(NCH):
        a_store(ast.at[c], c, z * NOWN, c).wait()

    def e_half(k, b):
        return eall.at[k, :, pl.ds(pl.multiple_of(b * TB, TB), TB)]

    def e_pair(b):
        return remote(e_half(0, b), e_half(1, b), ess.at[0, b], ers.at[1, b], pos.pair, j)

    def e_mirror(b):
        return remote(e_half(0, b), e_half(2, b), ess.at[1, b], ers.at[2, b], pos.mirror, j)

    def e_forward(k, b):
        to = 3 if k == 1 else k
        return remote(e_half(k, b), e_half(to, b), efs.at[k, b], ers.at[to, b], pos.mirror if k == 1 else pos.pair, j)

    def e_wait(k, b):
        remote(e_half(k, b), e_half(k, b), efs.at[k, b], ers.at[k, b], pos.pair, j).wait_recv()

    def step_of(s):
        return s // 8, (s % 8) // 2, s % 2

    def a_load(s):
        c, k, b = step_of(s)
        return pltpu.make_async_copy(a_hbm.at[c, pl.ds(share_row(k, b), TB)], ast.at[s % 2], as_sem.at[s % 2])

    def x_load(s):
        c, k, b = step_of(s)
        return pltpu.make_async_copy(x_hbm.at[pl.ds(share_row(k, b), TB)], xbuf.at[s % 2], xs_sem.at[s % 2])

    a_load(0).start()
    x_load(0).start()

    ld_l.wait()
    r = lax.broadcasted_iota(jnp.int32, (ER, TB), 0)
    first = r % 2 == 0
    real = r < 2 * NC
    neg = jnp.float32(-jnp.inf)
    for b in TWO:
        cols = slice(b * TB, (b + 1) * TB)
        logit = jnp.where(real, dot_nt(hcat[...], own_x[:, SIDES[b]]), neg)
        m0 = jnp.max(jnp.where(first, logit, neg), axis=0, keepdims=True)
        m1 = jnp.max(jnp.where(first, neg, logit), axis=0, keepdims=True)
        ex = jnp.exp(logit - jnp.where(first, m0, m1))
        s0 = jnp.sum(jnp.where(first, ex, 0.0), axis=0, keepdims=True)
        s1 = jnp.sum(jnp.where(first, 0.0, ex), axis=0, keepdims=True)
        prob = ex / jnp.where(first, s0, s1)
        lab = jnp.where(first, lab_v[0:1, cols], lab_v[1:2, cols])
        hot = jnp.where(jnp.logical_and(r // 2 == lab, real), 1.0, 0.0)
        eall[0, :, cols] = (prob - hot) / (NTOK * 8.0)
        e_pair(b).start()

        @pl.when(inner)
        def _():
            e_mirror(b).start()

    rows_of(NG, xss, xrs.at[0]).wait_send()
    rows_of(FAR, yss, yrs.at[0]).wait_send()
    rows_of(NG, dss, drs.at[0]).wait_send()
    for i in range(NG):
        rows_of(4, css.at[i], crs.at[i]).wait_send()
    rows_of(NCH, zss.at[0], zrs.at[0]).wait_send()

    @pl.when(inner)
    def _():
        for n, i in ((NCH, 1), (NG, 2), (FAR, 3)):
            rows_of(n, zss.at[i], zrs.at[0]).wait_send()

    everything = slice(None)
    up_sems, down_sems = (rss.at[0], rsr), (rss.at[1], rsr)

    def up(c, t):
        return Scatter(pos, acc1.at[c, t], r1a.at[c, t], r2a.at[c, t], r3a.at[c, t], everything, up_sems,
                       c * 6 + t, t == 0)

    def down(c, t, part=None):
        if part is None:
            lanes, idx, x_first = everything, c * 6 + 2 + t, t == 0
        else:
            lanes, idx, x_first = slice(part * (D // 2), (part + 1) * (D // 2)), c * 6 + 2 + t * 2 + part, part == 0
        return Scatter(pos, acc2.at[c, t], r1b.at[c, t], r2b.at[c, t], r3b.at[c, t], lanes, down_sems, idx, x_first)

    ups = [[up(c, t) for t in TWO] for c in range(NCH)]
    downs = [[down(c, t) for t in TWO] for c in range(LAST)]
    tails = [[down(LAST, t, part) for part in TWO] for t in TWO]

    def each(group, stage):
        for sc in group:
            getattr(sc, stage)()

    def fold(v):
        rows, cols = v.shape
        total = jnp.zeros((8, 128), F32)
        for q in range(cols // 128):
            total = total + jnp.sum(v[:, q * 128:(q + 1) * 128].reshape(rows // 8, 8, 128), axis=0)
        return total

    def shard(acc, c, t):
        return acc.at[c, t, pos.y, pos.x, pos.core]

    def out_copy(acc, out, c, sem, t):
        return pltpu.make_async_copy(shard(acc, c, t), out.at[c, t], sh_sem.at[sem])

    def finish(acc, out, c, sem):
        v0, v1 = shard(acc, c, 0)[...], shard(acc, c, 1)[...]
        gm[0] += fold(v0 * v0)
        gm[1] += fold(v0 * v1)
        gm[2] += fold(v1 * v1)
        for t in TWO:
            out_copy(acc, out, c, sem, t).start()

    def finish_chunk(c):
        each(ups[c] + downs[c], 'done')
        finish(acc1, sh1_hbm, c, 0)
        finish(acc2, sh2_hbm, c, 1)

    def backward(us_all, das):
        def prepare(s):
            a_load(s).wait()
            x_load(s).wait()

            @pl.when(s < 23)
            def _():
                a_load(s + 1).start()
                x_load(s + 1).start()

        def d_act(s, m, us):
            c, k, b = step_of(s)
            w2c = wown[c, :, :, HI].reshape(CH, D)
            u, slope = gelu_and_slope(ast[s % 2, sub(m), :])
            us[sub(m), :] = u.astype(BF)
            for task in TWO:
                da = dot_nt(dz[k * 2 + b, sub(m), SIDES[task]], w2c)
                das[sub(m), task * CH:(task + 1) * CH] = (da * slope).astype(BF)

        def add_up(s):
            c, _, _ = step_of(s)
            g = dot_tn(xbuf[s % 2], das[...])
            for task in TWO:
                acc1[c, task] += g[:, task * CH:(task + 1) * CH].reshape(acc1.shape[2:])

        def e_parts(s):
            _, k, b = step_of(s)
            e = e_half(k, b)[...]
            e1 = e.astype(BF).astype(F32)
            rest = e - e1
            e2 = rest.astype(BF).astype(F32)
            e3 = rest - e2
            return jnp.concatenate([e1, e2, e3], axis=0).astype(BF)

        def grads(s, us):
            c, k, b = step_of(s)
            add_up(s)
            g = dot_tn(us[...], dz[k * 2 + b])
            for task in TWO:
                acc2[c, task] += g[:, SIDES[task]].reshape(acc2.shape[2:])

        def first_step(s, carry):
            _, k, b = step_of(s)
            prepare(s)

            @pl.when(jnp.logical_and(outer, k > 0))
            def _():
                e_wait(k, b)

            us = us_all.at[0]
            es = e_parts(s)

            def fill(m):
                dz[k * 2 + b, sub(m), :] = dot_tn(es[:, sub(m)], hbd[...]).astype(BF)

            for m in BLOCKS:
                fill(m)
            for m in BLOCKS:
                d_act(s, m, us)
            grads(s, us)

            for when, k_f, b_f in ((1, 1, 0), (1, 2, 0), (2, 1, 1), (2, 2, 1), (3, 3, 0), (4, 3, 1)):
                @pl.when(jnp.logical_and(s == when, inner))
                def _():
                    e_forward_after_wait(k_f, b_f)

            return carry

        def step(s, carry):
            us = us_all.at[0]
            prepare(s)
            for m in BLOCKS:
                d_act(s, m, us)
            grads(s, us)

            @pl.when(s == 9)
            def _():
                each(ups[0] + downs[0], 'side')

            @pl.when(s == 12)
            def _():
                each(ups[0], 'last')

            @pl.when(s == 13)
            def _():
                each(downs[0], 'last')

            return carry

        def e_forward_after_wait(k, b):
            e_wait(k, b)
            e_forward(k, b).start()

        lax.fori_loop(0, 8, first_step, 0)
        each(ups[0] + downs[0], 'start')
        lax.fori_loop(8, 16, step, 0)
        each(ups[1] + downs[1], 'start')

        def last_step(s, carry):
            c, k, b = step_of(s)
            prepare(s)
            for m in BLOCKS:
                d_act(s, m, us_all.at[k * 2 + b])
            add_up(s)

            @pl.when(s == 16)
            def _():
                finish_chunk(0)

            @pl.when(s == 17)
            def _():
                each(ups[1], 'side')

            @pl.when(s == 19)
            def _():
                each(downs[1], 'side')

            @pl.when(s == 20)
            def _():
                each(ups[1], 'last')

            return carry

        lax.fori_loop(16, 24, last_step, 0)
        each(ups[LAST], 'start')
        each(downs[1], 'last')

        def down_pass(task):
            def two_blocks(i, carry):
                lanes = SIDES[task]
                g = dot_tn(us_all[i * 2], dz[i * 2, :, lanes])
                g = g + dot_tn(us_all[i * 2 + 1], dz[i * 2 + 1, :, lanes])
                acc2[LAST, task] += g.reshape(acc2.shape[2:])

                @pl.when(i == 1)
                def _():
                    each(ups[LAST] if task == 0 else tails[0], 'side')

                return carry

            lax.fori_loop(0, 4, two_blocks, 0)
            each(tails[task], 'start')

        down_pass(0)
        finish_chunk(1)
        down_pass(1)

    pl.run_scoped(backward, pltpu.VMEM((8, TB, CH), BF), pltpu.VMEM((TB, 2 * CH), BF))

    each(ups[LAST], 'last')
    each(tails[1], 'side')
    each(tails[0], 'last')
    each(ups[LAST], 'done')
    finish(acc1, sh1_hbm, LAST, 0)
    each(tails[1], 'last')
    each(tails[0], 'done')
    each(tails[1], 'done')
    finish(acc2, sh2_hbm, LAST, 1)

    def full(v):
        return jnp.sum(jnp.sum(v, axis=0, keepdims=True), axis=1, keepdims=True)

    lane = lax.broadcasted_iota(jnp.int32, (1, 128), 1)
    mbuf[pl.ds(me, 1), :] = jnp.where(lane == 0, full(gm[0]), jnp.where(lane == 1, full(gm[1]), full(gm[2])))

    def m_copy(i):
        to = (me + i) % NDEV
        line = mbuf.at[pl.ds(me, 1), :]
        return remote(line, line, mss, mrs, to // 8, to % 8)

    def m_start(i, carry):
        m_copy(i).start()
        return carry

    lax.fori_loop(1, NDEV, m_start, 0)

    for b in TWO:
        e_pair(b).wait_send()

        @pl.when(inner)
        def _():
            e_mirror(b).wait_send()
            for k in LINE:
                e_forward(k, b).wait_send()

    for kind, all_stages in enumerate(((r1a, r2a, r3a), (r1b, r2b, r3b))):
        for stage, buf in enumerate(all_stages):
            remote(buf, buf, rss.at[kind, stage], rsr.at[0, stage], z, pos.jc).wait_send()
    pltpu.make_async_copy(r3a, sh1_hbm, sh_sem.at[0]).wait()
    pltpu.make_async_copy(r3b, sh2_hbm, sh_sem.at[1]).wait()

    lines = mbuf.at[pl.ds(0, NDEV - 1), :]
    remote(lines, lines, mss, mrs, z, pos.jc).wait()
    rows_ref[...] = mbuf[...]


def main_call(x, w1, w2r, heads, labels):
    dma = pltpu.SemaphoreType.DMA
    anyspec = pl.BlockSpec(memory_space=pl.ANY)
    vspec = pl.BlockSpec(memory_space=pltpu.VMEM)
    up, down = (OWN, CH), (GR, D)
    pair, quad, octet = (2,), (2, 2), (2, 2, 2)
    per_chunk = (NCH, 2)
    vmem = pltpu.VMEM
    return pl.pallas_call(
        main_kernel,
        out_shape=(jax.ShapeDtypeStruct((NCH, NTOK, CH), F32),
                   jax.ShapeDtypeStruct(per_chunk + up, F32),
                   jax.ShapeDtypeStruct(per_chunk + down, F32),
                   jax.ShapeDtypeStruct((NDEV, 128), F32)),
        in_specs=[anyspec] * 5,
        out_specs=(anyspec, anyspec, anyspec, vspec),
        scratch_shapes=[
            vmem((8, TB, DD), BF),
            vmem((NCH, 8, GR, DD), BF),
            vmem(per_chunk + octet + up, F32), vmem(per_chunk + octet + down, F32),
            vmem(per_chunk + quad + up, F32), vmem(per_chunk + quad + down, F32),
            vmem(per_chunk + pair + up, F32), vmem(per_chunk + pair + down, F32),
            vmem(per_chunk + up, F32), vmem(per_chunk + down, F32),
            vmem((4, ER, NOWN), F32),
            vmem((NCH, TB, CH), F32),
            vmem((2, TB, D), BF),
            vmem((3 * ER, DD), BF),
            vmem((ER, D), BF),
            vmem((NC, 2, D), BF),
            vmem((2, NOWN), jnp.int32),
            vmem((3, 8, 128), F32), vmem((NDEV, 128), F32),
            dma((4,)), dma((NG,)), dma((NCH,)), dma(()), dma((NG,)), dma(()), dma((FAR,)), dma(()), dma((NG,)), dma((NG,)), dma((NG,)),
            dma((5,)), dma((NCH,)), dma(pair), dma((6,)), dma(quad), dma((4, 2)), dma((4, 2)),
            dma((2, NCH)), dma((6 * NCH, NCH)), dma(()), dma(()), dma(pair),
        ],
        compiler_params=pltpu.CompilerParams(
            collective_id=0, has_side_effects=True, vmem_limit_bytes=VMEM_BYTES),
        name='main',
    )(x, w1, w2r, heads, labels)


def result_kernel(rows_hbm, sh1_hbm, sh2_hbm, a_ref, g1_ref, g2_ref, rows, sh1, sh2, sem):
    ld_rows = pltpu.make_async_copy(rows_hbm, rows, sem.at[0])
    loads = [pltpu.make_async_copy(sh1_hbm, sh1, sem.at[1]), pltpu.make_async_copy(sh2_hbm, sh2, sem.at[2])]
    ld_rows.start()
    for cp in loads:
        cp.start()
    ld_rows.wait()

    gram = jnp.sum(rows[...], axis=0, keepdims=True)
    lane = lax.broadcasted_iota(jnp.int32, gram.shape, 1)

    def entry(i):
        return jnp.sum(jnp.where(lane == i, gram, 0.0), axis=1, keepdims=True)

    g00, g01, g11 = entry(0), entry(1), entry(2)
    scale = (g00 + g11) / 2.0

    def eg_step(i, weights):
        a0, a1 = weights
        v0 = a0 * jnp.exp(-(g00 * a0 + g01 * a1) / scale)
        v1 = a1 * jnp.exp(-(g01 * a0 + g11 * a1) / scale)
        tot = v0 + v1
        return v0 / tot, v1 / tot

    half = jnp.full((1, 1), 0.5, F32)
    a0, a1 = lax.fori_loop(0, STEPS, eg_step, (half, half))
    a_ref[0] = a0[0, 0]
    a_ref[1] = a1[0, 0]
    for cp in loads:
        cp.wait()
    for c in range(NCH):
        comb = a0 * sh1[c, 0] + a1 * sh1[c, 1]
        for g in range(8):
            col = g * NCH * GR + c * GR
            g1_ref[:, col:col + GR] = comb[:, g * GR:(g + 1) * GR]
        g2_ref[c * GR:(c + 1) * GR, :] = a0 * sh2[c, 0] + a1 * sh2[c, 1]


def result_call(rows, sh1, sh2):
    vspec = pl.BlockSpec(memory_space=pltpu.VMEM)
    anyspec = pl.BlockSpec(memory_space=pl.ANY)
    return pl.pallas_call(
        result_kernel,
        out_shape=(jax.ShapeDtypeStruct((2,), F32), jax.ShapeDtypeStruct((OWN, D), F32),
                   jax.ShapeDtypeStruct((OWN, D), F32)),
        in_specs=[anyspec] * NCH,
        out_specs=(pl.BlockSpec(memory_space=pltpu.SMEM), vspec, vspec),
        scratch_shapes=[pltpu.VMEM(v.shape, F32) for v in (rows, sh1, sh2)] + [pltpu.SemaphoreType.DMA((NCH,))],
        name='result',
    )(rows, sh1, sh2)


def solution(mesh):
    def local_step(tokens, w_up, w_down, task_heads, labels):
        w2r = w_down.reshape(8, NCH, GR, D)
        heads = jnp.transpose(task_heads, (2, 0, 1))
        _, sh1, sh2, rows = main_call(tokens, w_up, w2r, heads, labels)
        return result_call(rows, sh1, sh2)

    return jax.shard_map(
        local_step, mesh=mesh,
        in_specs=(P('data', None), P(None, 'model'), P('model', None), P(None, None, None), P(None, 'data')),
        out_specs=(P(None), P('data', 'model'), P(('model', 'data'), None)),
        check_vma=False)
```

```python
import jax
import jax.numpy as jnp
from jax import lax
from jax.experimental import pallas as pl
from jax.experimental.pallas import tpu as pltpu
from jax.sharding import PartitionSpec as P

STEPS = 20
BF = jnp.bfloat16
F32 = jnp.float32
MESH = pl.DeviceIdType.MESH
VMEM_BYTES = 67043328

D = 768
DD = D + D
NTOK = 8192
NOWN = 2048
TB = 1024
SUB = 256
NC = 19
ER = 40
CH = 256
NCH = 3
LAST = NCH - 1
NG = NCH * NCH
FAR = NG - NCH
GR = 32
OWN = CH // GR * 12
LO = slice(D)
HI = slice(D, DD)
SIDES = (LO, HI)
TWO = range(2)
MATES = range(1, 8)
LINE = range(1, 4)
BLOCKS = range(TB // SUB)
NDEV = 32

IN_OTHER = ('', 't0o0', 't1o1i3', 't2o2i4', 's0i5', 's1T3o3')
IN_OWN = ('i6', 's2d0T4o4i7', 'd1i8', 's3T5o5g6')
IN_LOOP = ('d2g7s4', 'd3g8', 's5B6x6d4', 'B7x7', 'd5p6B8x8', 'p7', 'p8', '', '')

G0 = 0.7978845608028654
G1C = 0.044715 * G0


def dot_nn(a, b):
    return lax.dot_general(a, b, (((1,), (0,)), ((), ())), preferred_element_type=F32)


def dot_nt(a, b):
    return lax.dot_general(a, b, (((1,), (1,)), ((), ())), preferred_element_type=F32)


def dot_tn(a, b):
    return lax.dot_general(a, b, (((0,), (0,)), ((), ())), preferred_element_type=F32)


def gelu(x):
    t = jnp.tanh(x * (G0 + G1C * (x * x)))
    h = 0.5 * x
    return h + h * t


def gelu_and_slope(x):
    x2 = x * x
    t = jnp.tanh(x * (G0 + G1C * x2))
    h = 0.5 * x
    u = h + h * t
    s = 0.5 + 0.5 * t + h * (1.0 - t * t) * (G0 + (3.0 * G1C) * x2)
    return u, s


class Place:
    def __init__(self):
        self.z = lax.axis_index('model')
        self.j = lax.axis_index('data')
        self.core = self.j % 2
        self.x = (self.j // 2) % 2
        self.y = self.j // 4
        self.jc = self.j + 1 - 2 * self.core
        self.jx = self.j + 2 - 4 * self.x
        self.jy = self.j + 4 - 8 * self.y
        self.jd = self.jx + 4 - 8 * self.y
        self.js = self.jx + self.core * (self.jy - self.jx)
        self.j2 = self.jx + self.jy - self.js

        self.inner = self.z % 3 > 0
        self.pair = self.z + 1 - 2 * (self.z % 2)
        self.mirror = 3 - self.z
        half = self.z // 2
        self.shares = (self.z, self.pair, 2 - half, 3 - 3 * half)

    def share(self, k):
        own, near, far, end = self.shares
        return jnp.where(k == 0, own, jnp.where(k == 1, near, jnp.where(k == 2, far, end)))


def remote(src, dst, ssem, rsem, z, j):
    return pltpu.make_async_remote_copy(
        src_ref=src, dst_ref=dst, send_sem=ssem, recv_sem=rsem, device_id=(z, j), device_id_type=MESH)


class Scatter:
    def __init__(self, pos, acc, r1, r2, r3, lanes, sems, idx, x_first):
        self.pos, self.acc, self.r1, self.r2, self.r3 = pos, acc, r1, r2, r3
        self.lanes, self.sems, self.idx, self.x_first = lanes, sems, idx, x_first

    def copy(self, stage):
        p, ln = self.pos, self.lanes
        ssem, rsem = self.sems[0].at[stage], self.sems[1].at[self.idx, stage]
        if stage == 0:
            return remote(self.acc.at[:, :, 1 - p.core, :, ln], self.r1.at[:, :, :, ln], ssem, rsem, p.z, p.jc)
        if stage == 1:
            if self.x_first:
                return remote(self.acc.at[:, 1 - p.x, p.core, :, ln], self.r2.at[:, :, ln], ssem, rsem, p.z, p.jx)
            return remote(self.acc.at[1 - p.y, :, p.core, :, ln], self.r2.at[:, :, ln], ssem, rsem, p.z, p.jy)
        if self.x_first:
            return remote(self.acc.at[1 - p.y, p.x, p.core, :, ln], self.r3.at[:, ln], ssem, rsem, p.z, p.jy)
        return remote(self.acc.at[p.y, 1 - p.x, p.core, :, ln], self.r3.at[:, ln], ssem, rsem, p.z, p.jx)

    def start(self):
        self.copy(0).start()

    def side(self):
        p, ln = self.pos, self.lanes
        self.copy(0).wait_recv()
        for yy in TWO:
            for xx in TWO:
                self.acc[yy, xx, p.core, :, ln] += self.r1[yy, xx, :, ln]
        self.copy(1).start()

    def last(self):
        p, ln = self.pos, self.lanes
        self.copy(1).wait_recv()
        for i in TWO:
            if self.x_first:
                self.acc[i, p.x, p.core, :, ln] += self.r2[i, :, ln]
            else:
                self.acc[p.y, i, p.core, :, ln] += self.r2[i, :, ln]
        self.copy(2).start()

    def done(self):
        p, ln = self.pos, self.lanes
        self.copy(2).wait_recv()
        self.acc[p.y, p.x, p.core, :, ln] += self.r3[:, ln]


def main_kernel(x_hbm, w1_hbm, w2_hbm, heads_hbm, lab_hbm,
                a_hbm, sh1_hbm, sh2_hbm, rows_ref,
                dz, wown, acc1, acc2, r1a, r1b, r2a, r2b, r3a, r3b, eall, ast, hbd, hcat, heads, lab_v,
                gm, mbuf,
                zss, zrs, zqs, xss, xrs, yss, yrs, dss, drs, css, crs,
                ld_sem, w2_sem, xs_sem, as_sem, ess, efs, ers,
                rss, rsr, mss, mrs, sh_sem):
    pos = Place()
    z, j, inner = pos.z, pos.j, pos.inner
    outer = jnp.logical_not(inner)

    barrier = pltpu.get_barrier_semaphore()
    me = z * 8 + j
    pl.semaphore_signal(barrier, device_id=(pos.pair, j), device_id_type=MESH)

    @pl.when(inner)
    def _():
        pl.semaphore_signal(barrier, device_id=(pos.mirror, j), device_id_type=MESH)

    for jj in (pos.jx, pos.jy, pos.jc):
        pl.semaphore_signal(barrier, device_id=(z, jj), device_id_type=MESH)

    own_x, act, room = dz.at[0], dz.at[2], dz.at[3]
    w1_raw = room.at[LO, LO]
    w1_own = dz.at[4, LO, HI]

    def sub(m):
        return slice((m % 4) * SUB, (m % 4 + 1) * SUB)

    def xo_at(m):
        return own_x.at[sub(m), HI if m >= 4 else LO]

    def share_row(k, b):
        return pl.multiple_of((pos.share(k) * 2 + b) * TB, TB)

    own_row = pl.multiple_of(z * NOWN, NOWN)
    ld_w1 = pltpu.make_async_copy(w1_hbm, w1_raw, ld_sem.at[0])
    ld_x = [pltpu.make_async_copy(x_hbm.at[pl.ds(own_row + b * TB, TB)], own_x.at[:, SIDES[b]], ld_sem.at[1 + b])
            for b in TWO]
    ld_l = pltpu.make_async_copy(lab_hbm.at[:, pl.ds(own_row, NOWN)], lab_v, ld_sem.at[3])
    ld_h = pltpu.make_async_copy(heads_hbm, heads, ld_sem.at[4])
    ld_w2 = [pltpu.make_async_copy(w2_hbm.at[:, c], wown.at[c, :, :, HI], w2_sem.at[c]) for c in range(NCH)]

    def stream_half(i):
        return dz.at[1 + 3 * (i % 2), :, LO]

    def xs_load(i):
        return pltpu.make_async_copy(
            x_hbm.at[pl.ds(share_row(1 + i // 2, i % 2), TB)], stream_half(i), xs_sem.at[i % 2])

    ld_h.start()
    ld_w1.start()
    for cp in ld_w2:
        cp.start()
    xs_load(0).start()
    for cp in ld_x:
        cp.start()
    ld_l.start()

    ld_h.wait()
    hf = jnp.concatenate([heads[i].astype(F32) for i in range(NC)] + [jnp.zeros((2, D), F32)], axis=0)
    hcat[...] = hf.astype(BF)
    r = lax.broadcasted_iota(jnp.int32, (ER, D), 0)
    hb = jnp.concatenate([jnp.where(r % 2 == 0, hf, 0.0), jnp.where(r % 2 == 1, hf, 0.0)], axis=1)
    hbd[...] = jnp.concatenate([hb, hb, hb], axis=0).astype(BF)
    gm[...] = jnp.zeros_like(gm)
    acc1[...] = jnp.zeros_like(acc1)

    ld_w1.wait()
    w1t = w1_raw[...].T
    for c in range(NCH):
        for g in range(8):
            row = g * NCH * GR + c * GR
            wown[c, g, :, LO] = w1t[row:row + GR, :]
    for cp in ld_w2:
        cp.wait()
    pl.semaphore_wait(barrier, 4 + z * pos.mirror // 2)

    def piece(i, jj):
        row = pl.multiple_of((i % NCH) * CH + jj * GR, GR)
        return dz.at[5 + i // NCH, pl.ds(row, GR), :]

    def rows_of(n, ssem, rsem):
        part = dz.at[5, pl.ds(0, n * GR), :]
        return remote(part, part, ssem, rsem, z, pos.jc)

    def z_pair(c):
        return remote(wown.at[c, j], piece(c, j), zss.at[0], zrs.at[c], pos.pair, j)

    def z_mirror(c):
        return remote(wown.at[c, j], piece(NCH + c, j), zss.at[1], zrs.at[NCH + c], pos.mirror, j)

    def z_forward(i):
        first = i < NCH
        to = jnp.where(first, i + 2 * NCH, i)
        return remote(piece(i, j), piece(to, j), zss.at[2], zrs.at[to], jnp.where(first, pos.mirror, pos.pair), j)

    def more_forward(i):
        first = i < NCH
        to = jnp.where(first, i + 2 * NCH, i)
        return remote(piece(i, pos.j2), piece(to, pos.j2), zss.at[3], zqs.at[to - FAR], jnp.where(first, pos.mirror, pos.pair), j)

    def side_copy(i):
        return remote(piece(i, j), piece(i, j), xss, xrs.at[i], z, pos.js)

    def more_copy(i):
        return remote(piece(i, pos.j2), piece(i, pos.j2), dss, drs.at[i], z, pos.js)

    def x_copy(i):
        return remote(piece(i, j), piece(i, j), xss, xrs.at[i], z, pos.jx)

    def y_copy(i):
        return remote(piece(i, j), piece(i, j), yss, yrs.at[i], z, pos.jy)

    def diag_copy_y(i):
        return remote(piece(i, pos.jx), piece(i, pos.jx), dss, drs.at[i], z, pos.jy)

    def diag_copy_x(i):
        return remote(piece(i, pos.jy), piece(i, pos.jy), dss, drs.at[i], z, pos.jx)

    def core_copy(i, q):
        jj = (j, pos.jx, pos.jy, pos.jd)[q]
        return remote(piece(i, jj), piece(i, jj), css.at[i], crs.at[i], z, pos.jc)

    def core_side(i, q):
        jj = (j, pos.js, pos.j2, pos.jd)[q]
        return remote(piece(i, jj), piece(i, jj), css.at[i], crs.at[i], z, pos.jc)

    def take(i):
        remote(piece(i, j), piece(i, j), zss.at[2], zrs.at[i], pos.pair, j).wait_recv()

        @pl.when(inner)
        def _():
            z_forward(i).start()

    def take_more(i):
        remote(piece(i, j), piece(i, j), zss.at[3], zqs.at[i - FAR], pos.pair, j).wait_recv()

        @pl.when(inner)
        def _():
            more_forward(i).start()

    def take_both(i):
        take(i)
        take_more(i)

    def send_both(i):
        side_copy(i).start()
        more_copy(i).start()
        core_side(i, 0).start()
        core_side(i, 2).start()

    def pass_both(i):
        side_copy(i).wait_recv()
        core_side(i, 1).start()
        more_copy(i).wait_recv()
        core_side(i, 3).start()

    def send_own(i):
        x_copy(i).start()
        y_copy(i).start()
        core_copy(i, 0).start()

    def send_side(i):
        x_copy(i).wait_recv()

        @pl.when(pos.core == 0)
        def _():
            diag_copy_y(i).start()

        core_copy(i, 1).start()
        y_copy(i).wait_recv()

        @pl.when(pos.core == 1)
        def _():
            diag_copy_x(i).start()

        core_copy(i, 2).start()

    def send_diag(i):
        diag_copy_y(i).wait_recv()
        core_copy(i, 3).start()

    def side_and_on(i):
        send_side(i)
        if i < NCH:
            @pl.when(inner)
            def _():
                more_forward(i).start()

    def when_inner(f):
        return lambda i: pl.when(inner)(lambda: f(i))

    def when_outer(f):
        return lambda i: pl.when(outer)(lambda: f(i))

    kinds = {'t': take, 'T': when_outer(take), 'i': when_inner(take), 'o': send_own, 's': side_and_on, 'd': send_diag,
             'g': when_inner(take_more), 'B': when_outer(take_both), 'x': send_both, 'p': pass_both}

    def events(codes):
        for kind, i in zip(codes[::2], codes[1::2]):
            kinds[kind](int(i))

    def events_at(i, table):
        for n, codes in enumerate(table):
            if codes:
                pl.when(i == n)(lambda codes=codes: events(codes))

    for c in range(NCH):
        z_pair(c).start()

    @pl.when(inner)
    def _():
        for c in range(NCH):
            z_mirror(c).start()

    def a_store(src, c, row, sem):
        return pltpu.make_async_copy(src, a_hbm.at[c, pl.ds(pl.multiple_of(row, TB), TB)], as_sem.at[sem])

    def forward(facc, u_own, w1_nat, w2_nat):
        for c in range(NCH):
            w1_own[:, c * CH:(c + 1) * CH] = wown[c, :, :, LO].reshape(CH, D).T

        def staged(i, c):
            rows = pl.ds(pl.multiple_of((i % 2) * TB, TB), TB)
            return a_store(facc.at[rows, c * CH:(c + 1) * CH], c, share_row(1 + i // 2, i % 2), (i % 2) * NCH + c)

        def other_tokens(i, carry):
            xs_load(i).wait()

            @pl.when(i < 5)
            def _():
                xs_load(i + 1).start()

            @pl.when(i >= 2)
            def _():
                for c in range(NCH):
                    staged(i, c).wait()

            base = (i % 2) * TB
            for m in BLOCKS:
                rows = pl.ds(pl.multiple_of(base + m * SUB, SUB), SUB)
                facc[rows, :] = dot_nn(stream_half(i)[sub(m), :], w1_own[...])
            for c in range(NCH):
                staged(i, c).start()

            events_at(i, IN_OTHER)
            return carry

        lax.fori_loop(0, 6, other_tokens, 0)
        for cp in ld_x:
            cp.wait()

        for b in TWO:
            for c in range(NCH):
                staged(b, c).wait()
            for m in BLOCKS:
                a = dot_nn(xo_at(b * 4 + m)[...], w1_own[...])
                for c in range(NCH):
                    ast[c, sub(m), :] = a[:, c * CH:(c + 1) * CH]
                act[sub(m), LO] = gelu(a).astype(BF)
            events(IN_OWN[2 * b])
            for m in BLOCKS:
                facc[b * TB + m * SUB:b * TB + (m + 1) * SUB, :] = dot_nn(
                    act[sub(m), LO], wown[:, :, :, HI].reshape(D, D))
            for c in range(NCH):
                a_store(ast.at[c], c, (z * 2 + b) * TB, c).start()
            events(IN_OWN[2 * b + 1])
            if b == 0:
                for c in range(NCH):
                    a_store(ast.at[c], c, z * NOWN, c).wait()

        def granule(n, carry):
            g = jnp.where(n == FAR - 1, FAR, jnp.where(n == FAR, FAR - 1, n))
            rows_of(4, css.at[g], crs.at[g]).wait_recv()
            gran = dz.at[5 + g // NCH, pl.ds(pl.multiple_of((g % NCH) * CH, CH), CH), :]
            w1_nat[...] = gran[:, LO].T
            w2_nat[...] = gran[:, HI]
            for m in range(8):
                u_own[m * SUB:(m + 1) * SUB, :] = gelu(dot_nn(xo_at(m)[...], w1_nat[...])).astype(BF)
            for m in range(8):
                rows = slice(m * SUB, (m + 1) * SUB)
                facc[rows, :] += dot_nn(u_own[rows, :], w2_nat[...])

            @pl.when(n == 0)
            def _():
                acc2[...] = jnp.zeros_like(acc2)

            events_at(n, IN_LOOP)

            return carry

        lax.fori_loop(0, NG, granule, 0)
        for m in range(8):
            xo_at(m)[...] = (xo_at(m)[...].astype(F32) + facc[m * SUB:(m + 1) * SUB, :]).astype(BF)

    pl.run_scoped(forward, pltpu.VMEM((NOWN, D), F32), pltpu.VMEM((NOWN, CH), BF), pltpu.VMEM((D, CH), BF),
                  pltpu.VMEM((CH, D), BF))

    for c in range(NCH):
        a_store(ast.at[c], c, z * NOWN, c).wait()

    def e_half(k, b):
        return eall.at[k, :, pl.ds(pl.multiple_of(b * TB, TB), TB)]

    def e_pair(b):
        return remote(e_half(0, b), e_half(1, b), ess.at[0, b], ers.at[1, b], pos.pair, j)

    def e_mirror(b):
        return remote(e_half(0, b), e_half(2, b), ess.at[1, b], ers.at[2, b], pos.mirror, j)

    def e_forward(k, b):
        to = 3 if k == 1 else k
        return remote(e_half(k, b), e_half(to, b), efs.at[k, b], ers.at[to, b], pos.mirror if k == 1 else pos.pair, j)

    def e_wait(k, b):
        remote(e_half(k, b), e_half(k, b), efs.at[k, b], ers.at[k, b], pos.pair, j).wait_recv()

    def step_of(s):
        return s // 8, (s % 8) // 2, s % 2

    def a_load(s, slot):
        c, k, b = step_of(s)
        return pltpu.make_async_copy(a_hbm.at[c, pl.ds(share_row(k, b), TB)], ast.at[slot], as_sem.at[slot])

    everything = slice(None)
    up_sems, down_sems = (rss.at[0], rsr), (rss.at[1], rsr)

    def up(c, t):
        return Scatter(pos, acc1.at[c, t], r1a.at[c % 2, t], r2a.at[c % 2, t], r3a.at[c, t], everything, up_sems,
                       c * 6 + t, t == 0)

    def down(c, t, part=None):
        if part is None:
            lanes, idx, x_first = everything, c * 6 + 2 + t, t == 0
        else:
            lanes, idx, x_first = slice(part * (D // 2), (part + 1) * (D // 2)), c * 6 + 2 + t * 2 + part, part == 0
        return Scatter(pos, acc2.at[c, t], r1b.at[c % 2, t], r2b.at[c % 2, t], r3b.at[c, t], lanes, down_sems, idx, x_first)

    ups = [[up(c, t) for t in TWO] for c in range(NCH)]
    downs = [[down(c, t) for t in TWO] for c in range(LAST)]
    tails = [[down(LAST, t, part) for part in TWO] for t in TWO]

    def each(group, stage):
        for sc in group:
            getattr(sc, stage)()

    def fold(v):
        rows, cols = v.shape
        total = jnp.zeros((8, 128), F32)
        for q in range(cols // 128):
            total = total + jnp.sum(v[:, q * 128:(q + 1) * 128].reshape(rows // 8, 8, 128), axis=0)
        return total

    def shard(acc, c, t):
        return acc.at[c, t, pos.y, pos.x, pos.core]

    def out_copy(acc, out, c, sem, t):
        return pltpu.make_async_copy(shard(acc, c, t), out.at[c, t], sh_sem.at[sem])

    def finish(acc, out, c, sem):
        v0, v1 = shard(acc, c, 0)[...], shard(acc, c, 1)[...]
        gm[0] += fold(v0 * v0)
        gm[1] += fold(v0 * v1)
        gm[2] += fold(v1 * v1)
        for t in TWO:
            out_copy(acc, out, c, sem, t).start()

    def finish_chunk(c):
        each(ups[c] + downs[c], 'done')
        finish(acc1, sh1_hbm, c, 0)
        finish(acc2, sh2_hbm, c, 1)

    def backward(us_all, das, xbuf):
        def x_load(s, slot):
            _, k, b = step_of(s)
            return pltpu.make_async_copy(x_hbm.at[pl.ds(share_row(k, b), TB)], xbuf.at[slot], xs_sem.at[slot])

        def pair_slot(p):
            return 2 * ((p + 1) % 2)

        def load_pair(p, act):
            for b in TWO:
                getattr(a_load(p * 2 + b, pair_slot(p) + b), act)()
                getattr(x_load(p * 2 + b, pair_slot(p) + b), act)()

        a_load(0, 0).start()
        x_load(0, 0).start()

        ld_l.wait()
        r = lax.broadcasted_iota(jnp.int32, (ER, TB), 0)
        first = r % 2 == 0
        real = r < 2 * NC
        neg = jnp.float32(-jnp.inf)
        for b in TWO:
            cols = slice(b * TB, (b + 1) * TB)
            logit = jnp.where(real, dot_nt(hcat[...], own_x[:, SIDES[b]]), neg)
            m0 = jnp.max(jnp.where(first, logit, neg), axis=0, keepdims=True)
            m1 = jnp.max(jnp.where(first, neg, logit), axis=0, keepdims=True)
            ex = jnp.exp(logit - jnp.where(first, m0, m1))
            s0 = jnp.sum(jnp.where(first, ex, 0.0), axis=0, keepdims=True)
            s1 = jnp.sum(jnp.where(first, 0.0, ex), axis=0, keepdims=True)
            prob = ex / jnp.where(first, s0, s1)
            lab = jnp.where(first, lab_v[0:1, cols], lab_v[1:2, cols])
            hot = jnp.where(jnp.logical_and(r // 2 == lab, real), 1.0, 0.0)
            eall[0, :, cols] = (prob - hot) / (NTOK * 8.0)
            e_pair(b).start()

            @pl.when(inner)
            def _():
                e_mirror(b).start()

        rows_of(NG, xss, xrs.at[0]).wait_send()
        rows_of(FAR, yss, yrs.at[0]).wait_send()
        rows_of(NG, dss, drs.at[0]).wait_send()
        for i in range(NG):
            rows_of(4, css.at[i], crs.at[i]).wait_send()
        rows_of(NCH, zss.at[0], zrs.at[0]).wait_send()

        @pl.when(inner)
        def _():
            for n, i in ((NCH, 1), (NG, 2), (FAR, 3)):
                rows_of(n, zss.at[i], zrs.at[0]).wait_send()

        def d_act(src, t, sl, c, us, rows):
            w2c = wown[c, :, :, HI].reshape(CH, D)
            u, slope = gelu_and_slope(src[...])
            us[rows, :] = u.astype(BF)
            for task in TWO:
                da = dot_nt(dz[t, sl, SIDES[task]], w2c)
                das[rows, task * CH:(task + 1) * CH] = (da * slope).astype(BF)

        def add_up(c, g):
            for task in TWO:
                acc1[c, task] += g[:, task * CH:(task + 1) * CH].reshape(acc1.shape[2:])

        def add_down(c, g):
            for task in TWO:
                acc2[c, task] += g[:, SIDES[task]].reshape(acc2.shape[2:])

        def e_parts(s):
            _, k, b = step_of(s)
            e = e_half(k, b)[...]
            e1 = e.astype(BF).astype(F32)
            rest = e - e1
            e2 = rest.astype(BF).astype(F32)
            e3 = rest - e2
            return jnp.concatenate([e1, e2, e3], axis=0).astype(BF)

        def first_step(s, carry):
            _, k, b = step_of(s)
            t = k * 2 + b
            a_load(s, s % 2).wait()
            x_load(s, s % 2).wait()

            @pl.when(s < 7)
            def _():
                a_load(s + 1, (s + 1) % 2).start()
                x_load(s + 1, (s + 1) % 2).start()

            @pl.when(s == 7)
            def _():
                load_pair(4, 'start')

            @pl.when(jnp.logical_and(outer, k > 0))
            def _():
                e_wait(k, b)

            es = e_parts(s)
            for m in BLOCKS:
                dz[t, sub(m), :] = dot_tn(es[:, sub(m)], hbd[...]).astype(BF)
            us = us_all.at[0]
            for m in BLOCKS:
                d_act(ast.at[s % 2, sub(m)], t, sub(m), 0, us, sub(m))
            add_up(0, dot_tn(xbuf[s % 2], das[:TB]))
            add_down(0, dot_tn(us[:TB], dz[t]))

            for when, k_f, b_f in ((1, 1, 0), (1, 2, 0), (2, 1, 1), (2, 2, 1), (3, 3, 0), (4, 3, 1)):
                @pl.when(jnp.logical_and(s == when, inner))
                def _():
                    e_forward_after_wait(k_f, b_f)

            return carry

        def pair_front(p, c):
            k = p % 4
            load_pair(p, 'wait')

            @pl.when(p < 11)
            def _():
                load_pair(p + 1, 'start')

            for b in TWO:
                for m in BLOCKS:
                    rows = slice(b * TB + m * SUB, b * TB + (m + 1) * SUB)
                    d_act(ast.at[pair_slot(p) + b, sub(m)], k * 2 + b, sub(m), c, us_all.at[k], rows)
            add_up(c, dot_tn(xbuf[pl.ds(pair_slot(p), 2)].reshape(NOWN, D), das[...]))

        def step(p, carry):
            k = p % 4
            pair_front(p, 1)
            add_down(1, dot_tn(us_all[k], dz[pl.ds(k * 2, 2)].reshape(NOWN, DD)))

            @pl.when(p == 4)
            def _():
                each(ups[0] + downs[0], 'side')

            @pl.when(p == 6)
            def _():
                each(ups[0] + downs[0], 'last')

            return carry

        def e_forward_after_wait(k, b):
            e_wait(k, b)
            e_forward(k, b).start()

        lax.fori_loop(0, 8, first_step, 0)
        each(ups[0] + downs[0], 'start')
        lax.fori_loop(4, 8, step, 0)
        each(ups[1] + downs[1], 'start')

        def last_step(p, carry):
            pair_front(p, LAST)

            @pl.when(p == 8)
            def _():
                finish_chunk(0)
                each(ups[1], 'side')

            @pl.when(p == 9)
            def _():
                each(downs[1], 'side')

            @pl.when(p == 10)
            def _():
                each(ups[1], 'last')

            return carry

        lax.fori_loop(8, 12, last_step, 0)
        each(ups[LAST], 'start')
        each(downs[1], 'last')

        def down_pass(task):
            def half(i, carry):
                u = us_all[pl.ds(i * 2, 2)].reshape(4 * TB, CH)
                d = dz[pl.ds(i * 4, 4), :, SIDES[task]].reshape(4 * TB, D)
                acc2[LAST, task] += dot_tn(u, d).reshape(acc2.shape[2:])

                @pl.when(i == 0)
                def _():
                    each(ups[LAST] if task == 0 else tails[0], 'side')

                return carry

            lax.fori_loop(0, 2, half, 0)
            each(tails[task], 'start')

        down_pass(0)
        finish_chunk(1)
        down_pass(1)

    pl.run_scoped(backward, pltpu.VMEM((4, NOWN, CH), BF), pltpu.VMEM((NOWN, 2 * CH), BF),
                  pltpu.VMEM((4, TB, D), BF))

    each(ups[LAST], 'last')
    each(tails[1], 'side')
    each(tails[0], 'last')
    each(ups[LAST], 'done')
    finish(acc1, sh1_hbm, LAST, 0)
    each(tails[1], 'last')
    each(tails[0], 'done')
    each(tails[1], 'done')
    finish(acc2, sh2_hbm, LAST, 1)

    def full(v):
        return jnp.sum(jnp.sum(v, axis=0, keepdims=True), axis=1, keepdims=True)

    lane = lax.broadcasted_iota(jnp.int32, (1, 128), 1)
    mbuf[pl.ds(me, 1), :] = jnp.where(lane == 0, full(gm[0]), jnp.where(lane == 1, full(gm[1]), full(gm[2])))

    def m_copy(i):
        to = (me + i) % NDEV
        line = mbuf.at[pl.ds(me, 1), :]
        return remote(line, line, mss, mrs, to // 8, to % 8)

    def m_start(i, carry):
        m_copy(i).start()
        return carry

    lax.fori_loop(1, NDEV, m_start, 0)

    for b in TWO:
        e_pair(b).wait_send()

        @pl.when(inner)
        def _():
            e_mirror(b).wait_send()
            for k in LINE:
                e_forward(k, b).wait_send()

    for kind, acc in enumerate((acc1, acc2)):
        for stage, part in enumerate((acc.at[:, :, :, :, 0], acc.at[:, :, :, 0, 0], acc.at[:, :, 0, 0, 0])):
            remote(part, part, rss.at[kind, stage], rsr.at[0, stage], z, pos.jc).wait_send()
    pltpu.make_async_copy(r3a, sh1_hbm, sh_sem.at[0]).wait()
    pltpu.make_async_copy(r3b, sh2_hbm, sh_sem.at[1]).wait()

    lines = mbuf.at[pl.ds(0, NDEV - 1), :]
    remote(lines, lines, mss, mrs, z, pos.jc).wait()
    rows_ref[...] = mbuf[...]


def main_call(x, w1, w2r, heads, labels):
    dma = pltpu.SemaphoreType.DMA
    anyspec = pl.BlockSpec(memory_space=pl.ANY)
    vspec = pl.BlockSpec(memory_space=pltpu.VMEM)
    up, down = (OWN, CH), (GR, D)
    pair, quad, octet = (2,), (2, 2), (2, 2, 2)
    per_chunk = (NCH, 2)
    vmem = pltpu.VMEM
    return pl.pallas_call(
        main_kernel,
        out_shape=(jax.ShapeDtypeStruct((NCH, NTOK, CH), F32),
                   jax.ShapeDtypeStruct(per_chunk + up, F32),
                   jax.ShapeDtypeStruct(per_chunk + down, F32),
                   jax.ShapeDtypeStruct((NDEV, 128), F32)),
        in_specs=[anyspec] * 5,
        out_specs=(anyspec, anyspec, anyspec, vspec),
        scratch_shapes=[
            vmem((8, TB, DD), BF),
            vmem((NCH, 8, GR, DD), BF),
            vmem(per_chunk + octet + up, F32), vmem(per_chunk + octet + down, F32),
            vmem((2, 2) + quad + up, F32), vmem((2, 2) + quad + down, F32),
            vmem((2, 2) + pair + up, F32), vmem((2, 2) + pair + down, F32),
            vmem(per_chunk + up, F32), vmem(per_chunk + down, F32),
            vmem((4, ER, NOWN), F32),
            vmem((4, TB, CH), F32),
            vmem((3 * ER, DD), BF),
            vmem((ER, D), BF),
            vmem((NC, 2, D), BF),
            vmem((2, NOWN), jnp.int32),
            vmem((3, 8, 128), F32), vmem((NDEV, 128), F32),
            dma((4,)), dma((NG,)), dma((NCH,)), dma(()), dma((NG,)), dma(()), dma((FAR,)), dma(()), dma((NG,)), dma((NG,)), dma((NG,)),
            dma((5,)), dma((NCH,)), dma((4,)), dma((6,)), dma(quad), dma((4, 2)), dma((4, 2)),
            dma((2, NCH)), dma((6 * NCH, NCH)), dma(()), dma(()), dma(pair),
        ],
        compiler_params=pltpu.CompilerParams(
            collective_id=0, has_side_effects=True, vmem_limit_bytes=VMEM_BYTES),
        name='main',
    )(x, w1, w2r, heads, labels)


def result_kernel(rows_hbm, sh1_hbm, sh2_hbm, a_ref, g1_ref, g2_ref, rows, sh1, sh2, sem):
    ld_rows = pltpu.make_async_copy(rows_hbm, rows, sem.at[0])
    loads = [pltpu.make_async_copy(sh1_hbm, sh1, sem.at[1]), pltpu.make_async_copy(sh2_hbm, sh2, sem.at[2])]
    ld_rows.start()
    for cp in loads:
        cp.start()
    ld_rows.wait()

    gram = jnp.sum(rows[...], axis=0, keepdims=True)
    lane = lax.broadcasted_iota(jnp.int32, gram.shape, 1)

    def entry(i):
        return jnp.sum(jnp.where(lane == i, gram, 0.0), axis=1, keepdims=True)

    g00, g01, g11 = entry(0), entry(1), entry(2)
    scale = (g00 + g11) * -0.5
    g00, g01, g11 = g00 / scale, g01 / scale, g11 / scale
    a0 = a1 = jnp.full((1, 1), 0.5, F32)
    for _ in range(STEPS):
        v0 = a0 * jnp.exp(g00 * a0 + g01 * a1)
        v1 = a1 * jnp.exp(g01 * a0 + g11 * a1)
        tot = v0 + v1
        a0, a1 = v0 / tot, v1 / tot
    a_ref[0] = a0[0, 0]
    a_ref[1] = a1[0, 0]
    for cp in loads:
        cp.wait()
    for c in range(NCH):
        comb = a0 * sh1[c, 0] + a1 * sh1[c, 1]
        for g in range(8):
            col = g * NCH * GR + c * GR
            g1_ref[:, col:col + GR] = comb[:, g * GR:(g + 1) * GR]
        g2_ref[c * GR:(c + 1) * GR, :] = a0 * sh2[c, 0] + a1 * sh2[c, 1]


def result_call(rows, sh1, sh2):
    vspec = pl.BlockSpec(memory_space=pltpu.VMEM)
    anyspec = pl.BlockSpec(memory_space=pl.ANY)
    return pl.pallas_call(
        result_kernel,
        out_shape=(jax.ShapeDtypeStruct((2,), F32), jax.ShapeDtypeStruct((OWN, D), F32),
                   jax.ShapeDtypeStruct((OWN, D), F32)),
        in_specs=[anyspec] * NCH,
        out_specs=(pl.BlockSpec(memory_space=pltpu.SMEM), vspec, vspec),
        scratch_shapes=[pltpu.VMEM(v.shape, F32) for v in (rows, sh1, sh2)] + [pltpu.SemaphoreType.DMA((NCH,))],
        name='result',
    )(rows, sh1, sh2)


def solution(mesh):
    def local_step(tokens, w_up, w_down, task_heads, labels):
        w2r = w_down.reshape(8, NCH, GR, D)
        heads = jnp.transpose(task_heads, (2, 0, 1))
        _, sh1, sh2, rows = main_call(tokens, w_up, w2r, heads, labels)
        return result_call(rows, sh1, sh2)

    return jax.shard_map(
        local_step, mesh=mesh,
        in_specs=(P('data', None), P(None, 'model'), P('model', None), P(None, None, None), P(None, 'data')),
        out_specs=(P(None), P('data', 'model'), P(('model', 'data'), None)),
        check_vma=False)
```

```python
import jax
import jax.numpy as jnp
from jax import lax
from jax.experimental import pallas as pl
from jax.experimental.pallas import tpu as pltpu
from jax.sharding import PartitionSpec as P

STEPS = 20
BF = jnp.bfloat16
F32 = jnp.float32
MESH = pl.DeviceIdType.MESH
VMEM_BYTES = 67043328

D = 768
DD = D + D
NTOK = 8192
NOWN = 2048
TB = 1024
SUB = 256
NC = 19
ER = 40
CH = 256
NCH = 3
LAST = NCH - 1
NG = NCH * NCH
FAR = NG - NCH
GR = 32
OWN = CH // GR * 12
LO = slice(D)
HI = slice(D, DD)
SIDES = (LO, HI)
TWO = range(2)
MATES = range(1, 8)
LINE = range(1, 4)
BLOCKS = range(TB // SUB)
NDEV = 32

E_ON = ('', '1020', '1121', '30', '31')
IN_OTHER = ('', 't0o0', 't1o1i3', 't2o2i4', 's0i5', 's1T3o3')
IN_OWN = ('i6', 's2d0T4o4i7', 'd1i8', 's3T5o5g6')
IN_LOOP = ('d2g7s4', 'd3g8', 's5B6x6d4', 'B7x7', 'd5p6B8x8', 'p7', 'p8', '', '')

G0 = 0.7978845608028654
G1C = 0.044715 * G0


def dot_nn(a, b):
    return lax.dot_general(a, b, (((1,), (0,)), ((), ())), preferred_element_type=F32)


def dot_nt(a, b):
    return lax.dot_general(a, b, (((1,), (1,)), ((), ())), preferred_element_type=F32)


def dot_tn(a, b):
    return lax.dot_general(a, b, (((0,), (0,)), ((), ())), preferred_element_type=F32)


def gelu(x):
    t = jnp.tanh(x * (G0 + G1C * (x * x)))
    h = 0.5 * x
    return h + h * t


def gelu_and_slope(x):
    x2 = x * x
    t = jnp.tanh(x * (G0 + G1C * x2))
    h = 0.5 * x
    u = h + h * t
    s = 0.5 + 0.5 * t + h * (1.0 - t * t) * (G0 + (3.0 * G1C) * x2)
    return u, s


class Place:
    def __init__(self):
        self.z = lax.axis_index('model')
        self.j = lax.axis_index('data')
        self.core = self.j % 2
        self.x = (self.j // 2) % 2
        self.y = self.j // 4
        self.jc = self.j + 1 - 2 * self.core
        self.jx = self.j + 2 - 4 * self.x
        self.jy = self.j + 4 - 8 * self.y
        self.jd = self.jx + 4 - 8 * self.y
        self.js = self.jx + self.core * (self.jy - self.jx)
        self.j2 = self.jx + self.jy - self.js

        self.inner = self.z % 3 > 0
        self.pair = self.z + 1 - 2 * (self.z % 2)
        self.mirror = 3 - self.z
        half = self.z // 2
        self.shares = (self.z, self.pair, 2 - half, 3 - 3 * half)

    def share(self, k):
        own, near, far, end = self.shares
        return jnp.where(k == 0, own, jnp.where(k == 1, near, jnp.where(k == 2, far, end)))


def remote(src, dst, ssem, rsem, z, j):
    return pltpu.make_async_remote_copy(
        src_ref=src, dst_ref=dst, send_sem=ssem, recv_sem=rsem, device_id=(z, j), device_id_type=MESH)


class Scatter:
    def __init__(self, pos, acc, r1, r2, r3, lanes, sems, idx, x_first):
        self.pos, self.acc, self.r1, self.r2, self.r3 = pos, acc, r1, r2, r3
        self.lanes, self.sems, self.idx, self.x_first = lanes, sems, idx, x_first

    def copy(self, stage):
        p, ln = self.pos, self.lanes
        ssem, rsem = self.sems[0].at[stage], self.sems[1].at[self.idx, stage]
        if stage == 0:
            return remote(self.acc.at[:, :, 1 - p.core, :, ln], self.r1.at[:, :, :, ln], ssem, rsem, p.z, p.jc)
        if stage == 1:
            if self.x_first:
                return remote(self.acc.at[:, 1 - p.x, p.core, :, ln], self.r2.at[:, :, ln], ssem, rsem, p.z, p.jx)
            return remote(self.acc.at[1 - p.y, :, p.core, :, ln], self.r2.at[:, :, ln], ssem, rsem, p.z, p.jy)
        if self.x_first:
            return remote(self.acc.at[1 - p.y, p.x, p.core, :, ln], self.r3.at[:, ln], ssem, rsem, p.z, p.jy)
        return remote(self.acc.at[p.y, 1 - p.x, p.core, :, ln], self.r3.at[:, ln], ssem, rsem, p.z, p.jx)

    def start(self):
        self.copy(0).start()

    def side(self):
        p, ln = self.pos, self.lanes
        self.copy(0).wait_recv()
        for yy in TWO:
            for xx in TWO:
                self.acc[yy, xx, p.core, :, ln] += self.r1[yy, xx, :, ln]
        self.copy(1).start()

    def last(self):
        p, ln = self.pos, self.lanes
        self.copy(1).wait_recv()
        for i in TWO:
            if self.x_first:
                self.acc[i, p.x, p.core, :, ln] += self.r2[i, :, ln]
            else:
                self.acc[p.y, i, p.core, :, ln] += self.r2[i, :, ln]
        self.copy(2).start()

    def done(self):
        p, ln = self.pos, self.lanes
        self.copy(2).wait_recv()
        self.acc[p.y, p.x, p.core, :, ln] += self.r3[:, ln]


def main_kernel(x_hbm, w1_hbm, w2_hbm, heads_hbm, lab_hbm,
                a_hbm, sh1_hbm, sh2_hbm, rows_hbm,
                dz, wown, acc1, acc2, r1a, r1b, r2a, r2b, r3a, r3b, eall, ast, hbd, hcat, heads, lab_v,
                gm, mbuf,
                zss, zrs, zqs, xss, xrs, yss, yrs, dss, drs, css, crs,
                ld_sem, w2_sem, xs_sem, as_sem, ess, efs, ers,
                rss, rsr, mss, mrs, sh_sem):
    pos = Place()
    z, j, inner = pos.z, pos.j, pos.inner
    outer = jnp.logical_not(inner)

    barrier = pltpu.get_barrier_semaphore()
    me = z * 8 + j
    pl.semaphore_signal(barrier, device_id=(pos.pair, j), device_id_type=MESH)

    @pl.when(inner)
    def _():
        pl.semaphore_signal(barrier, device_id=(pos.mirror, j), device_id_type=MESH)

    for jj in (pos.jx, pos.jy, pos.jc):
        pl.semaphore_signal(barrier, device_id=(z, jj), device_id_type=MESH)

    own_x, act, room = dz.at[0], dz.at[2], dz.at[3]
    w1_raw = room.at[LO, LO]
    w1_own = dz.at[4, LO, HI]

    def sub(m):
        return slice((m % 4) * SUB, (m % 4 + 1) * SUB)

    def xo_at(m):
        return own_x.at[sub(m), HI if m >= 4 else LO]

    def share_row(k, b):
        return pl.multiple_of((pos.share(k) * 2 + b) * TB, TB)

    own_row = pl.multiple_of(z * NOWN, NOWN)
    ld_w1 = pltpu.make_async_copy(w1_hbm, w1_raw, ld_sem.at[0])
    ld_x = [pltpu.make_async_copy(x_hbm.at[pl.ds(own_row + b * TB, TB)], own_x.at[:, SIDES[b]], ld_sem.at[1 + b])
            for b in TWO]
    ld_l = pltpu.make_async_copy(lab_hbm.at[:, pl.ds(own_row, NOWN)], lab_v, ld_sem.at[3])
    ld_h = pltpu.make_async_copy(heads_hbm, heads, ld_sem.at[4])
    ld_w2 = [pltpu.make_async_copy(w2_hbm.at[:, c], wown.at[c, :, :, HI], w2_sem.at[c]) for c in range(NCH)]

    def stream_half(i):
        return dz.at[1 + 3 * (i % 2), :, LO]

    def xs_load(i):
        return pltpu.make_async_copy(
            x_hbm.at[pl.ds(share_row(1 + i // 2, i % 2), TB)], stream_half(i), xs_sem.at[i % 2])

    ld_h.start()
    ld_w1.start()
    for cp in ld_w2:
        cp.start()
    xs_load(0).start()
    for cp in ld_x:
        cp.start()
    ld_l.start()

    ld_h.wait()
    hf = jnp.concatenate([heads[i].astype(F32) for i in range(NC)] + [jnp.zeros((2, D), F32)], axis=0)
    hcat[...] = hf.astype(BF)
    r = lax.broadcasted_iota(jnp.int32, (ER, D), 0)
    hb = jnp.concatenate([jnp.where(r % 2 == 0, hf, 0.0), jnp.where(r % 2 == 1, hf, 0.0)], axis=1)
    hbd[...] = jnp.concatenate([hb, hb, hb], axis=0).astype(BF)
    gm[...] = jnp.zeros_like(gm)
    acc1[...] = jnp.zeros_like(acc1)

    ld_w1.wait()
    w1t = w1_raw[...].T
    for c in range(NCH):
        for g in range(8):
            row = g * NCH * GR + c * GR
            wown[c, g, :, LO] = w1t[row:row + GR, :]
    for cp in ld_w2:
        cp.wait()
    pl.semaphore_wait(barrier, 4 + z * pos.mirror // 2)

    def piece(i, jj):
        row = pl.multiple_of((i % NCH) * CH + jj * GR, GR)
        return dz.at[5 + i // NCH, pl.ds(row, GR), :]

    def rows_of(n, ssem, rsem):
        part = dz.at[5, pl.ds(0, n * GR), :]
        return remote(part, part, ssem, rsem, z, pos.jc)

    def z_pair(c):
        return remote(wown.at[c, j], piece(c, j), zss.at[0], zrs.at[c], pos.pair, j)

    def z_mirror(c):
        return remote(wown.at[c, j], piece(NCH + c, j), zss.at[1], zrs.at[NCH + c], pos.mirror, j)

    def z_forward(i):
        first = i < NCH
        to = jnp.where(first, i + 2 * NCH, i)
        return remote(piece(i, j), piece(to, j), zss.at[2], zrs.at[to], jnp.where(first, pos.mirror, pos.pair), j)

    def more_forward(i):
        first = i < NCH
        to = jnp.where(first, i + 2 * NCH, i)
        return remote(piece(i, pos.j2), piece(to, pos.j2), zss.at[3], zqs.at[to - FAR], jnp.where(first, pos.mirror, pos.pair), j)

    def side_copy(i):
        return remote(piece(i, j), piece(i, j), xss, xrs.at[i], z, pos.js)

    def more_copy(i):
        return remote(piece(i, pos.j2), piece(i, pos.j2), dss, drs.at[i], z, pos.js)

    def x_copy(i):
        return remote(piece(i, j), piece(i, j), xss, xrs.at[i], z, pos.jx)

    def y_copy(i):
        return remote(piece(i, j), piece(i, j), yss, yrs.at[i], z, pos.jy)

    def diag_copy_y(i):
        return remote(piece(i, pos.jx), piece(i, pos.jx), dss, drs.at[i], z, pos.jy)

    def diag_copy_x(i):
        return remote(piece(i, pos.jy), piece(i, pos.jy), dss, drs.at[i], z, pos.jx)

    def core_copy(i, q):
        jj = (j, pos.jx, pos.jy, pos.jd)[q]
        return remote(piece(i, jj), piece(i, jj), css.at[i], crs.at[i], z, pos.jc)

    def core_side(i, q):
        jj = (j, pos.js, pos.j2, pos.jd)[q]
        return remote(piece(i, jj), piece(i, jj), css.at[i], crs.at[i], z, pos.jc)

    def take(i):
        remote(piece(i, j), piece(i, j), zss.at[2], zrs.at[i], pos.pair, j).wait_recv()

        @pl.when(inner)
        def _():
            z_forward(i).start()

    def take_more(i):
        remote(piece(i, j), piece(i, j), zss.at[3], zqs.at[i - FAR], pos.pair, j).wait_recv()

        @pl.when(inner)
        def _():
            more_forward(i).start()

    def take_both(i):
        take(i)
        take_more(i)

    def send_both(i):
        side_copy(i).start()
        more_copy(i).start()
        core_side(i, 0).start()
        core_side(i, 2).start()

    def pass_both(i):
        side_copy(i).wait_recv()
        core_side(i, 1).start()
        more_copy(i).wait_recv()
        core_side(i, 3).start()

    def send_own(i):
        x_copy(i).start()
        y_copy(i).start()
        core_copy(i, 0).start()

    def send_side(i):
        x_copy(i).wait_recv()

        @pl.when(pos.core == 0)
        def _():
            diag_copy_y(i).start()

        core_copy(i, 1).start()
        y_copy(i).wait_recv()

        @pl.when(pos.core == 1)
        def _():
            diag_copy_x(i).start()

        core_copy(i, 2).start()

    def send_diag(i):
        diag_copy_y(i).wait_recv()
        core_copy(i, 3).start()

    def side_and_on(i):
        send_side(i)
        if i < NCH:
            @pl.when(inner)
            def _():
                more_forward(i).start()

    def when_inner(f):
        return lambda i: pl.when(inner)(lambda: f(i))

    def when_outer(f):
        return lambda i: pl.when(outer)(lambda: f(i))

    kinds = {'t': take, 'T': when_outer(take), 'i': when_inner(take), 'o': send_own, 's': side_and_on, 'd': send_diag,
             'g': when_inner(take_more), 'B': when_outer(take_both), 'x': send_both, 'p': pass_both}

    def events(codes):
        for kind, i in zip(codes[::2], codes[1::2]):
            kinds[kind](int(i))

    def events_at(i, table):
        for n, codes in enumerate(table):
            if codes:
                pl.when(i == n)(lambda codes=codes: events(codes))

    for c in range(NCH):
        z_pair(c).start()

    @pl.when(inner)
    def _():
        for c in range(NCH):
            z_mirror(c).start()

    def a_store(src, c, row, sem):
        return pltpu.make_async_copy(src, a_hbm.at[c, pl.ds(pl.multiple_of(row, TB), TB)], as_sem.at[sem])

    def forward(facc, u_own, w1_nat, w2_nat):
        for c in range(NCH):
            w1_own[:, c * CH:(c + 1) * CH] = wown[c, :, :, LO].reshape(CH, D).T

        def staged(i, c):
            rows = pl.ds(pl.multiple_of((i % 2) * TB, TB), TB)
            return a_store(facc.at[rows, c * CH:(c + 1) * CH], c, share_row(1 + i // 2, i % 2), (i % 2) * NCH + c)

        def other_tokens(i, carry):
            xs_load(i).wait()

            @pl.when(i < 5)
            def _():
                xs_load(i + 1).start()

            @pl.when(i >= 2)
            def _():
                for c in range(NCH):
                    staged(i, c).wait()

            base = (i % 2) * TB
            for m in BLOCKS:
                rows = pl.ds(pl.multiple_of(base + m * SUB, SUB), SUB)
                facc[rows, :] = dot_nn(stream_half(i)[sub(m), :], w1_own[...])
            for c in range(NCH):
                staged(i, c).start()

            events_at(i, IN_OTHER)
            return carry

        lax.fori_loop(0, 6, other_tokens, 0)
        for cp in ld_x:
            cp.wait()

        for b in TWO:
            for c in range(NCH):
                staged(b, c).wait()
            for m in BLOCKS:
                a = dot_nn(xo_at(b * 4 + m)[...], w1_own[...])
                for c in range(NCH):
                    ast[c, sub(m), :] = a[:, c * CH:(c + 1) * CH]
                act[sub(m), LO] = gelu(a).astype(BF)
            events(IN_OWN[2 * b])
            for m in BLOCKS:
                facc[b * TB + m * SUB:b * TB + (m + 1) * SUB, :] = dot_nn(
                    act[sub(m), LO], wown[:, :, :, HI].reshape(D, D))
            for c in range(NCH):
                a_store(ast.at[c], c, (z * 2 + b) * TB, c).start()
            events(IN_OWN[2 * b + 1])
            if b == 0:
                for c in range(NCH):
                    a_store(ast.at[c], c, z * NOWN, c).wait()

        def granule(n, carry):
            g = jnp.where(n == FAR - 1, FAR, jnp.where(n == FAR, FAR - 1, n))
            rows_of(4, css.at[g], crs.at[g]).wait_recv()
            gran = dz.at[5 + g // NCH, pl.ds(pl.multiple_of((g % NCH) * CH, CH), CH), :]
            w1_nat[...] = gran[:, LO].T
            w2_nat[...] = gran[:, HI]
            for m in range(8):
                u_own[m * SUB:(m + 1) * SUB, :] = gelu(dot_nn(xo_at(m)[...], w1_nat[...])).astype(BF)
            for m in range(8):
                rows = slice(m * SUB, (m + 1) * SUB)
                facc[rows, :] += dot_nn(u_own[rows, :], w2_nat[...])

            @pl.when(n == 0)
            def _():
                acc2[...] = jnp.zeros_like(acc2)

            events_at(n, IN_LOOP)

            return carry

        lax.fori_loop(0, NG, granule, 0)
        for m in range(8):
            xo_at(m)[...] = (xo_at(m)[...].astype(F32) + facc[m * SUB:(m + 1) * SUB, :]).astype(BF)

    pl.run_scoped(forward, pltpu.VMEM((NOWN, D), F32), pltpu.VMEM((NOWN, CH), BF), pltpu.VMEM((D, CH), BF),
                  pltpu.VMEM((CH, D), BF))

    for c in range(NCH):
        a_store(ast.at[c], c, z * NOWN, c).wait()

    def e_half(k, b):
        return eall.at[k, :, pl.ds(pl.multiple_of(b * TB, TB), TB)]

    def e_pair(b):
        return remote(e_half(0, b), e_half(1, b), ess.at[0, b], ers.at[1, b], pos.pair, j)

    def e_mirror(b):
        return remote(e_half(0, b), e_half(2, b), ess.at[1, b], ers.at[2, b], pos.mirror, j)

    def e_forward(k, b):
        to = 3 if k == 1 else k
        return remote(e_half(k, b), e_half(to, b), efs.at[k, b], ers.at[to, b], pos.mirror if k == 1 else pos.pair, j)

    def e_wait(k, b):
        remote(e_half(k, b), e_half(k, b), efs.at[k, b], ers.at[k, b], pos.pair, j).wait_recv()

    def step_of(s):
        return s // 8, (s % 8) // 2, s % 2

    def a_load(s, slot):
        c, k, b = step_of(s)
        return pltpu.make_async_copy(a_hbm.at[c, pl.ds(share_row(k, b), TB)], ast.at[slot], as_sem.at[slot])

    everything = slice(None)
    up_sems, down_sems = (rss.at[0], rsr), (rss.at[1], rsr)

    def up(c, t):
        return Scatter(pos, acc1.at[c, t], r1a.at[c % 2, t], r2a.at[c % 2, t], r3a.at[c, t], everything, up_sems,
                       c * 6 + t, t == 0)

    def down(c, t, part=None):
        if part is None:
            lanes, idx, x_first = everything, c * 6 + 2 + t, t == 0
        else:
            lanes, idx, x_first = slice(part * (D // 2), (part + 1) * (D // 2)), c * 6 + 2 + t * 2 + part, part == 0
        return Scatter(pos, acc2.at[c, t], r1b.at[c % 2, t], r2b.at[c % 2, t], r3b.at[c, t], lanes, down_sems, idx, x_first)

    ups = [[up(c, t) for t in TWO] for c in range(NCH)]
    downs = [[down(c, t) for t in TWO] for c in range(LAST)]
    tails = [[down(LAST, t, part) for part in TWO] for t in TWO]

    def each(group, stage):
        for sc in group:
            getattr(sc, stage)()

    def fold(v):
        rows, cols = v.shape
        total = jnp.zeros((8, 128), F32)
        for q in range(cols // 128):
            total = total + jnp.sum(v[:, q * 128:(q + 1) * 128].reshape(rows // 8, 8, 128), axis=0)
        return total

    def shard(acc, c, t):
        return acc.at[c, t, pos.y, pos.x, pos.core]

    def out_copy(acc, out, c, sem, t):
        return pltpu.make_async_copy(shard(acc, c, t), out.at[c, t], sh_sem.at[sem])

    def finish(acc, out, c, sem):
        v0, v1 = shard(acc, c, 0)[...], shard(acc, c, 1)[...]
        gm[0] += fold(v0 * v0)
        gm[1] += fold(v0 * v1)
        gm[2] += fold(v1 * v1)
        for t in TWO:
            out_copy(acc, out, c, sem, t).start()

    def finish_chunk(c):
        each(ups[c] + downs[c], 'done')
        finish(acc1, sh1_hbm, c, 0)
        finish(acc2, sh2_hbm, c, 1)

    def backward(us_all, das, xbuf):
        def x_load(s, slot):
            _, k, b = step_of(s)
            return pltpu.make_async_copy(x_hbm.at[pl.ds(share_row(k, b), TB)], xbuf.at[slot], xs_sem.at[slot])

        def pair_slot(p):
            return 2 * ((p + 1) % 2)

        def load_pair(p, act):
            for b in TWO:
                getattr(a_load(p * 2 + b, pair_slot(p) + b), act)()
                getattr(x_load(p * 2 + b, pair_slot(p) + b), act)()

        a_load(0, 0).start()
        x_load(0, 0).start()

        ld_l.wait()
        r = lax.broadcasted_iota(jnp.int32, (ER, TB), 0)
        first = r % 2 == 0
        real = r < 2 * NC
        neg = jnp.float32(-jnp.inf)
        for b in TWO:
            cols = slice(b * TB, (b + 1) * TB)
            logit = jnp.where(real, dot_nt(hcat[...], own_x[:, SIDES[b]]), neg)
            m0 = jnp.max(jnp.where(first, logit, neg), axis=0, keepdims=True)
            m1 = jnp.max(jnp.where(first, neg, logit), axis=0, keepdims=True)
            ex = jnp.exp(logit - jnp.where(first, m0, m1))
            s0 = jnp.sum(jnp.where(first, ex, 0.0), axis=0, keepdims=True)
            s1 = jnp.sum(jnp.where(first, 0.0, ex), axis=0, keepdims=True)
            prob = ex / jnp.where(first, s0, s1)
            lab = jnp.where(first, lab_v[0:1, cols], lab_v[1:2, cols])
            hot = jnp.where(jnp.logical_and(r // 2 == lab, real), 1.0, 0.0)
            eall[0, :, cols] = (prob - hot) / (NTOK * 8.0)
            e_pair(b).start()

            @pl.when(inner)
            def _():
                e_mirror(b).start()

        rows_of(NG, xss, xrs.at[0]).wait_send()
        rows_of(FAR, yss, yrs.at[0]).wait_send()
        rows_of(NG, dss, drs.at[0]).wait_send()
        for i in range(NG):
            rows_of(4, css.at[i], crs.at[i]).wait_send()
        rows_of(NCH, zss.at[0], zrs.at[0]).wait_send()

        @pl.when(inner)
        def _():
            for n, i in ((NCH, 1), (NG, 2), (FAR, 3)):
                rows_of(n, zss.at[i], zrs.at[0]).wait_send()

        def d_act(src, t, sl, c, us, rows):
            w2c = wown[c, :, :, HI].reshape(CH, D)
            u, slope = gelu_and_slope(src[...])
            us[rows, :] = u.astype(BF)
            for task in TWO:
                da = dot_nt(dz[t, sl, SIDES[task]], w2c)
                das[rows, task * CH:(task + 1) * CH] = (da * slope).astype(BF)

        def add_up(c, g):
            for task in TWO:
                acc1[c, task] += g[:, task * CH:(task + 1) * CH].reshape(acc1.shape[2:])

        def add_down(c, g):
            for task in TWO:
                acc2[c, task] += g[:, SIDES[task]].reshape(acc2.shape[2:])

        def e_parts(s):
            _, k, b = step_of(s)
            e = e_half(k, b)[...]
            e1 = e.astype(BF).astype(F32)
            rest = e - e1
            e2 = rest.astype(BF).astype(F32)
            e3 = rest - e2
            return jnp.concatenate([e1, e2, e3], axis=0).astype(BF)

        def first_step(s, carry):
            _, k, b = step_of(s)
            t = k * 2 + b
            a_load(s, s % 2).wait()
            x_load(s, s % 2).wait()

            @pl.when(s < 7)
            def _():
                a_load(s + 1, (s + 1) % 2).start()
                x_load(s + 1, (s + 1) % 2).start()

            @pl.when(s == 7)
            def _():
                load_pair(4, 'start')

            @pl.when(jnp.logical_and(outer, k > 0))
            def _():
                e_wait(k, b)

            es = e_parts(s)
            for m in BLOCKS:
                dz[t, sub(m), :] = dot_tn(es[:, sub(m)], hbd[...]).astype(BF)
            us = us_all.at[0]
            for m in BLOCKS:
                d_act(ast.at[s % 2, sub(m)], t, sub(m), 0, us, sub(m))
            add_up(0, dot_tn(xbuf[s % 2], das[:TB]))
            add_down(0, dot_tn(us[:TB], dz[t]))

            for when, codes in enumerate(E_ON):
                if codes:
                    @pl.when(jnp.logical_and(s == when, inner))
                    def _():
                        for k_f, b_f in zip(codes[::2], codes[1::2]):
                            e_forward_after_wait(int(k_f), int(b_f))

            return carry

        def pair_front(p, c):
            k = p % 4
            load_pair(p, 'wait')

            @pl.when(p < 11)
            def _():
                load_pair(p + 1, 'start')

            for b in TWO:
                for m in BLOCKS:
                    rows = slice(b * TB + m * SUB, b * TB + (m + 1) * SUB)
                    d_act(ast.at[pair_slot(p) + b, sub(m)], k * 2 + b, sub(m), c, us_all.at[k], rows)
            add_up(c, dot_tn(xbuf[pl.ds(pair_slot(p), 2)].reshape(NOWN, D), das[...]))

        def step(p, carry):
            k = p % 4
            pair_front(p, 1)
            add_down(1, dot_tn(us_all[k], dz[pl.ds(k * 2, 2)].reshape(NOWN, DD)))

            @pl.when(p == 4)
            def _():
                each(ups[0] + downs[0], 'side')

            @pl.when(p == 6)
            def _():
                each(ups[0] + downs[0], 'last')

            return carry

        def e_forward_after_wait(k, b):
            e_wait(k, b)
            e_forward(k, b).start()

        lax.fori_loop(0, 8, first_step, 0)
        each(ups[0] + downs[0], 'start')
        lax.fori_loop(4, 8, step, 0)
        each(ups[1] + downs[1], 'start')

        def last_step(p, carry):
            pair_front(p, LAST)

            @pl.when(p == 8)
            def _():
                finish_chunk(0)
                each(ups[1], 'side')

            @pl.when(p == 9)
            def _():
                each(downs[1], 'side')

            @pl.when(p == 10)
            def _():
                each(ups[1], 'last')

            return carry

        lax.fori_loop(8, 12, last_step, 0)
        each(ups[LAST], 'start')
        each(downs[1], 'last')

        def down_pass(task):
            def half(i, carry):
                u = us_all[pl.ds(i * 2, 2)].reshape(4 * TB, CH)
                d = dz[pl.ds(i * 4, 4), :, SIDES[task]].reshape(4 * TB, D)
                acc2[LAST, task] += dot_tn(u, d).reshape(acc2.shape[2:])

                @pl.when(i == 0)
                def _():
                    each(ups[LAST] if task == 0 else tails[0], 'side')

                return carry

            lax.fori_loop(0, 2, half, 0)
            each(tails[task], 'start')

        down_pass(0)
        finish_chunk(1)
        down_pass(1)

    pl.run_scoped(backward, pltpu.VMEM((4, NOWN, CH), BF), pltpu.VMEM((NOWN, 2 * CH), BF),
                  pltpu.VMEM((4, TB, D), BF))

    each(ups[LAST], 'last')
    each(tails[1], 'side')
    each(tails[0], 'last')
    each(ups[LAST], 'done')
    finish(acc1, sh1_hbm, LAST, 0)
    each(tails[1], 'last')
    each(tails[0], 'done')
    each(tails[1], 'done')
    finish(acc2, sh2_hbm, LAST, 1)

    def full(v):
        return jnp.sum(jnp.sum(v, axis=0, keepdims=True), axis=1, keepdims=True)

    lane = lax.broadcasted_iota(jnp.int32, (1, 128), 1)
    mbuf[pl.ds(me, 1), :] = jnp.where(lane == 0, full(gm[0]), jnp.where(lane == 1, full(gm[1]), full(gm[2])))

    def row_of(ref):
        return ref.at[pl.ds(me, 1), :]

    keep = pltpu.make_async_copy(row_of(mbuf), row_of(rows_hbm), ld_sem.at[0])
    keep.start()

    def m_send(to_z, to_j):
        remote(row_of(mbuf), row_of(rows_hbm), mss, mrs, to_z, to_j).start()

    mates = [(j + i) % 8 for i in MATES]
    for to_z in reversed(pos.shares[1:]):
        for to_j in [j] + mates:
            m_send(to_z, to_j)
    for to_j in mates:
        m_send(z, to_j)

    for b in TWO:
        e_pair(b).wait_send()

        @pl.when(inner)
        def _():
            e_mirror(b).wait_send()
            for k in LINE:
                e_forward(k, b).wait_send()

    for kind, acc in enumerate((acc1, acc2)):
        for stage, part in enumerate((acc.at[:, :, :, :, 0], acc.at[:, :, :, 0, 0], acc.at[:, :, 0, 0, 0])):
            remote(part, part, rss.at[kind, stage], rsr.at[0, stage], z, pos.jc).wait_send()
    pltpu.make_async_copy(r3a, sh1_hbm, sh_sem.at[0]).wait()
    pltpu.make_async_copy(r3b, sh2_hbm, sh_sem.at[1]).wait()

    keep.wait()
    lines = pl.ds(0, NDEV - 1)
    remote(mbuf.at[lines, :], rows_hbm.at[lines, :], mss, mrs, z, pos.jc).wait()


def main_call(x, w1, w2r, heads, labels):
    dma = pltpu.SemaphoreType.DMA
    anyspec = pl.BlockSpec(memory_space=pl.ANY)
    up, down = (OWN, CH), (GR, D)
    pair, quad, octet = (2,), (2, 2), (2, 2, 2)
    per_chunk = (NCH, 2)
    vmem = pltpu.VMEM
    return pl.pallas_call(
        main_kernel,
        out_shape=(jax.ShapeDtypeStruct((NCH, NTOK, CH), F32),
                   jax.ShapeDtypeStruct(per_chunk + up, F32),
                   jax.ShapeDtypeStruct(per_chunk + down, F32),
                   jax.ShapeDtypeStruct((NDEV, 128), F32)),
        in_specs=[anyspec] * 5,
        out_specs=(anyspec, anyspec, anyspec, anyspec),
        scratch_shapes=[
            vmem((8, TB, DD), BF),
            vmem((NCH, 8, GR, DD), BF),
            vmem(per_chunk + octet + up, F32), vmem(per_chunk + octet + down, F32),
            vmem((2, 2) + quad + up, F32), vmem((2, 2) + quad + down, F32),
            vmem((2, 2) + pair + up, F32), vmem((2, 2) + pair + down, F32),
            vmem(per_chunk + up, F32), vmem(per_chunk + down, F32),
            vmem((4, ER, NOWN), F32),
            vmem((4, TB, CH), F32),
            vmem((3 * ER, DD), BF),
            vmem((ER, D), BF),
            vmem((NC, 2, D), BF),
            vmem((2, NOWN), jnp.int32),
            vmem((3, 8, 128), F32), vmem((NDEV, 128), F32),
            dma((4,)), dma((NG,)), dma((NCH,)), dma(()), dma((NG,)), dma(()), dma((FAR,)), dma(()), dma((NG,)), dma((NG,)), dma((NG,)),
            dma((5,)), dma((NCH,)), dma((4,)), dma((6,)), dma(quad), dma((4, 2)), dma((4, 2)),
            dma((2, NCH)), dma((6 * NCH, NCH)), dma(()), dma(()), dma(pair),
        ],
        compiler_params=pltpu.CompilerParams(
            collective_id=0, has_side_effects=True, vmem_limit_bytes=VMEM_BYTES),
        name='main',
    )(x, w1, w2r, heads, labels)


def result_kernel(rows_hbm, sh1_hbm, sh2_hbm, a_ref, g1_ref, g2_ref, rows, sh1, sh2, sem):
    ld_rows = pltpu.make_async_copy(rows_hbm, rows, sem.at[0])
    loads = [pltpu.make_async_copy(sh1_hbm, sh1, sem.at[1]), pltpu.make_async_copy(sh2_hbm, sh2, sem.at[2])]
    ld_rows.start()
    for cp in loads:
        cp.start()
    ld_rows.wait()

    gram = jnp.sum(rows[...], axis=0, keepdims=True)
    lane = lax.broadcasted_iota(jnp.int32, gram.shape, 1)

    def entry(i):
        return jnp.sum(jnp.where(lane == i, gram, 0.0), axis=1, keepdims=True)

    g00, g01, g11 = entry(0), entry(1), entry(2)
    scale = (g00 + g11) * -0.5
    g00, g01, g11 = g00 / scale, g01 / scale, g11 / scale
    a0 = a1 = jnp.full((1, 1), 0.5, F32)
    for _ in range(STEPS):
        v0 = a0 * jnp.exp(g00 * a0 + g01 * a1)
        v1 = a1 * jnp.exp(g01 * a0 + g11 * a1)
        tot = v0 + v1
        a0, a1 = v0 / tot, v1 / tot
    a_ref[0] = a0[0, 0]
    a_ref[1] = a1[0, 0]
    for cp in loads:
        cp.wait()
    for c in range(NCH):
        comb = a0 * sh1[c, 0] + a1 * sh1[c, 1]
        for g in range(8):
            col = g * NCH * GR + c * GR
            g1_ref[:, col:col + GR] = comb[:, g * GR:(g + 1) * GR]
        g2_ref[c * GR:(c + 1) * GR, :] = a0 * sh2[c, 0] + a1 * sh2[c, 1]


def result_call(rows, sh1, sh2):
    vspec = pl.BlockSpec(memory_space=pltpu.VMEM)
    anyspec = pl.BlockSpec(memory_space=pl.ANY)
    return pl.pallas_call(
        result_kernel,
        out_shape=(jax.ShapeDtypeStruct((2,), F32), jax.ShapeDtypeStruct((OWN, D), F32),
                   jax.ShapeDtypeStruct((OWN, D), F32)),
        in_specs=[anyspec] * NCH,
        out_specs=(pl.BlockSpec(memory_space=pltpu.SMEM), vspec, vspec),
        scratch_shapes=[pltpu.VMEM(v.shape, F32) for v in (rows, sh1, sh2)] + [pltpu.SemaphoreType.DMA((NCH,))],
        name='result',
    )(rows, sh1, sh2)


def solution(mesh):
    def local_step(tokens, w_up, w_down, task_heads, labels):
        w2r = w_down.reshape(8, NCH, GR, D)
        heads = jnp.transpose(task_heads, (2, 0, 1))
        _, sh1, sh2, rows = main_call(tokens, w_up, w2r, heads, labels)
        return result_call(rows, sh1, sh2)

    return jax.shard_map(
        local_step, mesh=mesh,
        in_specs=(P('data', None), P(None, 'model'), P('model', None), P(None, None, None), P(None, 'data')),
        out_specs=(P(None), P('data', 'model'), P(('model', 'data'), None)),
        check_vma=False)
```

```python
import jax
import jax.numpy as jnp
from jax import lax
from jax.experimental import pallas as pl
from jax.experimental.pallas import tpu as pltpu
from jax.sharding import PartitionSpec as P

STEPS = 20
BF = jnp.bfloat16
F32 = jnp.float32
MESH = pl.DeviceIdType.MESH
VMEM_BYTES = 67043328

D = 768
DD = D + D
NTOK = 8192
NOWN = 2048
TB = 1024
SUB = 256
NC = 19
ER = 40
CH = 256
NCH = 3
LAST = NCH - 1
NG = NCH * NCH
FAR = NG - NCH
GR = 32
OWN = CH // GR * 12
LO = slice(D)
HI = slice(D, DD)
SIDES = (LO, HI)
TWO = range(2)
MATES = range(1, 8)
LINE = range(1, 4)
BLOCKS = range(TB // SUB)
NDEV = 32

E_ON = ('', '1020', '1121', '30', '31')
IN_OTHER = ('', 't0o0', 't1o1i3', 't2o2i4', 's0i5', 's1T3o3')
IN_OWN = ('i6', 's2d0T4o4i7', 'd1i8', 's3T5o5g6')
IN_LOOP = ('d2g7s4', 'd3g8', 's5B6x6d4', 'B7x7', 'B8x8p6d5', 'p7', 'p8', '', '')

G0 = 0.7978845608028654
G1C = 0.044715 * G0


def dot_nn(a, b):
    return lax.dot_general(a, b, (((1,), (0,)), ((), ())), preferred_element_type=F32)


def dot_nt(a, b):
    return lax.dot_general(a, b, (((1,), (1,)), ((), ())), preferred_element_type=F32)


def dot_tn(a, b):
    return lax.dot_general(a, b, (((0,), (0,)), ((), ())), preferred_element_type=F32)


def gelu(x):
    t = jnp.tanh(x * (G0 + G1C * (x * x)))
    h = 0.5 * x
    return h + h * t


def gelu_and_slope(x):
    x2 = x * x
    t = jnp.tanh(x * (G0 + G1C * x2))
    h = 0.5 * x
    u = h + h * t
    s = 0.5 + 0.5 * t + h * (1.0 - t * t) * (G0 + (3.0 * G1C) * x2)
    return u, s


class Place:
    def __init__(self):
        self.z = lax.axis_index('model')
        self.j = lax.axis_index('data')
        self.core = self.j % 2
        self.x = (self.j // 2) % 2
        self.y = self.j // 4
        self.jc = self.j + 1 - 2 * self.core
        self.jx = self.j + 2 - 4 * self.x
        self.jy = self.j + 4 - 8 * self.y
        self.jd = self.jx + 4 - 8 * self.y
        self.js = self.jx + self.core * (self.jy - self.jx)
        self.j2 = self.jx + self.jy - self.js

        self.inner = self.z % 3 > 0
        self.pair = self.z + 1 - 2 * (self.z % 2)
        self.mirror = 3 - self.z
        half = self.z // 2
        self.shares = (self.z, self.pair, 2 - half, 3 - 3 * half)

    def share(self, k):
        own, near, far, end = self.shares
        return jnp.where(k == 0, own, jnp.where(k == 1, near, jnp.where(k == 2, far, end)))


def remote(src, dst, ssem, rsem, z, j):
    return pltpu.make_async_remote_copy(
        src_ref=src, dst_ref=dst, send_sem=ssem, recv_sem=rsem, device_id=(z, j), device_id_type=MESH)


class Scatter:
    def __init__(self, pos, acc, r1, r2, r3, lanes, sems, idx, x_first):
        self.pos, self.acc, self.r1, self.r2, self.r3 = pos, acc, r1, r2, r3
        self.lanes, self.sems, self.idx, self.x_first = lanes, sems, idx, x_first

    def copy(self, stage):
        p, ln = self.pos, self.lanes
        ssem, rsem = self.sems[0].at[stage], self.sems[1].at[self.idx, stage]
        if stage == 0:
            return remote(self.acc.at[:, :, 1 - p.core, :, ln], self.r1.at[:, :, :, ln], ssem, rsem, p.z, p.jc)
        if stage == 1:
            if self.x_first:
                return remote(self.acc.at[:, 1 - p.x, p.core, :, ln], self.r2.at[:, :, ln], ssem, rsem, p.z, p.jx)
            return remote(self.acc.at[1 - p.y, :, p.core, :, ln], self.r2.at[:, :, ln], ssem, rsem, p.z, p.jy)
        if self.x_first:
            return remote(self.acc.at[1 - p.y, p.x, p.core, :, ln], self.r3.at[:, ln], ssem, rsem, p.z, p.jy)
        return remote(self.acc.at[p.y, 1 - p.x, p.core, :, ln], self.r3.at[:, ln], ssem, rsem, p.z, p.jx)

    def start(self):
        self.copy(0).start()

    def side(self):
        p, ln = self.pos, self.lanes
        self.copy(0).wait_recv()
        for yy in TWO:
            for xx in TWO:
                self.acc[yy, xx, p.core, :, ln] += self.r1[yy, xx, :, ln]
        self.copy(1).start()

    def last(self):
        p, ln = self.pos, self.lanes
        self.copy(1).wait_recv()
        for i in TWO:
            if self.x_first:
                self.acc[i, p.x, p.core, :, ln] += self.r2[i, :, ln]
            else:
                self.acc[p.y, i, p.core, :, ln] += self.r2[i, :, ln]
        self.copy(2).start()

    def done(self):
        p, ln = self.pos, self.lanes
        self.copy(2).wait_recv()
        self.acc[p.y, p.x, p.core, :, ln] += self.r3[:, ln]


def main_kernel(x_hbm, w1_hbm, w2_hbm, heads_hbm, lab_hbm,
                a_hbm, sh1_hbm, sh2_hbm, rows_hbm,
                dz, wown, acc1, acc2, r1a, r1b, r2a, r2b, r3a, r3b, eall, ast, hbd, hcat, heads, lab_v,
                gm, mbuf,
                zss, zrs, zqs, xss, xrs, yss, yrs, dss, drs, css, crs,
                ld_sem, w2_sem, xs_sem, as_sem, ess, efs, ers,
                rss, rsr, mss, mrs, sh_sem):
    pos = Place()
    z, j, inner = pos.z, pos.j, pos.inner
    outer = jnp.logical_not(inner)

    barrier = pltpu.get_barrier_semaphore()
    me = z * 8 + j
    pl.semaphore_signal(barrier, device_id=(pos.pair, j), device_id_type=MESH)

    @pl.when(inner)
    def _():
        pl.semaphore_signal(barrier, device_id=(pos.mirror, j), device_id_type=MESH)

    for jj in (pos.jx, pos.jy, pos.jc):
        pl.semaphore_signal(barrier, device_id=(z, jj), device_id_type=MESH)

    own_x, act, room = dz.at[0], dz.at[2], dz.at[3]
    w1_raw = room.at[LO, LO]
    w1_own = dz.at[4, LO, HI]

    def sub(m):
        return slice((m % 4) * SUB, (m % 4 + 1) * SUB)

    def xo_at(m):
        return own_x.at[sub(m), HI if m >= 4 else LO]

    def share_row(k, b):
        return pl.multiple_of((pos.share(k) * 2 + b) * TB, TB)

    own_row = pl.multiple_of(z * NOWN, NOWN)
    ld_w1 = pltpu.make_async_copy(w1_hbm, w1_raw, ld_sem.at[0])
    ld_x = [pltpu.make_async_copy(x_hbm.at[pl.ds(own_row + b * TB, TB)], own_x.at[:, SIDES[b]], ld_sem.at[1 + b])
            for b in TWO]
    ld_l = pltpu.make_async_copy(lab_hbm.at[:, pl.ds(own_row, NOWN)], lab_v, ld_sem.at[3])
    ld_h = pltpu.make_async_copy(heads_hbm, heads, ld_sem.at[4])
    ld_w2 = [pltpu.make_async_copy(w2_hbm.at[:, c], wown.at[c, :, :, HI], w2_sem.at[c]) for c in range(NCH)]

    def stream_half(i):
        return dz.at[1 + 3 * (i % 2), :, LO]

    def xs_load(i):
        return pltpu.make_async_copy(
            x_hbm.at[pl.ds(share_row(1 + i // 2, i % 2), TB)], stream_half(i), xs_sem.at[i % 2])

    ld_h.start()
    ld_w1.start()
    for cp in ld_w2:
        cp.start()
    xs_load(0).start()
    for cp in ld_x:
        cp.start()
    ld_l.start()

    ld_h.wait()
    hf = jnp.concatenate([heads[i].astype(F32) for i in range(NC)] + [jnp.zeros((2, D), F32)], axis=0)
    hcat[...] = hf.astype(BF)
    r = lax.broadcasted_iota(jnp.int32, (ER, D), 0)
    hb = jnp.concatenate([jnp.where(r % 2 == 0, hf, 0.0), jnp.where(r % 2 == 1, hf, 0.0)], axis=1)
    hbd[...] = jnp.concatenate([hb, hb, hb], axis=0).astype(BF)
    gm[...] = jnp.zeros_like(gm)
    acc1[...] = jnp.zeros_like(acc1)

    ld_w1.wait()
    w1t = w1_raw[...].T
    for c in range(NCH):
        for g in range(8):
            row = g * NCH * GR + c * GR
            wown[c, g, :, LO] = w1t[row:row + GR, :]
    for cp in ld_w2:
        cp.wait()
    pl.semaphore_wait(barrier, 4 + z * pos.mirror // 2)

    def piece(i, jj):
        row = pl.multiple_of((i % NCH) * CH + jj * GR, GR)
        return dz.at[5 + i // NCH, pl.ds(row, GR), :]

    def rows_of(n, ssem, rsem):
        part = dz.at[5, pl.ds(0, n * GR), :]
        return remote(part, part, ssem, rsem, z, pos.jc)

    def z_pair(c):
        return remote(wown.at[c, j], piece(c, j), zss.at[0], zrs.at[c], pos.pair, j)

    def z_mirror(c):
        return remote(wown.at[c, j], piece(NCH + c, j), zss.at[1], zrs.at[NCH + c], pos.mirror, j)

    def z_forward(i):
        first = i < NCH
        to = jnp.where(first, i + 2 * NCH, i)
        return remote(piece(i, j), piece(to, j), zss.at[2], zrs.at[to], jnp.where(first, pos.mirror, pos.pair), j)

    def more_forward(i):
        first = i < NCH
        to = jnp.where(first, i + 2 * NCH, i)
        return remote(piece(i, pos.j2), piece(to, pos.j2), zss.at[3], zqs.at[to - FAR], jnp.where(first, pos.mirror, pos.pair), j)

    def side_copy(i):
        return remote(piece(i, j), piece(i, j), xss, xrs.at[i], z, pos.js)

    def more_copy(i):
        return remote(piece(i, pos.j2), piece(i, pos.j2), dss, drs.at[i], z, pos.js)

    def x_copy(i):
        return remote(piece(i, j), piece(i, j), xss, xrs.at[i], z, pos.jx)

    def y_copy(i):
        return remote(piece(i, j), piece(i, j), yss, yrs.at[i], z, pos.jy)

    def diag_copy_y(i):
        return remote(piece(i, pos.jx), piece(i, pos.jx), dss, drs.at[i], z, pos.jy)

    def diag_copy_x(i):
        return remote(piece(i, pos.jy), piece(i, pos.jy), dss, drs.at[i], z, pos.jx)

    def core_copy(i, q):
        jj = (j, pos.jx, pos.jy, pos.jd)[q]
        return remote(piece(i, jj), piece(i, jj), css.at[i], crs.at[i], z, pos.jc)

    def core_side(i, q):
        jj = (j, pos.js, pos.j2, pos.jd)[q]
        return remote(piece(i, jj), piece(i, jj), css.at[i], crs.at[i], z, pos.jc)

    def take(i):
        remote(piece(i, j), piece(i, j), zss.at[2], zrs.at[i], pos.pair, j).wait_recv()

        @pl.when(inner)
        def _():
            z_forward(i).start()

    def take_more(i):
        remote(piece(i, j), piece(i, j), zss.at[3], zqs.at[i - FAR], pos.pair, j).wait_recv()

        @pl.when(inner)
        def _():
            more_forward(i).start()

    def take_both(i):
        take(i)
        take_more(i)

    def send_both(i):
        side_copy(i).start()
        more_copy(i).start()
        core_side(i, 0).start()
        core_side(i, 2).start()

    def pass_both(i):
        side_copy(i).wait_recv()
        core_side(i, 1).start()
        more_copy(i).wait_recv()
        core_side(i, 3).start()

    def send_own(i):
        x_copy(i).start()
        y_copy(i).start()
        core_copy(i, 0).start()

    def send_side(i):
        x_copy(i).wait_recv()

        @pl.when(pos.core == 0)
        def _():
            diag_copy_y(i).start()

        core_copy(i, 1).start()
        y_copy(i).wait_recv()

        @pl.when(pos.core == 1)
        def _():
            diag_copy_x(i).start()

        core_copy(i, 2).start()

    def send_diag(i):
        diag_copy_y(i).wait_recv()
        core_copy(i, 3).start()

    def side_and_on(i):
        send_side(i)
        if i < NCH:
            @pl.when(inner)
            def _():
                more_forward(i).start()

    def when_inner(f):
        return lambda i: pl.when(inner)(lambda: f(i))

    def when_outer(f):
        return lambda i: pl.when(outer)(lambda: f(i))

    kinds = {'t': take, 'T': when_outer(take), 'i': when_inner(take), 'o': send_own, 's': side_and_on, 'd': send_diag,
             'g': when_inner(take_more), 'B': when_outer(take_both), 'x': send_both, 'p': pass_both}

    def events(codes):
        for kind, i in zip(codes[::2], codes[1::2]):
            kinds[kind](int(i))

    def events_at(i, table):
        for n, codes in enumerate(table):
            if codes:
                pl.when(i == n)(lambda codes=codes: events(codes))

    for c in range(NCH):
        z_pair(c).start()

    @pl.when(inner)
    def _():
        for c in range(NCH):
            z_mirror(c).start()

    def a_store(src, c, row, sem):
        return pltpu.make_async_copy(src, a_hbm.at[c, pl.ds(pl.multiple_of(row, TB), TB)], as_sem.at[sem])

    def forward(facc, u_own, w1_nat, w2_nat):
        for c in range(NCH):
            w1_own[:, c * CH:(c + 1) * CH] = wown[c, :, :, LO].reshape(CH, D).T

        def staged(i, c):
            rows = pl.ds(pl.multiple_of((i % 2) * TB, TB), TB)
            return a_store(facc.at[rows, c * CH:(c + 1) * CH], c, share_row(1 + i // 2, i % 2), (i % 2) * NCH + c)

        def other_tokens(i, carry):
            xs_load(i).wait()

            @pl.when(i < 5)
            def _():
                xs_load(i + 1).start()

            @pl.when(i >= 2)
            def _():
                for c in range(NCH):
                    staged(i, c).wait()

            base = (i % 2) * TB
            for m in BLOCKS:
                rows = pl.ds(pl.multiple_of(base + m * SUB, SUB), SUB)
                facc[rows, :] = dot_nn(stream_half(i)[sub(m), :], w1_own[...])
            for c in range(NCH):
                staged(i, c).start()

            events_at(i, IN_OTHER)
            return carry

        lax.fori_loop(0, 6, other_tokens, 0)
        for cp in ld_x:
            cp.wait()

        for b in TWO:
            for c in range(NCH):
                staged(b, c).wait()
            for m in BLOCKS:
                a = dot_nn(xo_at(b * 4 + m)[...], w1_own[...])
                for c in range(NCH):
                    ast[c, sub(m), :] = a[:, c * CH:(c + 1) * CH]
                act[sub(m), LO] = gelu(a).astype(BF)
            events(IN_OWN[2 * b])
            for m in BLOCKS:
                facc[b * TB + m * SUB:b * TB + (m + 1) * SUB, :] = dot_nn(
                    act[sub(m), LO], wown[:, :, :, HI].reshape(D, D))
            for c in range(NCH):
                a_store(ast.at[c], c, (z * 2 + b) * TB, c).start()
            events(IN_OWN[2 * b + 1])
            if b == 0:
                for c in range(NCH):
                    a_store(ast.at[c], c, z * NOWN, c).wait()

        def act_of(g):
            rows_of(4, css.at[g], crs.at[g]).wait_recv()
            gran = dz.at[5 + g // NCH, pl.ds(pl.multiple_of((g % NCH) * CH, CH), CH), :]
            w1_nat[...] = gran[:, LO].T
            w2_nat[...] = gran[:, HI]
            for m in range(8):
                u_own[m * SUB:(m + 1) * SUB, :] = gelu(dot_nn(xo_at(m)[...], w1_nat[...])).astype(BF)

        def granule(n, carry):
            act_of(jnp.where(n == FAR - 1, FAR, jnp.where(n == FAR, FAR - 1, n)))
            for m in range(8):
                rows = slice(m * SUB, (m + 1) * SUB)
                facc[rows, :] += dot_nn(u_own[rows, :], w2_nat[...])

            @pl.when(n == 0)
            def _():
                acc2[...] = jnp.zeros_like(acc2)

            events_at(n, IN_LOOP)

            return carry

        lax.fori_loop(0, NG - 1, granule, 0)
        act_of(NG - 1)
        for m in range(8):
            rows = slice(m * SUB, (m + 1) * SUB)
            out = facc[rows, :] + dot_nn(u_own[rows, :], w2_nat[...])
            xo_at(m)[...] = (xo_at(m)[...].astype(F32) + out).astype(BF)

    pl.run_scoped(forward, pltpu.VMEM((NOWN, D), F32), pltpu.VMEM((NOWN, CH), BF), pltpu.VMEM((D, CH), BF),
                  pltpu.VMEM((CH, D), BF))

    for c in range(NCH):
        a_store(ast.at[c], c, z * NOWN, c).wait()

    def e_half(k, b):
        return eall.at[k, :, pl.ds(pl.multiple_of(b * TB, TB), TB)]

    def e_pair(b):
        return remote(e_half(0, b), e_half(1, b), ess.at[0, b], ers.at[1, b], pos.pair, j)

    def e_mirror(b):
        return remote(e_half(0, b), e_half(2, b), ess.at[1, b], ers.at[2, b], pos.mirror, j)

    def e_forward(k, b):
        to = 3 if k == 1 else k
        return remote(e_half(k, b), e_half(to, b), efs.at[k, b], ers.at[to, b], pos.mirror if k == 1 else pos.pair, j)

    def e_wait(k, b):
        remote(e_half(k, b), e_half(k, b), efs.at[k, b], ers.at[k, b], pos.pair, j).wait_recv()

    def step_of(s):
        return s // 8, (s % 8) // 2, s % 2

    def a_load(s, slot):
        c, k, b = step_of(s)
        return pltpu.make_async_copy(a_hbm.at[c, pl.ds(share_row(k, b), TB)], ast.at[slot], as_sem.at[slot])

    everything = slice(None)
    up_sems, down_sems = (rss.at[0], rsr), (rss.at[1], rsr)

    def up(c, t):
        return Scatter(pos, acc1.at[c, t], r1a.at[c % 2, t], r2a.at[c % 2, t], r3a.at[c, t], everything, up_sems,
                       c * 6 + t, t == 0)

    def down(c, t, part=None):
        if part is None:
            lanes, idx, x_first = everything, c * 6 + 2 + t, t == 0
        else:
            lanes, idx, x_first = slice(part * (D // 2), (part + 1) * (D // 2)), c * 6 + 2 + t * 2 + part, part == 0
        return Scatter(pos, acc2.at[c, t], r1b.at[c % 2, t], r2b.at[c % 2, t], r3b.at[c, t], lanes, down_sems, idx, x_first)

    ups = [[up(c, t) for t in TWO] for c in range(NCH)]
    downs = [[down(c, t) for t in TWO] for c in range(LAST)]
    tails = [[down(LAST, t, part) for part in TWO] for t in TWO]

    def each(group, stage):
        for sc in group:
            getattr(sc, stage)()

    def fold(v):
        rows, cols = v.shape
        total = jnp.zeros((8, 128), F32)
        for q in range(cols // 128):
            total = total + jnp.sum(v[:, q * 128:(q + 1) * 128].reshape(rows // 8, 8, 128), axis=0)
        return total

    def shard(acc, c, t):
        return acc.at[c, t, pos.y, pos.x, pos.core]

    def out_copy(acc, out, c, sem, t):
        return pltpu.make_async_copy(shard(acc, c, t), out.at[c, t], sh_sem.at[sem])

    def finish(acc, out, c, sem):
        v0, v1 = shard(acc, c, 0)[...], shard(acc, c, 1)[...]
        gm[0] += fold(v0 * v0)
        gm[1] += fold(v0 * v1)
        gm[2] += fold(v1 * v1)
        for t in TWO:
            out_copy(acc, out, c, sem, t).start()

    def finish_chunk(c):
        each(ups[c] + downs[c], 'done')
        finish(acc1, sh1_hbm, c, 0)
        finish(acc2, sh2_hbm, c, 1)

    def backward(us_all, das, xbuf):
        def x_load(s, slot):
            _, k, b = step_of(s)
            return pltpu.make_async_copy(x_hbm.at[pl.ds(share_row(k, b), TB)], xbuf.at[slot], xs_sem.at[slot])

        def pair_slot(p):
            return 2 * ((p + 1) % 2)

        def load_pair(p, act):
            for b in TWO:
                getattr(a_load(p * 2 + b, pair_slot(p) + b), act)()
                getattr(x_load(p * 2 + b, pair_slot(p) + b), act)()

        a_load(0, 0).start()
        x_load(0, 0).start()

        ld_l.wait()
        r = lax.broadcasted_iota(jnp.int32, (ER, TB), 0)
        first = r % 2 == 0
        real = r < 2 * NC
        neg = jnp.float32(-jnp.inf)
        for b in TWO:
            cols = slice(b * TB, (b + 1) * TB)
            logit = jnp.where(real, dot_nt(hcat[...], own_x[:, SIDES[b]]), neg)
            m0 = jnp.max(jnp.where(first, logit, neg), axis=0, keepdims=True)
            m1 = jnp.max(jnp.where(first, neg, logit), axis=0, keepdims=True)
            ex = jnp.exp(logit - jnp.where(first, m0, m1))
            s0 = jnp.sum(jnp.where(first, ex, 0.0), axis=0, keepdims=True)
            s1 = jnp.sum(jnp.where(first, 0.0, ex), axis=0, keepdims=True)
            prob = ex / jnp.where(first, s0, s1)
            lab = jnp.where(first, lab_v[0:1, cols], lab_v[1:2, cols])
            hot = jnp.where(jnp.logical_and(r // 2 == lab, real), 1.0, 0.0)
            eall[0, :, cols] = (prob - hot) / (NTOK * 8.0)
            e_pair(b).start()

            @pl.when(inner)
            def _():
                e_mirror(b).start()

        rows_of(NG, xss, xrs.at[0]).wait_send()
        rows_of(FAR, yss, yrs.at[0]).wait_send()
        rows_of(NG, dss, drs.at[0]).wait_send()
        for i in range(NG):
            rows_of(4, css.at[i], crs.at[i]).wait_send()
        rows_of(NCH, zss.at[0], zrs.at[0]).wait_send()

        @pl.when(inner)
        def _():
            for n, i in ((NCH, 1), (NG, 2), (FAR, 3)):
                rows_of(n, zss.at[i], zrs.at[0]).wait_send()

        def d_act(src, t, sl, c, us, rows):
            w2c = wown[c, :, :, HI].reshape(CH, D)
            u, slope = gelu_and_slope(src[...])
            us[rows, :] = u.astype(BF)
            for task in TWO:
                da = dot_nt(dz[t, sl, SIDES[task]], w2c)
                das[rows, task * CH:(task + 1) * CH] = (da * slope).astype(BF)

        def add_up(c, g):
            for task in TWO:
                acc1[c, task] += g[:, task * CH:(task + 1) * CH].reshape(acc1.shape[2:])

        def add_down(c, g):
            for task in TWO:
                acc2[c, task] += g[:, SIDES[task]].reshape(acc2.shape[2:])

        def e_parts(s):
            _, k, b = step_of(s)
            e = e_half(k, b)[...]
            e1 = e.astype(BF).astype(F32)
            rest = e - e1
            e2 = rest.astype(BF).astype(F32)
            e3 = rest - e2
            return jnp.concatenate([e1, e2, e3], axis=0).astype(BF)

        def first_step(s, carry):
            _, k, b = step_of(s)
            t = k * 2 + b
            a_load(s, s % 2).wait()
            x_load(s, s % 2).wait()

            @pl.when(s < 7)
            def _():
                a_load(s + 1, (s + 1) % 2).start()
                x_load(s + 1, (s + 1) % 2).start()

            @pl.when(s == 7)
            def _():
                load_pair(4, 'start')

            @pl.when(jnp.logical_and(outer, k > 0))
            def _():
                e_wait(k, b)

            es = e_parts(s)
            for m in BLOCKS:
                dz[t, sub(m), :] = dot_tn(es[:, sub(m)], hbd[...]).astype(BF)
            us = us_all.at[0]
            for m in BLOCKS:
                d_act(ast.at[s % 2, sub(m)], t, sub(m), 0, us, sub(m))
            add_up(0, dot_tn(xbuf[s % 2], das[:TB]))
            add_down(0, dot_tn(us[:TB], dz[t]))

            for when, codes in enumerate(E_ON):
                if codes:
                    @pl.when(jnp.logical_and(s == when, inner))
                    def _():
                        for k_f, b_f in zip(codes[::2], codes[1::2]):
                            e_forward_after_wait(int(k_f), int(b_f))

            return carry

        def pair_front(p, c):
            k = p % 4
            load_pair(p, 'wait')

            @pl.when(p < 11)
            def _():
                load_pair(p + 1, 'start')

            for b in TWO:
                for m in BLOCKS:
                    rows = slice(b * TB + m * SUB, b * TB + (m + 1) * SUB)
                    d_act(ast.at[pair_slot(p) + b, sub(m)], k * 2 + b, sub(m), c, us_all.at[k], rows)
            add_up(c, dot_tn(xbuf[pl.ds(pair_slot(p), 2)].reshape(NOWN, D), das[...]))

        def step(p, carry):
            k = p % 4
            pair_front(p, 1)
            add_down(1, dot_tn(us_all[k], dz[pl.ds(k * 2, 2)].reshape(NOWN, DD)))

            @pl.when(p == 4)
            def _():
                each(ups[0] + downs[0], 'side')

            @pl.when(p == 6)
            def _():
                each(ups[0] + downs[0], 'last')

            return carry

        def e_forward_after_wait(k, b):
            e_wait(k, b)
            e_forward(k, b).start()

        lax.fori_loop(0, 8, first_step, 0)
        each(ups[0] + downs[0], 'start')
        lax.fori_loop(4, 8, step, 0)
        each(ups[1] + downs[1], 'start')

        def last_step(p, carry):
            pair_front(p, LAST)

            @pl.when(p == 8)
            def _():
                finish_chunk(0)
                each(ups[1], 'side')

            @pl.when(p == 9)
            def _():
                each(downs[1], 'side')

            @pl.when(p == 10)
            def _():
                each(ups[1], 'last')

            return carry

        lax.fori_loop(8, 12, last_step, 0)
        each(ups[LAST], 'start')
        each(downs[1], 'last')

        def down_pass(task):
            def half(i, carry):
                u = us_all[pl.ds(i * 2, 2)].reshape(4 * TB, CH)
                d = dz[pl.ds(i * 4, 4), :, SIDES[task]].reshape(4 * TB, D)
                acc2[LAST, task] += dot_tn(u, d).reshape(acc2.shape[2:])

                @pl.when(i == 0)
                def _():
                    each(ups[LAST] if task == 0 else tails[0], 'side')

                return carry

            lax.fori_loop(0, 2, half, 0)
            each(tails[task], 'start')

        down_pass(0)
        finish_chunk(1)
        down_pass(1)

    pl.run_scoped(backward, pltpu.VMEM((4, NOWN, CH), BF), pltpu.VMEM((NOWN, 2 * CH), BF),
                  pltpu.VMEM((4, TB, D), BF))

    each(ups[LAST], 'last')
    each(tails[1], 'side')
    each(tails[0], 'last')
    each(ups[LAST], 'done')
    finish(acc1, sh1_hbm, LAST, 0)
    each(tails[1], 'last')
    each(tails[0], 'done')
    each(tails[1], 'done')
    finish(acc2, sh2_hbm, LAST, 1)

    def full(v):
        return jnp.sum(jnp.sum(v, axis=0, keepdims=True), axis=1, keepdims=True)

    lane = lax.broadcasted_iota(jnp.int32, (1, 128), 1)
    mbuf[pl.ds(me, 1), :] = jnp.where(lane == 0, full(gm[0]), jnp.where(lane == 1, full(gm[1]), full(gm[2])))

    def row_of(ref):
        return ref.at[pl.ds(me, 1), :]

    keep = pltpu.make_async_copy(row_of(mbuf), row_of(rows_hbm), ld_sem.at[0])
    keep.start()

    def m_send(to_z, to_j):
        remote(row_of(mbuf), row_of(rows_hbm), mss, mrs, to_z, to_j).start()

    mates = [(j + i) % 8 for i in MATES]
    for to_z in reversed(pos.shares[1:]):
        for to_j in [j] + mates:
            m_send(to_z, to_j)
    for to_j in mates:
        m_send(z, to_j)

    for b in TWO:
        e_pair(b).wait_send()

        @pl.when(inner)
        def _():
            e_mirror(b).wait_send()
            for k in LINE:
                e_forward(k, b).wait_send()

    for kind, acc in enumerate((acc1, acc2)):
        for stage, part in enumerate((acc.at[:, :, :, :, 0], acc.at[:, :, :, 0, 0], acc.at[:, :, 0, 0, 0])):
            remote(part, part, rss.at[kind, stage], rsr.at[0, stage], z, pos.jc).wait_send()
    pltpu.make_async_copy(r3a, sh1_hbm, sh_sem.at[0]).wait()
    pltpu.make_async_copy(r3b, sh2_hbm, sh_sem.at[1]).wait()

    keep.wait()
    lines = pl.ds(0, NDEV - 1)
    remote(mbuf.at[lines, :], rows_hbm.at[lines, :], mss, mrs, z, pos.jc).wait()


def main_call(x, w1, w2r, heads, labels):
    dma = pltpu.SemaphoreType.DMA
    anyspec = pl.BlockSpec(memory_space=pl.ANY)
    up, down = (OWN, CH), (GR, D)
    pair, quad, octet = (2,), (2, 2), (2, 2, 2)
    per_chunk = (NCH, 2)
    vmem = pltpu.VMEM
    return pl.pallas_call(
        main_kernel,
        out_shape=(jax.ShapeDtypeStruct((NCH, NTOK, CH), F32),
                   jax.ShapeDtypeStruct(per_chunk + up, F32),
                   jax.ShapeDtypeStruct(per_chunk + down, F32),
                   jax.ShapeDtypeStruct((NDEV, 128), F32)),
        in_specs=[anyspec] * 5,
        out_specs=(anyspec, anyspec, anyspec, anyspec),
        scratch_shapes=[
            vmem((8, TB, DD), BF),
            vmem((NCH, 8, GR, DD), BF),
            vmem(per_chunk + octet + up, F32), vmem(per_chunk + octet + down, F32),
            vmem((2, 2) + quad + up, F32), vmem((2, 2) + quad + down, F32),
            vmem((2, 2) + pair + up, F32), vmem((2, 2) + pair + down, F32),
            vmem(per_chunk + up, F32), vmem(per_chunk + down, F32),
            vmem((4, ER, NOWN), F32),
            vmem((4, TB, CH), F32),
            vmem((3 * ER, DD), BF),
            vmem((ER, D), BF),
            vmem((NC, 2, D), BF),
            vmem((2, NOWN), jnp.int32),
            vmem((3, 8, 128), F32), vmem((NDEV, 128), F32),
            dma((4,)), dma((NG,)), dma((NCH,)), dma(()), dma((NG,)), dma(()), dma((FAR,)), dma(()), dma((NG,)), dma((NG,)), dma((NG,)),
            dma((5,)), dma((NCH,)), dma((4,)), dma((6,)), dma(quad), dma((4, 2)), dma((4, 2)),
            dma((2, NCH)), dma((6 * NCH, NCH)), dma(()), dma(()), dma(pair),
        ],
        compiler_params=pltpu.CompilerParams(
            collective_id=0, has_side_effects=True, vmem_limit_bytes=VMEM_BYTES),
        name='main',
    )(x, w1, w2r, heads, labels)


def result_kernel(rows_hbm, sh1_hbm, sh2_hbm, a_ref, g1_ref, g2_ref, rows, sh1, sh2, sem):
    ld_rows = pltpu.make_async_copy(rows_hbm, rows, sem.at[0])
    loads = [pltpu.make_async_copy(sh1_hbm, sh1, sem.at[1]), pltpu.make_async_copy(sh2_hbm, sh2, sem.at[2])]
    ld_rows.start()
    for cp in loads:
        cp.start()
    ld_rows.wait()

    gram = jnp.sum(rows[...], axis=0, keepdims=True)
    lane = lax.broadcasted_iota(jnp.int32, gram.shape, 1)

    def entry(i):
        return jnp.sum(jnp.where(lane == i, gram, 0.0), axis=1, keepdims=True)

    g00, g01, g11 = entry(0), entry(1), entry(2)
    scale = (g00 + g11) * -0.5
    g00, g01, g11 = g00 / scale, g01 / scale, g11 / scale
    a0 = a1 = jnp.full((1, 1), 0.5, F32)
    for _ in range(STEPS):
        v0 = a0 * jnp.exp(g00 * a0 + g01 * a1)
        v1 = a1 * jnp.exp(g01 * a0 + g11 * a1)
        tot = v0 + v1
        a0, a1 = v0 / tot, v1 / tot
    a_ref[0] = a0[0, 0]
    a_ref[1] = a1[0, 0]
    for cp in loads:
        cp.wait()
    for c in range(NCH):
        comb = a0 * sh1[c, 0] + a1 * sh1[c, 1]
        for g in range(8):
            col = g * NCH * GR + c * GR
            g1_ref[:, col:col + GR] = comb[:, g * GR:(g + 1) * GR]
        g2_ref[c * GR:(c + 1) * GR, :] = a0 * sh2[c, 0] + a1 * sh2[c, 1]


def result_call(rows, sh1, sh2):
    vspec = pl.BlockSpec(memory_space=pltpu.VMEM)
    anyspec = pl.BlockSpec(memory_space=pl.ANY)
    return pl.pallas_call(
        result_kernel,
        out_shape=(jax.ShapeDtypeStruct((2,), F32), jax.ShapeDtypeStruct((OWN, D), F32),
                   jax.ShapeDtypeStruct((OWN, D), F32)),
        in_specs=[anyspec] * NCH,
        out_specs=(pl.BlockSpec(memory_space=pltpu.SMEM), vspec, vspec),
        scratch_shapes=[pltpu.VMEM(v.shape, F32) for v in (rows, sh1, sh2)] + [pltpu.SemaphoreType.DMA((NCH,))],
        name='result',
    )(rows, sh1, sh2)


def solution(mesh):
    def local_step(tokens, w_up, w_down, task_heads, labels):
        w2r = w_down.reshape(8, NCH, GR, D)
        heads = jnp.transpose(task_heads, (2, 0, 1))
        _, sh1, sh2, rows = main_call(tokens, w_up, w2r, heads, labels)
        return result_call(rows, sh1, sh2)

    return jax.shard_map(
        local_step, mesh=mesh,
        in_specs=(P('data', None), P(None, 'model'), P('model', None), P(None, None, None), P(None, 'data')),
        out_specs=(P(None), P('data', 'model'), P(('model', 'data'), None)),
        check_vma=False)
```

```python
import jax
import jax.numpy as jnp
from jax import lax
from jax.experimental import pallas as pl
from jax.experimental.pallas import tpu as pltpu
from jax.sharding import PartitionSpec as P

STEPS = 20
BF = jnp.bfloat16
F32 = jnp.float32
MESH = pl.DeviceIdType.MESH
VMEM_BYTES = 67043328

D = 768
DD = D + D
NTOK = 8192
NOWN = 2048
TB = 1024
SUB = 256
NC = 19
ER = 40
CH = 256
NCH = 3
LAST = NCH - 1
NG = NCH * NCH
FAR = NG - NCH
GR = 32
OWN = CH // GR * 12
LO = slice(D)
HI = slice(D, DD)
SIDES = (LO, HI)
TWO = range(2)
MATES = range(1, 8)
LINE = range(1, 4)
BLOCKS = range(TB // SUB)
NDEV = 32

E_ON = ('', '1020', '1121', '30', '31')
IN_OTHER = ('', 't0o0', 't1o1i3', 't2o2i4', 's0i5', 's1T3o3')
IN_OWN = ('i6', 's2d0T4o4i7', 'd1i8', 's3T5o5g6')
IN_LOOP = ('d2g7s4', 'd3g8', 's5B6x6d4', 'B7x7', 'B8x8p6d5', 'p7', 'p8', '', '')

G0 = 0.7978845608028654
G1C = 0.044715 * G0


def dot_nn(a, b):
    return lax.dot_general(a, b, (((1,), (0,)), ((), ())), preferred_element_type=F32)


def dot_nt(a, b):
    return lax.dot_general(a, b, (((1,), (1,)), ((), ())), preferred_element_type=F32)


def dot_tn(a, b):
    return lax.dot_general(a, b, (((0,), (0,)), ((), ())), preferred_element_type=F32)


def gelu(x):
    t = jnp.tanh(x * (G0 + G1C * (x * x)))
    h = 0.5 * x
    return h + h * t


def gelu_and_slope(x):
    x2 = x * x
    t = jnp.tanh(x * (G0 + G1C * x2))
    h = 0.5 * x
    u = h + h * t
    s = 0.5 + 0.5 * t + h * (1.0 - t * t) * (G0 + (3.0 * G1C) * x2)
    return u, s


class Place:
    def __init__(self):
        self.z = lax.axis_index('model')
        self.j = lax.axis_index('data')
        self.core = self.j % 2
        self.x = (self.j // 2) % 2
        self.y = self.j // 4
        self.jc = self.j + 1 - 2 * self.core
        self.jx = self.j + 2 - 4 * self.x
        self.jy = self.j + 4 - 8 * self.y
        self.jd = self.jx + 4 - 8 * self.y
        self.js = self.jx + self.core * (self.jy - self.jx)
        self.j2 = self.jx + self.jy - self.js

        self.inner = self.z % 3 > 0
        self.pair = self.z + 1 - 2 * (self.z % 2)
        self.mirror = 3 - self.z
        half = self.z // 2
        self.shares = (self.z, self.pair, 2 - half, 3 - 3 * half)

    def share(self, k):
        own, near, far, end = self.shares
        return jnp.where(k == 0, own, jnp.where(k == 1, near, jnp.where(k == 2, far, end)))


def remote(src, dst, ssem, rsem, z, j):
    return pltpu.make_async_remote_copy(
        src_ref=src, dst_ref=dst, send_sem=ssem, recv_sem=rsem, device_id=(z, j), device_id_type=MESH)


class Scatter:
    def __init__(self, pos, acc, r1, r2, r3, lanes, sems, idx, x_first):
        self.pos, self.acc, self.r1, self.r2, self.r3 = pos, acc, r1, r2, r3
        self.lanes, self.sems, self.idx, self.x_first = lanes, sems, idx, x_first

    def copy(self, stage):
        p, ln = self.pos, self.lanes
        ssem, rsem = self.sems[0].at[stage], self.sems[1].at[self.idx, stage]
        if stage == 0:
            return remote(self.acc.at[:, :, 1 - p.core, :, ln], self.r1.at[:, :, :, ln], ssem, rsem, p.z, p.jc)
        if stage == 1:
            if self.x_first:
                return remote(self.acc.at[:, 1 - p.x, p.core, :, ln], self.r2.at[:, :, ln], ssem, rsem, p.z, p.jx)
            return remote(self.acc.at[1 - p.y, :, p.core, :, ln], self.r2.at[:, :, ln], ssem, rsem, p.z, p.jy)
        if self.x_first:
            return remote(self.acc.at[1 - p.y, p.x, p.core, :, ln], self.r3.at[:, ln], ssem, rsem, p.z, p.jy)
        return remote(self.acc.at[p.y, 1 - p.x, p.core, :, ln], self.r3.at[:, ln], ssem, rsem, p.z, p.jx)

    def start(self):
        self.copy(0).start()

    def side(self):
        p, ln = self.pos, self.lanes
        self.copy(0).wait_recv()
        for yy in TWO:
            for xx in TWO:
                self.acc[yy, xx, p.core, :, ln] += self.r1[yy, xx, :, ln]
        self.copy(1).start()

    def last(self):
        p, ln = self.pos, self.lanes
        self.copy(1).wait_recv()
        for i in TWO:
            if self.x_first:
                self.acc[i, p.x, p.core, :, ln] += self.r2[i, :, ln]
            else:
                self.acc[p.y, i, p.core, :, ln] += self.r2[i, :, ln]
        self.copy(2).start()

    def done(self):
        p, ln = self.pos, self.lanes
        self.copy(2).wait_recv()
        self.acc[p.y, p.x, p.core, :, ln] += self.r3[:, ln]


def main_kernel(x_hbm, w1_hbm, w2_hbm, heads_hbm, lab_hbm,
                a_hbm, sh1_hbm, sh2_hbm, rows_hbm,
                dz, wown, acc1, acc2, r1a, r1b, r2a, r2b, r3a, r3b, eall, ast, hbd, hcat, heads, lab_v,
                gm, mbuf,
                zss, zrs, zqs, xss, xrs, yss, yrs, dss, drs, css, crs,
                ld_sem, w2_sem, xs_sem, as_sem, ess, efs, ers,
                rss, rsr, mss, mrs, sh_sem):
    pos = Place()
    z, j, inner = pos.z, pos.j, pos.inner
    outer = jnp.logical_not(inner)

    barrier = pltpu.get_barrier_semaphore()
    me = z * 8 + j
    pl.semaphore_signal(barrier, device_id=(pos.pair, j), device_id_type=MESH)

    @pl.when(inner)
    def _():
        pl.semaphore_signal(barrier, device_id=(pos.mirror, j), device_id_type=MESH)

    for jj in (pos.jx, pos.jy, pos.jc):
        pl.semaphore_signal(barrier, device_id=(z, jj), device_id_type=MESH)

    own_x, act, room = dz.at[0], dz.at[2], dz.at[3]
    w1_raw = room.at[LO, LO]
    w1_own = dz.at[4, LO, HI]

    def sub(m):
        return slice((m % 4) * SUB, (m % 4 + 1) * SUB)

    def xo_at(m):
        return own_x.at[sub(m), HI if m >= 4 else LO]

    def share_row(k, b):
        return pl.multiple_of((pos.share(k) * 2 + b) * TB, TB)

    own_row = pl.multiple_of(z * NOWN, NOWN)
    ld_w1 = pltpu.make_async_copy(w1_hbm, w1_raw, ld_sem.at[0])
    ld_x = [pltpu.make_async_copy(x_hbm.at[pl.ds(own_row + b * TB, TB)], own_x.at[:, SIDES[b]], ld_sem.at[1 + b])
            for b in TWO]
    ld_l = pltpu.make_async_copy(lab_hbm.at[:, pl.ds(own_row, NOWN)], lab_v, ld_sem.at[3])
    ld_h = pltpu.make_async_copy(heads_hbm, heads, ld_sem.at[4])
    ld_w2 = [pltpu.make_async_copy(w2_hbm.at[:, c], wown.at[c, :, :, HI], w2_sem.at[c]) for c in range(NCH)]

    def stream_half(i):
        return dz.at[1 + 3 * (i % 2), :, LO]

    def xs_load(i):
        return pltpu.make_async_copy(
            x_hbm.at[pl.ds(share_row(1 + i // 2, i % 2), TB)], stream_half(i), xs_sem.at[i % 2])

    ld_h.start()
    ld_w1.start()
    for cp in ld_w2:
        cp.start()
    xs_load(0).start()
    for cp in ld_x:
        cp.start()
    ld_l.start()

    ld_h.wait()
    hf = jnp.concatenate([heads[i].astype(F32) for i in range(NC)] + [jnp.zeros((2, D), F32)], axis=0)
    hcat[...] = hf.astype(BF)
    r = lax.broadcasted_iota(jnp.int32, (ER, D), 0)
    hb = jnp.concatenate([jnp.where(r % 2 == 0, hf, 0.0), jnp.where(r % 2 == 1, hf, 0.0)], axis=1)
    hbd[...] = jnp.concatenate([hb, hb, hb], axis=0).astype(BF)
    gm[...] = jnp.zeros_like(gm)
    acc1[...] = jnp.zeros_like(acc1)

    ld_w1.wait()
    w1t = w1_raw[...].T
    for c in range(NCH):
        for g in range(8):
            row = g * NCH * GR + c * GR
            wown[c, g, :, LO] = w1t[row:row + GR, :]
    for cp in ld_w2:
        cp.wait()
    pl.semaphore_wait(barrier, 4 + z * pos.mirror // 2)

    def piece(i, jj):
        row = pl.multiple_of((i % NCH) * CH + jj * GR, GR)
        return dz.at[5 + i // NCH, pl.ds(row, GR), :]

    def rows_of(n, ssem, rsem):
        part = dz.at[5, pl.ds(0, n * GR), :]
        return remote(part, part, ssem, rsem, z, pos.jc)

    def z_pair(c):
        return remote(wown.at[c, j], piece(c, j), zss.at[0], zrs.at[c], pos.pair, j)

    def z_mirror(c):
        return remote(wown.at[c, j], piece(NCH + c, j), zss.at[1], zrs.at[NCH + c], pos.mirror, j)

    def z_forward(i):
        first = i < NCH
        to = jnp.where(first, i + 2 * NCH, i)
        return remote(piece(i, j), piece(to, j), zss.at[2], zrs.at[to], jnp.where(first, pos.mirror, pos.pair), j)

    def more_forward(i):
        first = i < NCH
        to = jnp.where(first, i + 2 * NCH, i)
        return remote(piece(i, pos.j2), piece(to, pos.j2), zss.at[3], zqs.at[to - FAR], jnp.where(first, pos.mirror, pos.pair), j)

    def side_copy(i):
        return remote(piece(i, j), piece(i, j), xss, xrs.at[i], z, pos.js)

    def more_copy(i):
        return remote(piece(i, pos.j2), piece(i, pos.j2), dss, drs.at[i], z, pos.js)

    def x_copy(i):
        return remote(piece(i, j), piece(i, j), xss, xrs.at[i], z, pos.jx)

    def y_copy(i):
        return remote(piece(i, j), piece(i, j), yss, yrs.at[i], z, pos.jy)

    def diag_copy_y(i):
        return remote(piece(i, pos.jx), piece(i, pos.jx), dss, drs.at[i], z, pos.jy)

    def diag_copy_x(i):
        return remote(piece(i, pos.jy), piece(i, pos.jy), dss, drs.at[i], z, pos.jx)

    def core_copy(i, q):
        jj = (j, pos.jx, pos.jy, pos.jd)[q]
        return remote(piece(i, jj), piece(i, jj), css, crs.at[i], z, pos.jc)

    def core_side(i, q):
        jj = (j, pos.js, pos.j2, pos.jd)[q]
        return remote(piece(i, jj), piece(i, jj), css, crs.at[i], z, pos.jc)

    def take(i):
        remote(piece(i, j), piece(i, j), zss.at[2], zrs.at[i], pos.pair, j).wait_recv()

        @pl.when(inner)
        def _():
            z_forward(i).start()

    def take_more(i):
        remote(piece(i, j), piece(i, j), zss.at[3], zqs.at[i - FAR], pos.pair, j).wait_recv()

        @pl.when(inner)
        def _():
            more_forward(i).start()

    def take_both(i):
        take(i)
        take_more(i)

    def send_both(i):
        side_copy(i).start()
        more_copy(i).start()
        core_side(i, 0).start()
        core_side(i, 2).start()

    def pass_both(i):
        side_copy(i).wait_recv()
        core_side(i, 1).start()
        more_copy(i).wait_recv()
        core_side(i, 3).start()

    def send_own(i):
        x_copy(i).start()
        y_copy(i).start()
        core_copy(i, 0).start()

    def send_side(i):
        x_copy(i).wait_recv()

        @pl.when(pos.core == 0)
        def _():
            diag_copy_y(i).start()

        core_copy(i, 1).start()
        y_copy(i).wait_recv()

        @pl.when(pos.core == 1)
        def _():
            diag_copy_x(i).start()

        core_copy(i, 2).start()

    def send_diag(i):
        diag_copy_y(i).wait_recv()
        core_copy(i, 3).start()

    def side_and_on(i):
        send_side(i)
        if i < NCH:
            @pl.when(inner)
            def _():
                more_forward(i).start()

    def when_inner(f):
        return lambda i: pl.when(inner)(lambda: f(i))

    def when_outer(f):
        return lambda i: pl.when(outer)(lambda: f(i))

    kinds = {'t': take, 'T': when_outer(take), 'i': when_inner(take), 'o': send_own, 's': side_and_on, 'd': send_diag,
             'g': when_inner(take_more), 'B': when_outer(take_both), 'x': send_both, 'p': pass_both}

    def events(codes):
        for kind, i in zip(codes[::2], codes[1::2]):
            kinds[kind](int(i))

    def events_at(i, table):
        for n, codes in enumerate(table):
            if codes:
                pl.when(i == n)(lambda codes=codes: events(codes))

    for c in range(NCH):
        z_pair(c).start()

    @pl.when(inner)
    def _():
        for c in range(NCH):
            z_mirror(c).start()

    def a_store(src, c, row, sem):
        return pltpu.make_async_copy(src, a_hbm.at[c, pl.ds(pl.multiple_of(row, TB), TB)], as_sem.at[sem])

    def forward(facc, u_own, w1_nat, w2_nat):
        for c in range(NCH):
            w1_own[:, c * CH:(c + 1) * CH] = wown[c, :, :, LO].reshape(CH, D).T

        def staged(i, c):
            rows = pl.ds(pl.multiple_of((i % 2) * TB, TB), TB)
            return a_store(facc.at[rows, c * CH:(c + 1) * CH], c, share_row(1 + i // 2, i % 2), (i % 2) * NCH + c)

        def other_tokens(i, carry):
            xs_load(i).wait()

            @pl.when(i < 5)
            def _():
                xs_load(i + 1).start()

            @pl.when(i >= 2)
            def _():
                for c in range(NCH):
                    staged(i, c).wait()

            base = (i % 2) * TB
            for m in BLOCKS:
                rows = pl.ds(pl.multiple_of(base + m * SUB, SUB), SUB)
                facc[rows, :] = dot_nn(stream_half(i)[sub(m), :], w1_own[...])
            for c in range(NCH):
                staged(i, c).start()

            events_at(i, IN_OTHER)
            return carry

        lax.fori_loop(0, 6, other_tokens, 0)
        for cp in ld_x:
            cp.wait()

        for b in TWO:
            for c in range(NCH):
                staged(b, c).wait()
            for m in BLOCKS:
                a = dot_nn(xo_at(b * 4 + m)[...], w1_own[...])
                for c in range(NCH):
                    ast[c, sub(m), :] = a[:, c * CH:(c + 1) * CH]
                act[sub(m), LO] = gelu(a).astype(BF)
            events(IN_OWN[2 * b])
            for m in BLOCKS:
                facc[b * TB + m * SUB:b * TB + (m + 1) * SUB, :] = dot_nn(
                    act[sub(m), LO], wown[:, :, :, HI].reshape(D, D))
            for c in range(NCH):
                a_store(ast.at[c], c, (z * 2 + b) * TB, c).start()
            events(IN_OWN[2 * b + 1])
            if b == 0:
                for c in range(NCH):
                    a_store(ast.at[c], c, z * NOWN, c).wait()

        def act_of(g):
            rows_of(4, css, crs.at[g]).wait_recv()
            gran = dz.at[5 + g // NCH, pl.ds(pl.multiple_of((g % NCH) * CH, CH), CH), :]
            w1_nat[...] = gran[:, LO].T
            w2_nat[...] = gran[:, HI]
            for m in range(8):
                u_own[m * SUB:(m + 1) * SUB, :] = gelu(dot_nn(xo_at(m)[...], w1_nat[...])).astype(BF)

        def granule(n, carry):
            act_of(jnp.where(n == FAR - 1, FAR, jnp.where(n == FAR, FAR - 1, n)))
            for m in range(8):
                rows = slice(m * SUB, (m + 1) * SUB)
                facc[rows, :] += dot_nn(u_own[rows, :], w2_nat[...])

            @pl.when(n == 0)
            def _():
                acc2[...] = jnp.zeros_like(acc2)

            events_at(n, IN_LOOP)

            return carry

        lax.fori_loop(0, NG - 1, granule, 0)
        act_of(NG - 1)
        for m in range(8):
            rows = slice(m * SUB, (m + 1) * SUB)
            out = facc[rows, :] + dot_nn(u_own[rows, :], w2_nat[...])
            xo_at(m)[...] = (xo_at(m)[...].astype(F32) + out).astype(BF)

    pl.run_scoped(forward, pltpu.VMEM((NOWN, D), F32), pltpu.VMEM((NOWN, CH), BF), pltpu.VMEM((D, CH), BF),
                  pltpu.VMEM((CH, D), BF))

    for c in range(NCH):
        a_store(ast.at[c], c, z * NOWN, c).wait()

    def e_half(k, b):
        return eall.at[k, :, pl.ds(pl.multiple_of(b * TB, TB), TB)]

    def e_pair(b):
        return remote(e_half(0, b), e_half(1, b), ess.at[0, b], ers.at[1, b], pos.pair, j)

    def e_mirror(b):
        return remote(e_half(0, b), e_half(2, b), ess.at[1, b], ers.at[2, b], pos.mirror, j)

    def e_forward(k, b):
        to = 3 if k == 1 else k
        return remote(e_half(k, b), e_half(to, b), efs.at[k, b], ers.at[to, b], pos.mirror if k == 1 else pos.pair, j)

    def e_wait(k, b):
        remote(e_half(k, b), e_half(k, b), efs.at[k, b], ers.at[k, b], pos.pair, j).wait_recv()

    def step_of(s):
        return s // 8, (s % 8) // 2, s % 2

    def a_load(s, slot):
        c, k, b = step_of(s)
        return pltpu.make_async_copy(a_hbm.at[c, pl.ds(share_row(k, b), TB)], ast.at[slot], as_sem.at[slot])

    everything = slice(None)
    up_sems, down_sems = (rss.at[0], rsr), (rss.at[1], rsr)

    def up(c, t):
        return Scatter(pos, acc1.at[c, t], r1a.at[c % 2, t], r2a.at[c % 2, t], r3a.at[c, t], everything, up_sems,
                       c * 4 + t, t == 0)

    def down(c, t, part=None):
        if part is None:
            lanes, idx, x_first = everything, c * 4 + 2 + t, t == 0
        else:
            lanes, idx, x_first = slice(part * (D // 2), (part + 1) * (D // 2)), c * 4 + 2 + t * 2 + part, part == 0
        return Scatter(pos, acc2.at[c, t], r1b.at[c % 2, t], r2b.at[c % 2, t], r3b.at[c, t], lanes, down_sems, idx, x_first)

    ups = [[up(c, t) for t in TWO] for c in range(NCH)]
    downs = [[down(c, t) for t in TWO] for c in range(LAST)]
    tails = [[down(LAST, t, part) for part in TWO] for t in TWO]

    def each(group, stage):
        for sc in group:
            getattr(sc, stage)()

    def fold(v):
        rows, cols = v.shape
        total = jnp.zeros((8, 128), F32)
        for q in range(cols // 128):
            total = total + jnp.sum(v[:, q * 128:(q + 1) * 128].reshape(rows // 8, 8, 128), axis=0)
        return total

    def shard(acc, c, t):
        return acc.at[c, t, pos.y, pos.x, pos.core]

    def out_copy(acc, out, c, sem, t):
        return pltpu.make_async_copy(shard(acc, c, t), out.at[c, t], sh_sem.at[sem])

    def finish(acc, out, c, sem):
        v0, v1 = shard(acc, c, 0)[...], shard(acc, c, 1)[...]
        gm[0] += fold(v0 * v0)
        gm[1] += fold(v0 * v1)
        gm[2] += fold(v1 * v1)
        for t in TWO:
            out_copy(acc, out, c, sem, t).start()

    def finish_chunk(c):
        each(ups[c] + downs[c], 'done')
        finish(acc1, sh1_hbm, c, 0)
        finish(acc2, sh2_hbm, c, 1)

    def backward(us_all, das, xbuf):
        def x_load(s, slot):
            _, k, b = step_of(s)
            return pltpu.make_async_copy(x_hbm.at[pl.ds(share_row(k, b), TB)], xbuf.at[slot], xs_sem.at[slot])

        def pair_slot(p):
            return 2 * ((p + 1) % 2)

        def load_pair(p, act):
            for b in TWO:
                getattr(a_load(p * 2 + b, pair_slot(p) + b), act)()
                getattr(x_load(p * 2 + b, pair_slot(p) + b), act)()

        a_load(0, 0).start()
        x_load(0, 0).start()

        ld_l.wait()
        r = lax.broadcasted_iota(jnp.int32, (ER, TB), 0)
        first = r % 2 == 0
        real = r < 2 * NC
        neg = jnp.float32(-jnp.inf)
        for b in TWO:
            cols = slice(b * TB, (b + 1) * TB)
            logit = jnp.where(real, dot_nt(hcat[...], own_x[:, SIDES[b]]), neg)
            m0 = jnp.max(jnp.where(first, logit, neg), axis=0, keepdims=True)
            m1 = jnp.max(jnp.where(first, neg, logit), axis=0, keepdims=True)
            ex = jnp.exp(logit - jnp.where(first, m0, m1))
            s0 = jnp.sum(jnp.where(first, ex, 0.0), axis=0, keepdims=True)
            s1 = jnp.sum(jnp.where(first, 0.0, ex), axis=0, keepdims=True)
            prob = ex / jnp.where(first, s0, s1)
            lab = jnp.where(first, lab_v[0:1, cols], lab_v[1:2, cols])
            hot = jnp.where(jnp.logical_and(r // 2 == lab, real), 1.0, 0.0)
            eall[0, :, cols] = (prob - hot) / (NTOK * 8.0)
            e_pair(b).start()

            @pl.when(inner)
            def _():
                e_mirror(b).start()

        rows_of(NG, xss, xrs.at[0]).wait_send()
        rows_of(FAR, yss, yrs.at[0]).wait_send()
        rows_of(NG, dss, drs.at[0]).wait_send()
        both = dz.at[pl.ds(5, 2), pl.ds(0, 2 * NG * GR), :]
        remote(both, both, css, crs.at[0], z, pos.jc).wait_send()
        rows_of(NCH, zss.at[0], zrs.at[0]).wait_send()

        @pl.when(inner)
        def _():
            for n, i in ((NCH, 1), (NG, 2), (FAR, 3)):
                rows_of(n, zss.at[i], zrs.at[0]).wait_send()

        def d_act(src, t, sl, c, us, rows):
            w2c = wown[c, :, :, HI].reshape(CH, D)
            u, slope = gelu_and_slope(src[...])
            us[rows, :] = u.astype(BF)
            for task in TWO:
                da = dot_nt(dz[t, sl, SIDES[task]], w2c)
                das[rows, task * CH:(task + 1) * CH] = (da * slope).astype(BF)

        def add_up(c, g):
            for task in TWO:
                acc1[c, task] += g[:, task * CH:(task + 1) * CH].reshape(acc1.shape[2:])

        def add_down(c, g):
            for task in TWO:
                acc2[c, task] += g[:, SIDES[task]].reshape(acc2.shape[2:])

        def e_parts(s):
            _, k, b = step_of(s)
            e = e_half(k, b)[...]
            e1 = e.astype(BF).astype(F32)
            rest = e - e1
            e2 = rest.astype(BF).astype(F32)
            e3 = rest - e2
            return jnp.concatenate([e1, e2, e3], axis=0).astype(BF)

        def first_step(s, carry):
            _, k, b = step_of(s)
            t = k * 2 + b
            a_load(s, s % 2).wait()
            x_load(s, s % 2).wait()

            @pl.when(s < 7)
            def _():
                a_load(s + 1, (s + 1) % 2).start()
                x_load(s + 1, (s + 1) % 2).start()

            @pl.when(s == 7)
            def _():
                load_pair(4, 'start')

            @pl.when(jnp.logical_and(outer, k > 0))
            def _():
                e_wait(k, b)

            es = e_parts(s)
            for m in BLOCKS:
                dz[t, sub(m), :] = dot_tn(es[:, sub(m)], hbd[...]).astype(BF)
            us = us_all.at[0]
            for m in BLOCKS:
                d_act(ast.at[s % 2, sub(m)], t, sub(m), 0, us, sub(m))
            add_up(0, dot_tn(xbuf[s % 2], das[:TB]))
            add_down(0, dot_tn(us[:TB], dz[t]))

            for when, codes in enumerate(E_ON):
                if codes:
                    @pl.when(jnp.logical_and(s == when, inner))
                    def _():
                        for k_f, b_f in zip(codes[::2], codes[1::2]):
                            e_forward_after_wait(int(k_f), int(b_f))

            return carry

        def pair_front(p, c):
            k = p % 4
            load_pair(p, 'wait')

            @pl.when(p < 11)
            def _():
                load_pair(p + 1, 'start')

            for b in TWO:
                for m in BLOCKS:
                    rows = slice(b * TB + m * SUB, b * TB + (m + 1) * SUB)
                    d_act(ast.at[pair_slot(p) + b, sub(m)], k * 2 + b, sub(m), c, us_all.at[k], rows)
            add_up(c, dot_tn(xbuf[pl.ds(pair_slot(p), 2)].reshape(NOWN, D), das[...]))

        def step(p, carry):
            k = p % 4
            pair_front(p, 1)
            add_down(1, dot_tn(us_all[k], dz[pl.ds(k * 2, 2)].reshape(NOWN, DD)))

            @pl.when(p == 4)
            def _():
                each(ups[0] + downs[0], 'side')

            @pl.when(p == 6)
            def _():
                each(ups[0] + downs[0], 'last')

            return carry

        def e_forward_after_wait(k, b):
            e_wait(k, b)
            e_forward(k, b).start()

        lax.fori_loop(0, 8, first_step, 0)
        each(ups[0] + downs[0], 'start')
        lax.fori_loop(4, 8, step, 0)
        each(ups[1] + downs[1], 'start')

        def last_step(p, carry):
            pair_front(p, LAST)

            @pl.when(p == 8)
            def _():
                finish_chunk(0)
                each(ups[1], 'side')

            @pl.when(p == 9)
            def _():
                each(downs[1], 'side')

            @pl.when(p == 10)
            def _():
                each(ups[1], 'last')

            return carry

        lax.fori_loop(8, 12, last_step, 0)
        each(ups[LAST], 'start')
        each(downs[1], 'last')

        def down_pass(task):
            def half(i, carry):
                u = us_all[pl.ds(i * 2, 2)].reshape(4 * TB, CH)
                d = dz[pl.ds(i * 4, 4), :, SIDES[task]].reshape(4 * TB, D)
                acc2[LAST, task] += dot_tn(u, d).reshape(acc2.shape[2:])

                @pl.when(i == 0)
                def _():
                    each(ups[LAST] if task == 0 else tails[0], 'side')

                return carry

            lax.fori_loop(0, 2, half, 0)
            each(tails[task], 'start')

        down_pass(0)
        finish_chunk(1)
        down_pass(1)

    pl.run_scoped(backward, pltpu.VMEM((4, NOWN, CH), BF), pltpu.VMEM((NOWN, 2 * CH), BF),
                  pltpu.VMEM((4, TB, D), BF))

    each(ups[LAST], 'last')
    each(tails[1], 'side')
    each(tails[0], 'last')
    each(ups[LAST], 'done')
    finish(acc1, sh1_hbm, LAST, 0)
    each(tails[1], 'last')
    each(tails[0], 'done')
    each(tails[1], 'done')
    finish(acc2, sh2_hbm, LAST, 1)

    def full(v):
        return jnp.sum(jnp.sum(v, axis=0, keepdims=True), axis=1, keepdims=True)

    lane = lax.broadcasted_iota(jnp.int32, (1, 128), 1)
    mbuf[pl.ds(me, 1), :] = jnp.where(lane == 0, full(gm[0]), jnp.where(lane == 1, full(gm[1]), full(gm[2])))

    def row_of(ref):
        return ref.at[pl.ds(me, 1), :]

    keep = pltpu.make_async_copy(row_of(mbuf), row_of(rows_hbm), ld_sem.at[0])
    keep.start()

    def m_send(to_z, to_j):
        remote(row_of(mbuf), row_of(rows_hbm), mss, mrs, to_z, to_j).start()

    mates = [(j + i) % 8 for i in MATES]
    for to_z in reversed(pos.shares[1:]):
        for to_j in [j] + mates:
            m_send(to_z, to_j)
    for to_j in mates:
        m_send(z, to_j)

    for b in TWO:
        e_pair(b).wait_send()

        @pl.when(inner)
        def _():
            e_mirror(b).wait_send()
            for k in LINE:
                e_forward(k, b).wait_send()

    for kind, acc in enumerate((acc1, acc2)):
        for stage, part in enumerate((acc.at[:, :, :, :, 0], acc.at[:, :, :, 0, 0], acc.at[:, :, 0, 0, 0])):
            remote(part, part, rss.at[kind, stage], rsr.at[0, stage], z, pos.jc).wait_send()
    pltpu.make_async_copy(r3a, sh1_hbm, sh_sem.at[0]).wait()
    pltpu.make_async_copy(r3b, sh2_hbm, sh_sem.at[1]).wait()

    keep.wait()
    lines = pl.ds(0, NDEV - 1)
    remote(mbuf.at[lines, :], rows_hbm.at[lines, :], mss, mrs, z, pos.jc).wait()


def main_call(x, w1, w2r, heads, labels):
    dma = pltpu.SemaphoreType.DMA
    anyspec = pl.BlockSpec(memory_space=pl.ANY)
    up, down = (OWN, CH), (GR, D)
    pair, quad, octet = (2,), (2, 2), (2, 2, 2)
    per_chunk = (NCH, 2)
    vmem = pltpu.VMEM
    return pl.pallas_call(
        main_kernel,
        out_shape=(jax.ShapeDtypeStruct((NCH, NTOK, CH), F32),
                   jax.ShapeDtypeStruct(per_chunk + up, F32),
                   jax.ShapeDtypeStruct(per_chunk + down, F32),
                   jax.ShapeDtypeStruct((NDEV, 128), F32)),
        in_specs=[anyspec] * 5,
        out_specs=(anyspec, anyspec, anyspec, anyspec),
        scratch_shapes=[
            vmem((8, TB, DD), BF),
            vmem((NCH, 8, GR, DD), BF),
            vmem(per_chunk + octet + up, F32), vmem(per_chunk + octet + down, F32),
            vmem((2, 2) + quad + up, F32), vmem((2, 2) + quad + down, F32),
            vmem((2, 2) + pair + up, F32), vmem((2, 2) + pair + down, F32),
            vmem(per_chunk + up, F32), vmem(per_chunk + down, F32),
            vmem((4, ER, NOWN), F32),
            vmem((4, TB, CH), F32),
            vmem((3 * ER, DD), BF),
            vmem((ER, D), BF),
            vmem((NC, 2, D), BF),
            vmem((2, NOWN), jnp.int32),
            vmem((3, 8, 128), F32), vmem((NDEV, 128), F32),
            dma((4,)), dma((NG,)), dma((NCH,)), dma(()), dma((NG,)), dma(()), dma((FAR,)), dma(()), dma((NG,)), dma(()), dma((NG,)),
            dma((5,)), dma((NCH,)), dma((4,)), dma((6,)), dma(quad), dma((4, 2)), dma((4, 2)),
            dma((2, NCH)), dma((14, NCH)), dma(()), dma(()), dma(pair),
        ],
        compiler_params=pltpu.CompilerParams(
            collective_id=0, has_side_effects=True, vmem_limit_bytes=VMEM_BYTES),
        name='main',
    )(x, w1, w2r, heads, labels)


def result_kernel(rows_hbm, sh1_hbm, sh2_hbm, a_ref, g1_hbm, g2_hbm, rows, sh1, sh2, g1_ref, g2_ref, sem):
    ld_rows = pltpu.make_async_copy(rows_hbm, rows, sem.at[0])
    loads = [pltpu.make_async_copy(sh1_hbm, sh1, sem.at[1]), pltpu.make_async_copy(sh2_hbm, sh2, sem.at[2])]
    ld_rows.start()
    for cp in loads:
        cp.start()
    ld_rows.wait()

    gram = jnp.sum(rows[...], axis=0, keepdims=True)
    lane = lax.broadcasted_iota(jnp.int32, gram.shape, 1)

    def entry(i):
        return jnp.sum(jnp.where(lane == i, gram, 0.0), axis=1, keepdims=True)

    g00, g01, g11 = entry(0), entry(1), entry(2)
    scale = (g00 + g11) * -0.5
    g00, g01, g11 = g00 / scale, g01 / scale, g11 / scale
    a0 = a1 = jnp.full((1, 1), 0.5, F32)
    for _ in range(STEPS):
        v0 = a0 * jnp.exp(g00 * a0 + g01 * a1)
        v1 = a1 * jnp.exp(g01 * a0 + g11 * a1)
        tot = v0 + v1
        a0, a1 = v0 / tot, v1 / tot
    a_ref[0] = a0[0, 0]
    a_ref[1] = a1[0, 0]
    for cp in loads:
        cp.wait()
    out1 = pltpu.make_async_copy(g1_ref, g1_hbm, sem.at[3])
    out2 = pltpu.make_async_copy(g2_ref, g2_hbm, sem.at[4])
    for c in range(NCH):
        g2_ref[c * GR:(c + 1) * GR, :] = a0 * sh2[c, 0] + a1 * sh2[c, 1]
    out2.start()
    for c in range(NCH):
        comb = a0 * sh1[c, 0] + a1 * sh1[c, 1]
        for g in range(8):
            col = g * NCH * GR + c * GR
            g1_ref[:, col:col + GR] = comb[:, g * GR:(g + 1) * GR]
    out1.start()
    out2.wait()
    out1.wait()


def result_call(rows, sh1, sh2):
    anyspec = pl.BlockSpec(memory_space=pl.ANY)
    return pl.pallas_call(
        result_kernel,
        out_shape=(jax.ShapeDtypeStruct((2,), F32), jax.ShapeDtypeStruct((OWN, D), F32),
                   jax.ShapeDtypeStruct((OWN, D), F32)),
        in_specs=[anyspec] * NCH,
        out_specs=(pl.BlockSpec(memory_space=pltpu.SMEM), anyspec, anyspec),
        scratch_shapes=[pltpu.VMEM(v.shape, F32) for v in (rows, sh1, sh2)] + [pltpu.VMEM((OWN, D), F32)] * 2 + [
            pltpu.SemaphoreType.DMA((5,))],
        name='result',
    )(rows, sh1, sh2)


def solution(mesh):
    def local_step(tokens, w_up, w_down, task_heads, labels):
        w2r = w_down.reshape(8, NCH, GR, D)
        heads = jnp.transpose(task_heads, (2, 0, 1))
        _, sh1, sh2, rows = main_call(tokens, w_up, w2r, heads, labels)
        return result_call(rows, sh1, sh2)

    return jax.shard_map(
        local_step, mesh=mesh,
        in_specs=(P('data', None), P(None, 'model'), P('model', None), P(None, None, None), P(None, 'data')),
        out_specs=(P(None), P('data', 'model'), P(('model', 'data'), None)),
        check_vma=False)
```

```python
import jax
import jax.numpy as jnp
from jax import lax
from jax.experimental import pallas as pl
from jax.experimental.pallas import tpu as pltpu
from jax.sharding import PartitionSpec as P

STEPS = 20
BF = jnp.bfloat16
F32 = jnp.float32
MESH = pl.DeviceIdType.MESH
VMEM_BYTES = 67043328

D = 768
DD = D + D
NTOK = 8192
NOWN = 2048
TB = 1024
SUB = 256
NC = 19
ER = 40
CH = 256
NCH = 3
LAST = NCH - 1
NG = NCH * NCH
FAR = NG - NCH
GR = 32
OWN = CH // GR * 12
LO = slice(D)
HI = slice(D, DD)
SIDES = (LO, HI)
TWO = range(2)
MATES = range(1, 8)
LINE = range(1, 4)
BLOCKS = range(TB // SUB)
NDEV = 32

E_ON = ('', '1020', '1121', '30', '31')
IN_OTHER = ('', 't0o0', 't1o1i3', 't2o2i4', 's0i5', 's1T3o3')
IN_OWN = ('i6', 's2d0T4o4i7', 'd1i8', 's3T5o5g6')
IN_LOOP = ('d2g7s4', 'd3g8', 's5B6x6d4', 'B7x7', 'B8x8p6d5', 'p7', 'p8', '', '')

G0 = 0.7978845608028654
G1C = 0.044715 * G0


def dot_nn(a, b):
    return lax.dot_general(a, b, (((1,), (0,)), ((), ())), preferred_element_type=F32)


def dot_nt(a, b):
    return lax.dot_general(a, b, (((1,), (1,)), ((), ())), preferred_element_type=F32)


def dot_tn(a, b):
    return lax.dot_general(a, b, (((0,), (0,)), ((), ())), preferred_element_type=F32)


def gelu(x):
    t = jnp.tanh(x * (G0 + G1C * (x * x)))
    h = 0.5 * x
    return h + h * t


def gelu_and_slope(x):
    x2 = x * x
    t = jnp.tanh(x * (G0 + G1C * x2))
    h = 0.5 * x
    u = h + h * t
    s = 0.5 + 0.5 * t + h * (1.0 - t * t) * (G0 + (3.0 * G1C) * x2)
    return u, s


class Place:
    def __init__(self):
        self.z = lax.axis_index('model')
        self.j = lax.axis_index('data')
        self.core = self.j % 2
        self.x = (self.j // 2) % 2
        self.y = self.j // 4
        self.jc = self.j + 1 - 2 * self.core
        self.jx = self.j + 2 - 4 * self.x
        self.jy = self.j + 4 - 8 * self.y
        self.jd = self.jx + 4 - 8 * self.y
        self.js = self.jx + self.core * (self.jy - self.jx)
        self.j2 = self.jx + self.jy - self.js

        self.inner = self.z % 3 > 0
        self.pair = self.z + 1 - 2 * (self.z % 2)
        self.mirror = 3 - self.z
        half = self.z // 2
        self.shares = (self.z, self.pair, 2 - half, 3 - 3 * half)

    def share(self, k):
        own, near, far, end = self.shares
        return jnp.where(k == 0, own, jnp.where(k == 1, near, jnp.where(k == 2, far, end)))


def remote(src, dst, ssem, rsem, z, j):
    return pltpu.make_async_remote_copy(
        src_ref=src, dst_ref=dst, send_sem=ssem, recv_sem=rsem, device_id=(z, j), device_id_type=MESH)


class Scatter:
    def __init__(self, pos, acc, r1, r2, r3, lanes, sems, idx, x_first):
        self.pos, self.acc, self.r1, self.r2, self.r3 = pos, acc, r1, r2, r3
        self.lanes, self.sems, self.idx, self.x_first = lanes, sems, idx, x_first

    def copy(self, stage):
        p, ln = self.pos, self.lanes
        ssem, rsem = self.sems[0].at[stage], self.sems[1].at[self.idx, stage]
        if stage == 0:
            return remote(self.acc.at[:, :, 1 - p.core, :, ln], self.r1.at[:, :, :, ln], ssem, rsem, p.z, p.jc)
        if stage == 1:
            if self.x_first:
                return remote(self.acc.at[:, 1 - p.x, p.core, :, ln], self.r2.at[:, :, ln], ssem, rsem, p.z, p.jx)
            return remote(self.acc.at[1 - p.y, :, p.core, :, ln], self.r2.at[:, :, ln], ssem, rsem, p.z, p.jy)
        if self.x_first:
            return remote(self.acc.at[1 - p.y, p.x, p.core, :, ln], self.r3.at[:, ln], ssem, rsem, p.z, p.jy)
        return remote(self.acc.at[p.y, 1 - p.x, p.core, :, ln], self.r3.at[:, ln], ssem, rsem, p.z, p.jx)

    def start(self):
        self.copy(0).start()

    def side(self):
        p, ln = self.pos, self.lanes
        self.copy(0).wait_recv()
        for yy in TWO:
            for xx in TWO:
                self.acc[yy, xx, p.core, :, ln] += self.r1[yy, xx, :, ln]
        self.copy(1).start()

    def last(self):
        p, ln = self.pos, self.lanes
        self.copy(1).wait_recv()
        for i in TWO:
            if self.x_first:
                self.acc[i, p.x, p.core, :, ln] += self.r2[i, :, ln]
            else:
                self.acc[p.y, i, p.core, :, ln] += self.r2[i, :, ln]
        self.copy(2).start()

    def done(self):
        p, ln = self.pos, self.lanes
        self.copy(2).wait_recv()
        self.acc[p.y, p.x, p.core, :, ln] += self.r3[:, ln]


def main_kernel(x_hbm, w1_hbm, w2_hbm, heads_hbm, lab_hbm,
                a_hbm, sh1_hbm, sh2_hbm, rows_hbm,
                dz, wown, acc1, acc2, r1a, r1b, r2a, r2b, r3a, r3b, eall, ast, hbd, hcat, heads, lab_v,
                gm, mbuf,
                zss, zrs, zqs, xss, xrs, yss, yrs, dss, drs, css, crs,
                ld_sem, w2_sem, xs_sem, as_sem, ess, efs, ers,
                rss, rsr, mss, mrs, sh_sem):
    pos = Place()
    z, j, inner = pos.z, pos.j, pos.inner
    outer = jnp.logical_not(inner)

    barrier = pltpu.get_barrier_semaphore()
    me = z * 8 + j
    pl.semaphore_signal(barrier, device_id=(pos.pair, j), device_id_type=MESH)

    @pl.when(inner)
    def _():
        pl.semaphore_signal(barrier, device_id=(pos.mirror, j), device_id_type=MESH)

    for jj in (pos.jx, pos.jy, pos.jc):
        pl.semaphore_signal(barrier, device_id=(z, jj), device_id_type=MESH)

    own_x, act, room = dz.at[0], dz.at[2], dz.at[3]
    w1_raw = room.at[LO, LO]
    w1_own = dz.at[4, LO, HI]

    def sub(m):
        return slice((m % 4) * SUB, (m % 4 + 1) * SUB)

    def xo_at(m):
        return own_x.at[sub(m), HI if m >= 4 else LO]

    def share_row(k, b):
        return pl.multiple_of((pos.share(k) * 2 + b) * TB, TB)

    own_row = pl.multiple_of(z * NOWN, NOWN)
    ld_w1 = pltpu.make_async_copy(w1_hbm, w1_raw, ld_sem.at[0])
    ld_x = [pltpu.make_async_copy(x_hbm.at[pl.ds(own_row + b * TB, TB)], own_x.at[:, SIDES[b]], ld_sem.at[1 + b])
            for b in TWO]
    ld_l = pltpu.make_async_copy(lab_hbm.at[:, pl.ds(own_row, NOWN)], lab_v, ld_sem.at[3])
    ld_h = pltpu.make_async_copy(heads_hbm, heads, ld_sem.at[4])
    ld_w2 = [pltpu.make_async_copy(w2_hbm.at[:, c], wown.at[c, :, :, HI], w2_sem.at[c]) for c in range(NCH)]

    def stream_half(i):
        return dz.at[1 + 3 * (i % 2), :, LO]

    def xs_load(i):
        return pltpu.make_async_copy(
            x_hbm.at[pl.ds(share_row(1 + i // 2, i % 2), TB)], stream_half(i), xs_sem.at[i % 2])

    ld_h.start()
    ld_w1.start()
    for cp in ld_w2:
        cp.start()
    xs_load(0).start()
    for cp in ld_x:
        cp.start()
    ld_l.start()

    ld_h.wait()
    hf = jnp.concatenate([heads[i].astype(F32) for i in range(NC)] + [jnp.zeros((2, D), F32)], axis=0)
    hcat[...] = hf.astype(BF)
    r = lax.broadcasted_iota(jnp.int32, (ER, D), 0)
    hb = jnp.concatenate([jnp.where(r % 2 == 0, hf, 0.0), jnp.where(r % 2 == 1, hf, 0.0)], axis=1)
    hbd[...] = jnp.concatenate([hb, hb, hb], axis=0).astype(BF)
    gm[...] = jnp.zeros_like(gm)
    acc1[...] = jnp.zeros_like(acc1)

    ld_w1.wait()
    w1t = w1_raw[...].T
    for c in range(NCH):
        for g in range(8):
            row = g * NCH * GR + c * GR
            wown[c, g, :, LO] = w1t[row:row + GR, :]
    for cp in ld_w2:
        cp.wait()
    pl.semaphore_wait(barrier, 4 + z * pos.mirror // 2)

    def piece(i, jj):
        row = pl.multiple_of((i % NCH) * CH + jj * GR, GR)
        return dz.at[5 + i // NCH, pl.ds(row, GR), :]

    def rows_of(n, ssem, rsem):
        part = dz.at[5, pl.ds(0, n * GR), :]
        return remote(part, part, ssem, rsem, z, pos.jc)

    def z_pair(c):
        return remote(wown.at[c, j], piece(c, j), zss.at[0], zrs.at[c], pos.pair, j)

    def z_mirror(c):
        return remote(wown.at[c, j], piece(NCH + c, j), zss.at[1], zrs.at[NCH + c], pos.mirror, j)

    def z_forward(i):
        first = i < NCH
        to = jnp.where(first, i + 2 * NCH, i)
        return remote(piece(i, j), piece(to, j), zss.at[2], zrs.at[to], jnp.where(first, pos.mirror, pos.pair), j)

    def more_forward(i):
        first = i < NCH
        to = jnp.where(first, i + 2 * NCH, i)
        return remote(piece(i, pos.j2), piece(to, pos.j2), zss.at[3], zqs.at[to - FAR], jnp.where(first, pos.mirror, pos.pair), j)

    def side_copy(i):
        return remote(piece(i, j), piece(i, j), xss, xrs.at[i], z, pos.js)

    def more_copy(i):
        return remote(piece(i, pos.j2), piece(i, pos.j2), dss, drs.at[i], z, pos.js)

    def x_copy(i):
        return remote(piece(i, j), piece(i, j), xss, xrs.at[i], z, pos.jx)

    def y_copy(i):
        return remote(piece(i, j), piece(i, j), yss, yrs.at[i], z, pos.jy)

    def diag_copy_y(i):
        return remote(piece(i, pos.jx), piece(i, pos.jx), dss, drs.at[i], z, pos.jy)

    def diag_copy_x(i):
        return remote(piece(i, pos.jy), piece(i, pos.jy), dss, drs.at[i], z, pos.jx)

    def core_copy(i, q):
        jj = (j, pos.jx, pos.jy, pos.jd)[q]
        return remote(piece(i, jj), piece(i, jj), css, crs.at[i], z, pos.jc)

    def core_side(i, q):
        jj = (j, pos.js, pos.j2, pos.jd)[q]
        return remote(piece(i, jj), piece(i, jj), css, crs.at[i], z, pos.jc)

    def take(i):
        remote(piece(i, j), piece(i, j), zss.at[2], zrs.at[i], pos.pair, j).wait_recv()

        @pl.when(inner)
        def _():
            z_forward(i).start()

    def take_more(i):
        remote(piece(i, j), piece(i, j), zss.at[3], zqs.at[i - FAR], pos.pair, j).wait_recv()

        @pl.when(inner)
        def _():
            more_forward(i).start()

    def take_both(i):
        take(i)
        take_more(i)

    def send_both(i):
        side_copy(i).start()
        more_copy(i).start()
        core_side(i, 0).start()
        core_side(i, 2).start()

    def pass_both(i):
        side_copy(i).wait_recv()
        core_side(i, 1).start()
        more_copy(i).wait_recv()
        core_side(i, 3).start()

    def send_own(i):
        x_copy(i).start()
        y_copy(i).start()
        core_copy(i, 0).start()

    def send_side(i):
        x_copy(i).wait_recv()

        @pl.when(pos.core == 0)
        def _():
            diag_copy_y(i).start()

        core_copy(i, 1).start()
        y_copy(i).wait_recv()

        @pl.when(pos.core == 1)
        def _():
            diag_copy_x(i).start()

        core_copy(i, 2).start()

    def send_diag(i):
        diag_copy_y(i).wait_recv()
        core_copy(i, 3).start()

    def side_and_on(i):
        send_side(i)
        if i < NCH:
            @pl.when(inner)
            def _():
                more_forward(i).start()

    def when_inner(f):
        return lambda i: pl.when(inner)(lambda: f(i))

    def when_outer(f):
        return lambda i: pl.when(outer)(lambda: f(i))

    kinds = {'t': take, 'T': when_outer(take), 'i': when_inner(take), 'o': send_own, 's': side_and_on, 'd': send_diag,
             'g': when_inner(take_more), 'B': when_outer(take_both), 'x': send_both, 'p': pass_both}

    def events(codes):
        for kind, i in zip(codes[::2], codes[1::2]):
            kinds[kind](int(i))

    def events_at(i, table):
        for n, codes in enumerate(table):
            if codes:
                pl.when(i == n)(lambda codes=codes: events(codes))

    for c in range(NCH):
        z_pair(c).start()

    @pl.when(inner)
    def _():
        for c in range(NCH):
            z_mirror(c).start()

    def a_store(src, c, row, sem):
        return pltpu.make_async_copy(src, a_hbm.at[c, pl.ds(pl.multiple_of(row, TB), TB)], as_sem.at[sem])

    def forward(facc, u_own, w1_nat, w2_nat):
        for c in range(NCH):
            w1_own[:, c * CH:(c + 1) * CH] = wown[c, :, :, LO].reshape(CH, D).T

        def staged(i, c):
            rows = pl.ds(pl.multiple_of((i % 2) * TB, TB), TB)
            return a_store(facc.at[rows, c * CH:(c + 1) * CH], c, share_row(1 + i // 2, i % 2), (i % 2) * NCH + c)

        def other_tokens(i, carry):
            xs_load(i).wait()

            @pl.when(i < 5)
            def _():
                xs_load(i + 1).start()

            @pl.when(i >= 2)
            def _():
                for c in range(NCH):
                    staged(i, c).wait()

            base = (i % 2) * TB
            for m in BLOCKS:
                rows = pl.ds(pl.multiple_of(base + m * SUB, SUB), SUB)
                facc[rows, :] = dot_nn(stream_half(i)[sub(m), :], w1_own[...])
            for c in range(NCH):
                staged(i, c).start()

            events_at(i, IN_OTHER)
            return carry

        lax.fori_loop(0, 6, other_tokens, 0)
        for cp in ld_x:
            cp.wait()

        for b in TWO:
            for c in range(NCH):
                staged(b, c).wait()
            for m in BLOCKS:
                a = dot_nn(xo_at(b * 4 + m)[...], w1_own[...])
                for c in range(NCH):
                    ast[c, sub(m), :] = a[:, c * CH:(c + 1) * CH]
                act[sub(m), LO] = gelu(a).astype(BF)
            events(IN_OWN[2 * b])
            for m in BLOCKS:
                facc[b * TB + m * SUB:b * TB + (m + 1) * SUB, :] = dot_nn(
                    act[sub(m), LO], wown[:, :, :, HI].reshape(D, D))
            for c in range(NCH):
                a_store(ast.at[c], c, (z * 2 + b) * TB, c).start()
            events(IN_OWN[2 * b + 1])
            if b == 0:
                for c in range(NCH):
                    a_store(ast.at[c], c, z * NOWN, c).wait()

        def act_of(g):
            rows_of(4, css, crs.at[g]).wait_recv()
            gran = dz.at[5 + g // NCH, pl.ds(pl.multiple_of((g % NCH) * CH, CH), CH), :]
            w1_nat[...] = gran[:, LO].T
            w2_nat[...] = gran[:, HI]
            for m in range(8):
                u_own[m * SUB:(m + 1) * SUB, :] = gelu(dot_nn(xo_at(m)[...], w1_nat[...])).astype(BF)

        def granule(n, carry):
            act_of(jnp.where(n == FAR - 1, FAR, jnp.where(n == FAR, FAR - 1, n)))
            for m in range(8):
                rows = slice(m * SUB, (m + 1) * SUB)
                facc[rows, :] += dot_nn(u_own[rows, :], w2_nat[...])

            @pl.when(n == 0)
            def _():
                acc2[...] = jnp.zeros_like(acc2)

            events_at(n, IN_LOOP)

            return carry

        lax.fori_loop(0, NG - 1, granule, 0)
        act_of(NG - 1)
        for m in range(8):
            rows = slice(m * SUB, (m + 1) * SUB)
            out = facc[rows, :] + dot_nn(u_own[rows, :], w2_nat[...])
            xo_at(m)[...] = (xo_at(m)[...].astype(F32) + out).astype(BF)

    pl.run_scoped(forward, pltpu.VMEM((NOWN, D), F32), pltpu.VMEM((NOWN, CH), BF), pltpu.VMEM((D, CH), BF),
                  pltpu.VMEM((CH, D), BF))

    for c in range(NCH):
        a_store(ast.at[c], c, z * NOWN, c).wait()

    def e_half(k, b):
        return eall.at[k, :, pl.ds(pl.multiple_of(b * TB, TB), TB)]

    def e_pair(b):
        return remote(e_half(0, b), e_half(1, b), ess.at[0, b], ers.at[1, b], pos.pair, j)

    def e_mirror(b):
        return remote(e_half(0, b), e_half(2, b), ess.at[1, b], ers.at[2, b], pos.mirror, j)

    def e_forward(k, b):
        to = 3 if k == 1 else k
        return remote(e_half(k, b), e_half(to, b), efs.at[k, b], ers.at[to, b], pos.mirror if k == 1 else pos.pair, j)

    def e_wait(k, b):
        remote(e_half(k, b), e_half(k, b), efs.at[k, b], ers.at[k, b], pos.pair, j).wait_recv()

    def step_of(s):
        return s // 8, (s % 8) // 2, s % 2

    def a_load(s, slot):
        c, k, b = step_of(s)
        return pltpu.make_async_copy(a_hbm.at[c, pl.ds(share_row(k, b), TB)], ast.at[slot], as_sem.at[slot])

    everything = slice(None)
    up_sems, down_sems = (rss.at[0], rsr), (rss.at[1], rsr)

    def up(c, t):
        return Scatter(pos, acc1.at[c, t], r1a.at[c % 2, t], r2a.at[c % 2, t], r3a.at[c, t], everything, up_sems,
                       c * 4 + t, t == 0)

    def down(c, t, part=None):
        if part is None:
            lanes, idx, x_first = everything, c * 4 + 2 + t, t == 0
        else:
            lanes, idx, x_first = slice(part * (D // 2), (part + 1) * (D // 2)), c * 4 + 2 + t * 2 + part, part == 0
        return Scatter(pos, acc2.at[c, t], r1b.at[c % 2, t], r2b.at[c % 2, t], r3b.at[c, t], lanes, down_sems, idx, x_first)

    ups = [[up(c, t) for t in TWO] for c in range(NCH)]
    downs = [[down(c, t) for t in TWO] for c in range(LAST)]
    tails = [[down(LAST, t, part) for part in TWO] for t in TWO]

    def each(group, stage):
        for sc in group:
            getattr(sc, stage)()

    def fold(v):
        rows, cols = v.shape
        total = jnp.zeros((8, 128), F32)
        for q in range(cols // 128):
            total = total + jnp.sum(v[:, q * 128:(q + 1) * 128].reshape(rows // 8, 8, 128), axis=0)
        return total

    def shard(acc, c, t):
        return acc.at[c, t, pos.y, pos.x, pos.core]

    def out_copy(acc, out, c, sem, t):
        return pltpu.make_async_copy(shard(acc, c, t), out.at[c, t], sh_sem.at[sem])

    def finish(acc, out, c, sem):
        v0, v1 = shard(acc, c, 0)[...], shard(acc, c, 1)[...]
        gm[0] += fold(v0 * v0)
        gm[1] += fold(v0 * v1)
        gm[2] += fold(v1 * v1)
        for t in TWO:
            out_copy(acc, out, c, sem, t).start()

    def finish_chunk(c):
        each(ups[c] + downs[c], 'done')
        finish(acc1, sh1_hbm, c, 0)
        finish(acc2, sh2_hbm, c, 1)

    def backward(us_all, das, xbuf):
        def x_load(s, slot):
            _, k, b = step_of(s)
            return pltpu.make_async_copy(x_hbm.at[pl.ds(share_row(k, b), TB)], xbuf.at[slot], xs_sem.at[slot])

        def pair_slot(p):
            return 2 * ((p + 1) % 2)

        def load_pair(p, act):
            for b in TWO:
                getattr(a_load(p * 2 + b, pair_slot(p) + b), act)()
                getattr(x_load(p * 2 + b, pair_slot(p) + b), act)()

        a_load(0, 0).start()
        x_load(0, 0).start()

        ld_l.wait()
        r = lax.broadcasted_iota(jnp.int32, (ER, TB), 0)
        first = r % 2 == 0
        real = r < 2 * NC
        neg = jnp.float32(-jnp.inf)
        for b in TWO:
            cols = slice(b * TB, (b + 1) * TB)
            logit = jnp.where(real, dot_nt(hcat[...], own_x[:, SIDES[b]]), neg)
            m0 = jnp.max(jnp.where(first, logit, neg), axis=0, keepdims=True)
            m1 = jnp.max(jnp.where(first, neg, logit), axis=0, keepdims=True)
            ex = jnp.exp(logit - jnp.where(first, m0, m1))
            s0 = jnp.sum(jnp.where(first, ex, 0.0), axis=0, keepdims=True)
            s1 = jnp.sum(jnp.where(first, 0.0, ex), axis=0, keepdims=True)
            prob = ex / jnp.where(first, s0, s1)
            lab = jnp.where(first, lab_v[0:1, cols], lab_v[1:2, cols])
            hot = jnp.where(jnp.logical_and(r // 2 == lab, real), 1.0, 0.0)
            eall[0, :, cols] = (prob - hot) / (NTOK * 8.0)
            e_pair(b).start()

            @pl.when(inner)
            def _():
                e_mirror(b).start()

        rows_of(NG, xss, xrs.at[0]).wait_send()
        rows_of(FAR, yss, yrs.at[0]).wait_send()
        rows_of(NG, dss, drs.at[0]).wait_send()
        both = dz.at[pl.ds(5, 2), pl.ds(0, 2 * NG * GR), :]
        remote(both, both, css, crs.at[0], z, pos.jc).wait_send()
        rows_of(NCH, zss.at[0], zrs.at[0]).wait_send()

        @pl.when(inner)
        def _():
            for n, i in ((NCH, 1), (NG, 2), (FAR, 3)):
                rows_of(n, zss.at[i], zrs.at[0]).wait_send()

        def d_act(src, t, sl, c, us, rows):
            w2c = wown[c, :, :, HI].reshape(CH, D)
            u, slope = gelu_and_slope(src[...])
            us[rows, :] = u.astype(BF)
            for task in TWO:
                da = dot_nt(dz[t, sl, SIDES[task]], w2c)
                das[rows, task * CH:(task + 1) * CH] = (da * slope).astype(BF)

        def add_up(c, g):
            for task in TWO:
                acc1[c, task] += g[:, task * CH:(task + 1) * CH].reshape(acc1.shape[2:])

        def add_down(c, g):
            for task in TWO:
                acc2[c, task] += g[:, SIDES[task]].reshape(acc2.shape[2:])

        def e_parts(s):
            _, k, b = step_of(s)
            e = e_half(k, b)[...]
            e1 = e.astype(BF).astype(F32)
            rest = e - e1
            e2 = rest.astype(BF).astype(F32)
            e3 = rest - e2
            return jnp.concatenate([e1, e2, e3], axis=0).astype(BF)

        def first_step(s, carry):
            _, k, b = step_of(s)
            t = k * 2 + b
            a_load(s, s % 2).wait()
            x_load(s, s % 2).wait()

            @pl.when(s < 7)
            def _():
                a_load(s + 1, (s + 1) % 2).start()
                x_load(s + 1, (s + 1) % 2).start()

            @pl.when(s == 7)
            def _():
                load_pair(4, 'start')

            @pl.when(jnp.logical_and(outer, k > 0))
            def _():
                e_wait(k, b)

            es = e_parts(s)
            for m in BLOCKS:
                dz[t, sub(m), :] = dot_tn(es[:, sub(m)], hbd[...]).astype(BF)
            us = us_all.at[0]
            for m in BLOCKS:
                d_act(ast.at[s % 2, sub(m)], t, sub(m), 0, us, sub(m))
            add_up(0, dot_tn(xbuf[s % 2], das[:TB]))
            add_down(0, dot_tn(us[:TB], dz[t]))

            for when, codes in enumerate(E_ON):
                if codes:
                    @pl.when(jnp.logical_and(s == when, inner))
                    def _():
                        for k_f, b_f in zip(codes[::2], codes[1::2]):
                            e_forward_after_wait(int(k_f), int(b_f))

            return carry

        def pair_front(p, c):
            k = p % 4
            load_pair(p, 'wait')

            @pl.when(p < 11)
            def _():
                load_pair(p + 1, 'start')

            for b in TWO:
                for m in BLOCKS:
                    rows = slice(b * TB + m * SUB, b * TB + (m + 1) * SUB)
                    d_act(ast.at[pair_slot(p) + b, sub(m)], k * 2 + b, sub(m), c, us_all.at[k], rows)
            add_up(c, dot_tn(xbuf[pl.ds(pair_slot(p), 2)].reshape(NOWN, D), das[...]))

        def step(p, carry):
            k = p % 4
            pair_front(p, 1)
            add_down(1, dot_tn(us_all[k], dz[pl.ds(k * 2, 2)].reshape(NOWN, DD)))

            @pl.when(p == 4)
            def _():
                each(ups[0] + downs[0], 'side')

            @pl.when(p == 6)
            def _():
                each(ups[0] + downs[0], 'last')

            return carry

        def e_forward_after_wait(k, b):
            e_wait(k, b)
            e_forward(k, b).start()

        lax.fori_loop(0, 8, first_step, 0)
        each(ups[0] + downs[0], 'start')
        lax.fori_loop(4, 8, step, 0)
        each(ups[1] + downs[1], 'start')

        def last_step(p, carry):
            pair_front(p, LAST)

            @pl.when(p == 8)
            def _():
                finish_chunk(0)
                each(ups[1], 'side')

            @pl.when(p == 9)
            def _():
                each(downs[1], 'side')

            @pl.when(p == 10)
            def _():
                each(ups[1], 'last')

            return carry

        lax.fori_loop(8, 12, last_step, 0)
        each(ups[LAST], 'start')
        each(downs[1], 'last')

        def down_pass(task):
            def half(i, carry):
                u = us_all[pl.ds(i * 2, 2)].reshape(4 * TB, CH)
                d = dz[pl.ds(i * 4, 4), :, SIDES[task]].reshape(4 * TB, D)
                acc2[LAST, task] += dot_tn(u, d).reshape(acc2.shape[2:])

                @pl.when(i == 0)
                def _():
                    each(ups[LAST] if task == 0 else tails[0], 'side')

                return carry

            lax.fori_loop(0, 2, half, 0)
            each(tails[task], 'start')

        down_pass(0)
        finish_chunk(1)
        down_pass(1)

    pl.run_scoped(backward, pltpu.VMEM((4, NOWN, CH), BF), pltpu.VMEM((NOWN, 2 * CH), BF),
                  pltpu.VMEM((4, TB, D), BF))

    each(ups[LAST], 'last')
    each(tails[1], 'side')
    each(tails[0], 'last')
    each(ups[LAST], 'done')
    finish(acc1, sh1_hbm, LAST, 0)
    each(tails[1], 'last')
    each(tails[0], 'done')
    each(tails[1], 'done')
    finish(acc2, sh2_hbm, LAST, 1)

    def full(v):
        return jnp.sum(jnp.sum(v, axis=0, keepdims=True), axis=1, keepdims=True)

    lane = lax.broadcasted_iota(jnp.int32, (1, 128), 1)
    mbuf[pl.ds(me, 1), :] = jnp.where(lane == 0, full(gm[0]), jnp.where(lane == 1, full(gm[1]), full(gm[2])))

    def row_of(ref):
        return ref.at[pl.ds(me, 1), :]

    keep = pltpu.make_async_copy(row_of(mbuf), row_of(rows_hbm), ld_sem.at[0])
    keep.start()

    def m_send(to_z, to_j):
        remote(row_of(mbuf), row_of(rows_hbm), mss, mrs, to_z, to_j).start()

    mates = [(j + i) % 8 for i in MATES]
    for to_z in reversed(pos.shares[1:]):
        for to_j in [j] + mates:
            m_send(to_z, to_j)
    for to_j in mates:
        m_send(z, to_j)

    for b in TWO:
        e_pair(b).wait_send()

        @pl.when(inner)
        def _():
            e_mirror(b).wait_send()
            for k in LINE:
                e_forward(k, b).wait_send()

    for kind, acc in enumerate((acc1, acc2)):
        for stage, part in enumerate((acc.at[:, :, :, :, 0], acc.at[:, :, :, 0, 0], acc.at[:, :, 0, 0, 0])):
            remote(part, part, rss.at[kind, stage], rsr.at[0, stage], z, pos.jc).wait_send()
    pltpu.make_async_copy(r3a, sh1_hbm, sh_sem.at[0]).wait()
    pltpu.make_async_copy(r3b, sh2_hbm, sh_sem.at[1]).wait()

    keep.wait()
    lines = pl.ds(0, NDEV - 1)
    remote(mbuf.at[lines, :], rows_hbm.at[lines, :], mss, mrs, z, pos.jc).wait()


def main_call(x, w1, w2r, heads, labels):
    dma = pltpu.SemaphoreType.DMA
    anyspec = pl.BlockSpec(memory_space=pl.ANY)
    up, down = (OWN, CH), (GR, D)
    pair, quad, octet = (2,), (2, 2), (2, 2, 2)
    per_chunk = (NCH, 2)
    vmem = pltpu.VMEM
    return pl.pallas_call(
        main_kernel,
        out_shape=(jax.ShapeDtypeStruct((NCH, NTOK, CH), F32),
                   jax.ShapeDtypeStruct(per_chunk + up, F32),
                   jax.ShapeDtypeStruct(per_chunk + down, F32),
                   jax.ShapeDtypeStruct((NDEV, 128), F32)),
        in_specs=[anyspec] * 5,
        out_specs=(anyspec, anyspec, anyspec, anyspec),
        scratch_shapes=[
            vmem((8, TB, DD), BF),
            vmem((NCH, 8, GR, DD), BF),
            vmem(per_chunk + octet + up, F32), vmem(per_chunk + octet + down, F32),
            vmem((2, 2) + quad + up, F32), vmem((2, 2) + quad + down, F32),
            vmem((2, 2) + pair + up, F32), vmem((2, 2) + pair + down, F32),
            vmem(per_chunk + up, F32), vmem(per_chunk + down, F32),
            vmem((4, ER, NOWN), F32),
            vmem((4, TB, CH), F32),
            vmem((3 * ER, DD), BF),
            vmem((ER, D), BF),
            vmem((NC, 2, D), BF),
            vmem((2, NOWN), jnp.int32),
            vmem((3, 8, 128), F32), vmem((NDEV, 128), F32),
            dma((4,)), dma((NG,)), dma((NCH,)), dma(()), dma((NG,)), dma(()), dma((FAR,)), dma(()), dma((NG,)), dma(()), dma((NG,)),
            dma((5,)), dma((NCH,)), dma((4,)), dma((6,)), dma(quad), dma((4, 2)), dma((4, 2)),
            dma((2, NCH)), dma((14, NCH)), dma(()), dma(()), dma(pair),
        ],
        compiler_params=pltpu.CompilerParams(
            collective_id=0, has_side_effects=True, vmem_limit_bytes=VMEM_BYTES),
        name='main',
    )(x, w1, w2r, heads, labels)


def result_kernel(rows_hbm, sh1_hbm, sh2_hbm, a_ref, g1_ref, g2_ref, rows, sh1, sh2, sem):
    ld_rows = pltpu.make_async_copy(rows_hbm, rows, sem.at[0])
    loads = [pltpu.make_async_copy(sh1_hbm, sh1, sem.at[1]), pltpu.make_async_copy(sh2_hbm, sh2, sem.at[2])]
    ld_rows.start()
    for cp in loads:
        cp.start()
    ld_rows.wait()

    gram = jnp.sum(rows[...], axis=0, keepdims=True)
    lane = lax.broadcasted_iota(jnp.int32, gram.shape, 1)

    def entry(i):
        return jnp.sum(jnp.where(lane == i, gram, 0.0), axis=1, keepdims=True)

    g00, g01, g11 = entry(0), entry(1), entry(2)
    scale = (g00 + g11) * -0.5
    g00, g01, g11 = g00 / scale, g01 / scale, g11 / scale
    a0 = a1 = jnp.full((1, 1), 0.5, F32)
    for _ in range(STEPS):
        v0 = a0 * jnp.exp(g00 * a0 + g01 * a1)
        v1 = a1 * jnp.exp(g01 * a0 + g11 * a1)
        tot = v0 + v1
        a0, a1 = v0 / tot, v1 / tot
    a_ref[0] = a0[0, 0]
    a_ref[1] = a1[0, 0]
    for cp in loads:
        cp.wait()
    for c in range(NCH):
        comb = a0 * sh1[c, 0] + a1 * sh1[c, 1]
        for g in range(8):
            col = g * NCH * GR + c * GR
            g1_ref[:, col:col + GR] = comb[:, g * GR:(g + 1) * GR]
        g2_ref[c * GR:(c + 1) * GR, :] = a0 * sh2[c, 0] + a1 * sh2[c, 1]


def result_call(rows, sh1, sh2):
    vspec = pl.BlockSpec(memory_space=pltpu.VMEM)
    anyspec = pl.BlockSpec(memory_space=pl.ANY)
    return pl.pallas_call(
        result_kernel,
        out_shape=(jax.ShapeDtypeStruct((2,), F32), jax.ShapeDtypeStruct((OWN, D), F32),
                   jax.ShapeDtypeStruct((OWN, D), F32)),
        in_specs=[anyspec] * NCH,
        out_specs=(pl.BlockSpec(memory_space=pltpu.SMEM), vspec, vspec),
        scratch_shapes=[pltpu.VMEM(v.shape, F32) for v in (rows, sh1, sh2)] + [pltpu.SemaphoreType.DMA((NCH,))],
        name='result',
    )(rows, sh1, sh2)


def solution(mesh):
    def local_step(tokens, w_up, w_down, task_heads, labels):
        w2r = w_down.reshape(8, NCH, GR, D)
        heads = jnp.transpose(task_heads, (2, 0, 1))
        _, sh1, sh2, rows = main_call(tokens, w_up, w2r, heads, labels)
        return result_call(rows, sh1, sh2)

    return jax.shard_map(
        local_step, mesh=mesh,
        in_specs=(P('data', None), P(None, 'model'), P('model', None), P(None, None, None), P(None, 'data')),
        out_specs=(P(None), P('data', 'model'), P(('model', 'data'), None)),
        check_vma=False)
```
